32 devices in a mesh: replica: 16 (over z, x, core), group: 2 (over y).
Axes of the slice: x: 2, y: 2, z: 4, core: 2. Of those that a mesh axis runs over, the one named last changes fastest.
Arguments:
- inputs: bfloat16 [640, 197, 384], P(('replica', 'group')), may hold values from -6 to 6
- cotangent: bfloat16 [640, 197, 384], P(('replica', 'group')), may hold values from -6 to 6
- gain_one: bfloat16 [384], P('group'), may hold values from 0.5 to 1.5
- shift_one: bfloat16 [384], P('group'), may hold values from -3 to 3
- w_qkv: bfloat16 [384, 1152], P('group'), may hold values from -2 to 2
- b_query: bfloat16 [384], P('group'), may hold values from -3 to 3
- b_value: bfloat16 [384], P('group'), may hold values from -3 to 3
- w_proj: bfloat16 [384, 384], P('group'), may hold values from -0.875 to 0.875
- b_proj: bfloat16 [384], P('group'), may hold values from -3 to 3
- gain_two: bfloat16 [384], P('group'), may hold values from 0.5 to 1.5
- shift_two: bfloat16 [384], P('group'), may hold values from -3 to 3
- w_fc1: bfloat16 [384, 1536], P('group'), may hold values from -0.3125 to 0.3125
- b_fc1: bfloat16 [1536], P('group'), may hold values from -3 to 3
- w_fc2: bfloat16 [1536, 384], P('group'), may hold values from -0.15625 to 0.15625
- b_fc2: bfloat16 [384], P('group'), may hold values from -3 to 3
Outputs:
- outputs: bfloat16 [640, 197, 384], P(('replica', 'group'))
- grad_inputs: float32 [640, 197, 384], P(('replica', 'group'))
- grad_gain_one: float32 [384], P('group')
- grad_shift_one: float32 [384], P('group')
- grad_w_qkv: float32 [384, 1152], P('group')
- grad_b_query: float32 [384], P('group')
- grad_b_value: float32 [384], P('group')
- grad_w_proj: float32 [384, 384], P('group')
- grad_b_proj: float32 [384], P('group')
- grad_gain_two: float32 [384], P('group')
- grad_shift_two: float32 [384], P('group')
- grad_w_fc1: float32 [384, 1536], P('group')
- grad_b_fc1: float32 [1536], P('group')
- grad_w_fc2: float32 [1536, 384], P('group')
- grad_b_fc2: float32 [384], P('group')
The draws below stay inside these ranges and needn't reach their ends.
All inputs are finite; a program needn't handle non-finite values.
Results may differ from the reference program's by a relative error of at most 0.012.
Values may be sent and summed in bfloat16 or wider, within the bound.
A program may use at most 256 MiB of HBM per device.

```python
import jax
import jax.numpy as jnp
from jax import lax

D = 384
HEADS = 6
FF = 1536
SEQ = 197
IMG_DEV = 20
IMAGES = 640


def draw_w_qkv(key, part):
    drawn_draw = jax.random.truncated_normal(key, -6.0, 6.0, (D, 3 * D), jnp.float32) * D ** (-0.5)
    drawn_draw = jnp.clip(drawn_draw, -2.0, 2.0)
    return drawn_draw.astype(jnp.bfloat16)


def block_levels(key, shape, split, low, largest):
    factor_of = 1.0
    for dim, blocks in split:
        draws = jax.random.uniform(jax.random.fold_in(jax.random.fold_in(key, 6), dim), (blocks,), jnp.float32, low / len(split), largest / len(split))
        factor_of = factor_of * jnp.repeat(jnp.exp(draws), shape[dim] // blocks).reshape((-1,) + (1,) * (len(shape) - 1 - dim))
    return factor_of


def bell_draw(stream_key, extent, scale, reach, split=(), kind=jnp.bfloat16):
    array = scale * jax.random.normal(stream_key, extent, jnp.float32)
    if split:
        array = array * block_levels(stream_key, extent, split, -0.22, 0.18)
    return jnp.clip(array, -reach, reach).astype(kind)


def setup_inputs(seed: int = 0) -> dict:
    arg_keys = jax.random.split(jax.random.key(seed), 16)
    inputs = bell_draw(arg_keys[0], (IMAGES, SEQ, D), 1.0, 6.0, ((0, 32),))
    cotangent = bell_draw(arg_keys[1], (IMAGES, SEQ, D), 1.0, 6.0, ((0, 32),))
    gain_one = jnp.clip(1.0 + 0.1 * jax.random.normal(arg_keys[2], (D,), jnp.float32), 0.5, 1.5).astype(jnp.bfloat16)
    shift_one = bell_draw(arg_keys[3], (D,), 0.5, 3.0, ((0, 2),))
    w_qkv = draw_w_qkv(jax.random.fold_in(arg_keys[15], 71), 0)
    b_query = bell_draw(arg_keys[5], (D,), 0.5, 3.0, ((0, 2),))
    b_value = bell_draw(arg_keys[6], (D,), 0.5, 3.0, ((0, 2),))
    w_proj = bell_draw(arg_keys[7], (D, D), (D // 8) ** -0.5, 0.875, ((0, 2),))
    b_proj = bell_draw(arg_keys[8], (D,), 0.5, 3.0, ((0, 2),))
    gain_two = jnp.clip(1.0 + 0.1 * jax.random.normal(arg_keys[9], (D,), jnp.float32), 0.5, 1.5).astype(jnp.bfloat16)
    shift_two = bell_draw(arg_keys[10], (D,), 0.5, 3.0, ((0, 2),))
    w_fc1 = bell_draw(arg_keys[11], (D, FF), D ** -0.5, 0.3125, ((0, 2),))
    b_fc1 = bell_draw(arg_keys[12], (FF,), 0.5, 3.0, ((0, 2),))
    w_fc2 = bell_draw(arg_keys[13], (FF, D), FF ** -0.5, 0.15625, ((0, 2),))
    b_fc2 = bell_draw(arg_keys[14], (D,), 0.5, 3.0, ((0, 2),))
    return {"inputs": inputs, "cotangent": cotangent, "gain_one": gain_one, "shift_one": shift_one, "w_qkv": w_qkv, "b_query": b_query, "b_value": b_value, "w_proj": w_proj, "b_proj": b_proj, "gain_two": gain_two, "shift_two": shift_two, "w_fc1": w_fc1, "b_fc1": b_fc1, "w_fc2": w_fc2, "b_fc2": b_fc2}


epsilon = 1e-06

def product(left, right):
    return jnp.dot(left, right, preferred_element_type=jnp.float32)

def layer_norm(token_rows, gain_row, shift_row):
    centre = lax.optimization_barrier(jnp.mean(token_rows, axis=-1, keepdims=True))
    centered = token_rows - centre
    inverse = lax.rsqrt(lax.optimization_barrier(jnp.mean(centered * centered, axis=-1, keepdims=True)) + epsilon)
    normed = centered * inverse
    hidden = (normed * gain_row.astype(jnp.float32) + shift_row.astype(jnp.float32)).astype(jnp.bfloat16)
    return (normed, inverse, hidden)

def norm_backward(grad_hidden, normed, inverse, gain_row):
    grad_normed = grad_hidden * gain_row.astype(jnp.float32)
    average_one = lax.optimization_barrier(jnp.mean(grad_normed, axis=-1, keepdims=True))
    average_two = lax.optimization_barrier(jnp.mean(grad_normed * normed, axis=-1, keepdims=True))
    grad_rows = inverse * (grad_normed - average_one - normed * average_two)
    return (grad_rows, lax.optimization_barrier(jnp.sum(grad_hidden * normed, axis=0)), lax.optimization_barrier(jnp.sum(grad_hidden, axis=0)))

def gelu_slope(values):
    return 0.5 * (1.0 + lax.erf(values * 0.7071067811865476)) + values * jnp.exp(-0.5 * values * values) * 0.3989422804014327

def batch_einsum(form, left, right):
    return jnp.einsum(form, left.astype(jnp.float32), right.astype(jnp.float32))

def local_pass(inputs, cotangent, params):
    gain_one, shift_one, w_qkv, b_query, b_value, w_proj, b_proj, gain_two, shift_two, w_fc1, b_fc1, w_fc2, b_fc2 = params
    images, length, width = inputs.shape
    head_dim = width // HEADS
    scaling = head_dim ** (-0.5)
    row_count = images * length
    token_rows = inputs.reshape(row_count, width).astype(jnp.float32)
    normed_one, inverse_one, hidden_one = layer_norm(token_rows, gain_one, shift_one)
    bias_full = jnp.concatenate([b_query, jnp.zeros_like(b_query), b_value]).astype(jnp.float32)
    packed = (product(hidden_one, w_qkv) + bias_full).astype(jnp.bfloat16)
    packed = packed.reshape(images, length, 3, HEADS, head_dim)
    query = packed[:, :, 0]
    keys = packed[:, :, 1]
    values = packed[:, :, 2]
    scores = batch_einsum('bshe,bthe->bhst', query, keys) * scaling
    log_total = jax.nn.logsumexp(scores, axis=-1, keepdims=True)
    probs = jnp.exp(scores - log_total)
    probs_b = probs.astype(jnp.bfloat16)
    attended = batch_einsum('bhst,bthe->bshe', probs_b, values).astype(jnp.bfloat16).reshape(row_count, width)
    resid = token_rows + product(attended, w_proj) + b_proj.astype(jnp.float32)
    normed_two, inverse_two, hidden_two = layer_norm(resid, gain_two, shift_two)
    pre_act = product(hidden_two, w_fc1) + b_fc1.astype(jnp.float32)
    act_b = jax.nn.gelu(pre_act, approximate=False).astype(jnp.bfloat16)
    outputs = (resid + product(act_b, w_fc2) + b_fc2.astype(jnp.float32)).astype(jnp.bfloat16)
    grad_out = cotangent.reshape(row_count, width)
    grad_top = grad_out.astype(jnp.float32)
    grad_b_fc2 = lax.optimization_barrier(jnp.sum(grad_top, axis=0))
    grad_w_fc2 = product(act_b.T, grad_out)
    grad_pre = product(grad_out, w_fc2.T) * gelu_slope(pre_act)
    grad_b_fc1 = lax.optimization_barrier(jnp.sum(grad_pre, axis=0))
    grad_pre_b = grad_pre.astype(jnp.bfloat16)
    grad_w_fc1 = product(hidden_two.T, grad_pre_b)
    grad_hidden_two = product(grad_pre_b, w_fc1.T)
    grad_part, grad_gain_two, grad_shift_two = norm_backward(grad_hidden_two, normed_two, inverse_two, gain_two)
    grad_resid = grad_top + grad_part
    grad_b_proj = lax.optimization_barrier(jnp.sum(grad_resid, axis=0))
    grad_resid_b = grad_resid.astype(jnp.bfloat16)
    grad_w_proj = product(attended.T, grad_resid_b)
    grad_attended = product(grad_resid_b, w_proj.T).astype(jnp.bfloat16).reshape(images, length, HEADS, head_dim)
    grad_values = batch_einsum('bhst,bshe->bthe', probs_b, grad_attended)
    grad_probs = batch_einsum('bshe,bthe->bhst', grad_attended, values)
    delta_rows = lax.optimization_barrier(jnp.sum(probs * grad_probs, axis=-1, keepdims=True))
    grad_scores = (probs * (grad_probs - delta_rows) * scaling).astype(jnp.bfloat16)
    grad_query = batch_einsum('bhst,bthe->bshe', grad_scores, keys)
    grad_keys = batch_einsum('bhst,bshe->bthe', grad_scores, query)
    grad_b_query = lax.optimization_barrier(jnp.sum(grad_query.reshape(row_count, width), axis=0))
    grad_b_value = lax.optimization_barrier(jnp.sum(grad_values.reshape(row_count, width), axis=0))
    grad_packed = jnp.stack([grad_query, grad_keys, grad_values], axis=2).reshape(row_count, 3 * width)
    grad_packed_b = grad_packed.astype(jnp.bfloat16)
    grad_w_qkv = product(hidden_one.T, grad_packed_b)
    grad_hidden_one = product(grad_packed_b, w_qkv.T)
    grad_first, grad_gain_one, grad_shift_one = norm_backward(grad_hidden_one, normed_one, inverse_one, gain_one)
    grad_inputs = grad_resid + grad_first
    grads = (grad_gain_one, grad_shift_one, grad_w_qkv, grad_b_query, grad_b_value, grad_w_proj, grad_b_proj, grad_gain_two, grad_shift_two, grad_w_fc1, grad_b_fc1, grad_w_fc2, grad_b_fc2)
    return (outputs.reshape(images, length, width), grad_inputs.reshape(images, length, width), grads)

def reference(inputs, cotangent, gain_one, shift_one, w_qkv, b_query, b_value, w_proj, b_proj, gain_two, shift_two, w_fc1, b_fc1, w_fc2, b_fc2):
    params = (gain_one, shift_one, w_qkv, b_query, b_value, w_proj, b_proj, gain_two, shift_two, w_fc1, b_fc1, w_fc2, b_fc2)
    block_count = IMAGES // IMG_DEV
    input_blocks = inputs.reshape(block_count, IMG_DEV, SEQ, D)
    cot_blocks = cotangent.reshape(block_count, IMG_DEV, SEQ, D)

    def one_block(totals, pair):
        block_out, block_grad, grads = local_pass(pair[0], pair[1], params)
        return (tuple((total + piece for total, piece in zip(totals, grads))), (block_out, block_grad))
    starting = tuple((jnp.zeros(param.shape, jnp.float32) for param in params))
    totals, (outs_all, grads_all) = lax.scan(one_block, starting, (input_blocks, cot_blocks))
    factor = float(IMAGES * SEQ) ** (-0.5)
    scaled = tuple((total * factor for total in totals))
    return (outs_all.reshape(IMAGES, SEQ, D), grads_all.reshape(IMAGES, SEQ, D), scaled[0], scaled[1], scaled[2], scaled[3], scaled[4], scaled[5], scaled[6], scaled[7], scaled[8], scaled[9], scaled[10], scaled[11], scaled[12])
```

```python
import functools

import jax
import jax.numpy as jnp
from jax import lax
from jax.experimental import pallas as pl
from jax.experimental.pallas import tpu as pltpu
from jax.sharding import PartitionSpec as P

HEADS = 6
EPS = 1e-06
BF = jnp.bfloat16
F32 = jnp.float32
LOG2E = 1.4426950408889634
VMEM_LIMIT = 60 * 1024 * 1024


def dot(left, right):
    return jnp.dot(left, right, preferred_element_type=F32)


def dot_lt(left, right):
    return lax.dot_general(left, right, (((0,), (0,)), ((), ())), preferred_element_type=F32)


def dot_rt(left, right):
    return lax.dot_general(left, right, (((1,), (1,)), ((), ())), preferred_element_type=F32)


def row_stats(rows):
    centre = jnp.mean(rows, axis=-1, keepdims=True)
    centered = rows - centre
    inverse = lax.rsqrt(jnp.mean(centered * centered, axis=-1, keepdims=True) + EPS)
    return centered * inverse, inverse


def norm_back(grad_hidden, normed, inverse, gain):
    grad_normed = grad_hidden * gain
    one = jnp.mean(grad_normed, axis=-1, keepdims=True)
    two = jnp.mean(grad_normed * normed, axis=-1, keepdims=True)
    return inverse * (grad_normed - one - normed * two)


def col_sum(rows):
    return jnp.sum(rows, axis=0, keepdims=True)


def attention_forward(length, pitch, count, x_ref, w_ref, vec_ref, bias_ref, packed_ref, probs_ref, att_ref, pad_ref):
    width = x_ref.shape[2]
    head_dim = width // HEADS
    pair = 2 * head_dim
    factor = head_dim ** (-0.5) * LOG2E

    @pl.when(pl.program_id(0) == 0)
    def _():
        pad_ref[...] = jnp.zeros_like(pad_ref)

    gain = vec_ref[0:1, :].astype(F32)
    shift = vec_ref[1:2, :].astype(F32)
    for image in range(count):
        pad_ref[image * pitch : image * pitch + length, :] = x_ref[image]
    normed, _ = row_stats(pad_ref[...].astype(F32))
    hidden = (normed * gain + shift).astype(BF)
    packed = (dot(hidden, w_ref[...]) + bias_ref[...].astype(F32)).astype(BF)
    for image in range(count):
        packed_ref[image] = packed[image * pitch : (image + 1) * pitch]
    lane = lax.broadcasted_iota(jnp.int32, (pitch, pair), 1)
    tail = length // 8 * 8
    row = lax.broadcasted_iota(jnp.int32, (pitch - tail, pitch), 0) + tail
    for image in range(count):
        for two in range(HEADS // 2):
            cols = slice(two * pair, (two + 1) * pair)
            query = packed_ref[image, :, two * pair : (two + 1) * pair]
            keys = packed_ref[image, :, width + two * pair : width + (two + 1) * pair]
            values = packed_ref[image, :, 2 * width + two * pair : 2 * width + (two + 1) * pair]
            values_t = values.T
            parts = []
            for side in range(2):
                own = (lane < head_dim) if side == 0 else (lane >= head_dim)
                scores = dot_rt(keys, jnp.where(own, query, jnp.zeros_like(query)))
                low = jnp.where(row < length, scores[tail:], -1e30)
                scores = jnp.concatenate([scores[:tail], low], axis=0)
                top = jnp.max(scores, axis=0, keepdims=True)
                raised = jnp.exp2((scores - top) * factor)
                total = jnp.sum(raised, axis=0, keepdims=True)
                probs = (raised * (1.0 / total)).astype(BF)
                probs_ref[image, 2 * two + side] = probs
                parts.append(dot(values_t[side * head_dim : (side + 1) * head_dim], probs))
            mixed = jnp.concatenate(parts, axis=0)
            att_ref[image, :, cols] = mixed.T.astype(BF)


def gelu_parts(values):
    half = 0.5 * (1.0 + lax.erf(values * 0.7071067811865476))
    slope = half + values * jnp.exp(-0.5 * values * values) * 0.3989422804014327
    return half, slope


def mlp_both(
    length, pitch, count, chunk,
    x_ref, ct_ref, att_ref, wp_ref, w1_ref, w2_ref, vec_ref, b1_ref,
    y_ref, gr_ref, dw1_ref, dw2t_ref, dwp_ref, dvec_ref, db1_ref,
    xpad, ctpad, act_ref, gp_ref, acc1, acc2, accp, accv, accb,
):
    step = pl.program_id(0)
    hidden_units = w1_ref.shape[1]

    @pl.when(step == 0)
    def _():
        for ref in (xpad, ctpad, acc1, acc2, accp, accv, accb):
            ref[...] = jnp.zeros_like(ref)

    for image in range(count):
        xpad[image * pitch : image * pitch + length, :] = x_ref[image]
        ctpad[image * pitch : image * pitch + length, :] = ct_ref[image]
    bias_p = vec_ref[4:5, :].astype(F32)
    gain = vec_ref[5:6, :].astype(F32)
    shift = vec_ref[6:7, :].astype(F32)
    bias_2 = vec_ref[7:8, :].astype(F32)
    ct = ctpad[...]
    att = att_ref[...].reshape(count * pitch, att_ref.shape[2])
    resid = xpad[...].astype(F32) + dot(att, wp_ref[...]) + bias_p
    normed, inverse = row_stats(resid)
    hidden = (normed * gain + shift).astype(BF)
    for start in range(0, hidden_units, chunk):
        cols = slice(start, start + chunk)
        pre = dot(hidden, w1_ref[:, cols]) + b1_ref[:, cols].astype(F32)
        half, slope = gelu_parts(pre)
        act_ref[:, cols] = (pre * half).astype(BF)
        grad_pre = dot_rt(ct, w2_ref[cols, :]) * slope
        accb[:, cols] += col_sum(grad_pre)
        gp_ref[:, cols] = grad_pre.astype(BF)
    out = resid + dot(act_ref[...], w2_ref[...]) + bias_2
    for image in range(count):
        y_ref[image] = out[image * pitch : image * pitch + length].astype(BF)
    grad_hidden = dot_rt(gp_ref[...], w1_ref[...])
    top = ct.astype(F32)
    grad_resid = top + norm_back(grad_hidden, normed, inverse, gain)
    accv[0:1, :] += col_sum(grad_resid)
    accv[1:2, :] += col_sum(grad_hidden * normed)
    accv[2:3, :] += col_sum(grad_hidden)
    accv[3:4, :] += col_sum(top)
    gr_ref[...] = grad_resid.reshape(gr_ref.shape)
    acc1[...] += dot_lt(hidden, gp_ref[...])
    acc2[...] += dot_lt(ct, act_ref[...])
    accp[...] += dot_lt(att, grad_resid.astype(BF))

    @pl.when(step == pl.num_programs(0) - 1)
    def _():
        dw1_ref[...] = acc1[...].astype(BF)
        dw2t_ref[...] = acc2[...].astype(BF)
        dwp_ref[...] = accp[...].astype(BF)
        dvec_ref[...] = accv[...]
        db1_ref[...] = accb[...]


def attention_backward(
    length, pitch, count,
    x_ref, gr_ref, packed_ref, probs_ref, wp_ref, w_ref, vec_ref,
    gx_ref, dw_ref, dvec_ref,
    pad_ref, gp_ref, acc, accv,
):
    step = pl.program_id(0)
    width = x_ref.shape[2]
    head_dim = width // HEADS
    pair = 2 * head_dim
    factor = head_dim ** (-0.5)

    @pl.when(step == 0)
    def _():
        for ref in (pad_ref, acc, accv):
            ref[...] = jnp.zeros_like(ref)

    gain = vec_ref[0:1, :].astype(F32)
    shift = vec_ref[1:2, :].astype(F32)
    for image in range(count):
        pad_ref[image * pitch : image * pitch + length, :] = x_ref[image]
    grad_resid = gr_ref[...].reshape(count * pitch, width)
    grad_att = dot_rt(grad_resid.astype(BF), wp_ref[...]).astype(BF)
    lane = lax.broadcasted_iota(jnp.int32, (pitch, pair), 1)
    for image in range(count):
        rows = slice(image * pitch, (image + 1) * pitch)
        for two in range(HEADS // 2):
            cols = slice(two * pair, (two + 1) * pair)
            query = packed_ref[image, :, two * pair : (two + 1) * pair]
            keys = packed_ref[image, :, width + two * pair : width + (two + 1) * pair]
            values = packed_ref[image, :, 2 * width + two * pair : 2 * width + (two + 1) * pair]
            grad_out = grad_att[rows, cols]
            keys_t = keys.T
            grad_values = None
            grad_keys = None
            parts = []
            for side in range(2):
                own = (lane < head_dim) if side == 0 else (lane >= head_dim)
                zero = jnp.zeros_like(query)
                grad_side = jnp.where(own, grad_out, zero)
                probs_b = probs_ref[image, 2 * two + side]
                probs = probs_b.astype(F32)
                grad_probs = dot_rt(values, grad_side)
                delta = jnp.sum(probs * grad_probs, axis=0, keepdims=True)
                grad_scores = (probs * (grad_probs - delta)).astype(BF)
                piece_v = dot(probs_b, grad_side)
                piece_k = dot(grad_scores, jnp.where(own, query, zero))
                grad_values = piece_v if grad_values is None else grad_values + piece_v
                grad_keys = piece_k if grad_keys is None else grad_keys + piece_k
                parts.append(dot(keys_t[side * head_dim : (side + 1) * head_dim], grad_scores))
            grad_query = jnp.concatenate(parts, axis=0).T * factor
            grad_keys = grad_keys * factor
            accv[0:1, cols] += col_sum(grad_query)
            accv[1:2, cols] += col_sum(grad_values)
            gp_ref[rows, two * pair : (two + 1) * pair] = grad_query.astype(BF)
            gp_ref[rows, width + two * pair : width + (two + 1) * pair] = grad_keys.astype(BF)
            gp_ref[rows, 2 * width + two * pair : 2 * width + (two + 1) * pair] = grad_values.astype(BF)
    normed, inverse = row_stats(pad_ref[...].astype(F32))
    hidden = (normed * gain + shift).astype(BF)
    acc[...] += dot_lt(hidden, gp_ref[...])
    grad_hidden = dot_rt(gp_ref[...], w_ref[...])
    accv[2:3, :] += col_sum(grad_hidden * normed)
    accv[3:4, :] += col_sum(grad_hidden)
    grad_x = grad_resid + norm_back(grad_hidden, normed, inverse, gain)
    for image in range(count):
        gx_ref[image] = grad_x[image * pitch : image * pitch + length]

    @pl.when(step == pl.num_programs(0) - 1)
    def _():
        dw_ref[...] = acc[...].astype(BF)
        dvec_ref[...] = accv[...]


def whole(array):
    return pl.BlockSpec(array.shape, lambda i: (0,) * len(array.shape))


def blocks(count, *rest):
    return pl.BlockSpec((count,) + rest, lambda i: (i,) + (0,) * len(rest))


def fixed(*shape):
    return pl.BlockSpec(shape, lambda i: (0,) * len(shape))


def compute(inputs, cotangent, w_qkv, w_proj, w_fc1, w_fc2, vecs, bias_qkv, bias_fc1):
    images, length, width = inputs.shape
    hidden_units = w_fc1.shape[1]
    pitch = (length + 15) // 16 * 16
    sds = jax.ShapeDtypeStruct
    params = pltpu.CompilerParams(vmem_limit_bytes=VMEM_LIMIT, dimension_semantics=("arbitrary",))

    count = 2
    packed, probs, attended = pl.pallas_call(
        functools.partial(attention_forward, length, pitch, count),
        grid=(images // count,),
        in_specs=[blocks(count, length, width), whole(w_qkv), whole(vecs), whole(bias_qkv)],
        out_specs=[
            blocks(count, pitch, 3 * width),
            blocks(count, HEADS, pitch, pitch),
            blocks(count, pitch, width),
        ],
        out_shape=[
            sds((images, pitch, 3 * width), BF),
            sds((images, HEADS, pitch, pitch), BF),
            sds((images, pitch, width), BF),
        ],
        scratch_shapes=[pltpu.VMEM((count * pitch, width), BF)],
        compiler_params=params,
        name="attention_forward",
    )(inputs, w_qkv, vecs, bias_qkv)

    count = 2
    rows = count * pitch
    outputs, grad_resid, d_fc1, d_fc2t, d_proj, d_vec, d_b1 = pl.pallas_call(
        functools.partial(mlp_both, length, pitch, count, 256),
        grid=(images // count,),
        in_specs=[
            blocks(count, length, width),
            blocks(count, length, width),
            blocks(count, pitch, width),
            whole(w_proj), whole(w_fc1), whole(w_fc2), whole(vecs), whole(bias_fc1),
        ],
        out_specs=[
            blocks(count, length, width),
            blocks(count, pitch, width),
            fixed(width, hidden_units), fixed(width, hidden_units), fixed(width, width),
            fixed(8, width), fixed(1, hidden_units),
        ],
        out_shape=[
            sds((images, length, width), BF),
            sds((images, pitch, width), F32),
            sds((width, hidden_units), BF), sds((width, hidden_units), BF), sds((width, width), BF),
            sds((8, width), F32), sds((1, hidden_units), F32),
        ],
        scratch_shapes=[
            pltpu.VMEM((rows, width), BF), pltpu.VMEM((rows, width), BF),
            pltpu.VMEM((rows, hidden_units), BF), pltpu.VMEM((rows, hidden_units), BF),
            pltpu.VMEM((width, hidden_units), F32), pltpu.VMEM((width, hidden_units), F32),
            pltpu.VMEM((width, width), F32), pltpu.VMEM((8, width), F32), pltpu.VMEM((1, hidden_units), F32),
        ],
        compiler_params=params,
        name="mlp_both",
    )(inputs, cotangent, attended, w_proj, w_fc1, w_fc2, vecs, bias_fc1)

    count = 2
    rows = count * pitch
    grad_inputs, d_qkv, d_vec2 = pl.pallas_call(
        functools.partial(attention_backward, length, pitch, count),
        grid=(images // count,),
        in_specs=[
            blocks(count, length, width),
            blocks(count, pitch, width),
            blocks(count, pitch, 3 * width),
            blocks(count, HEADS, pitch, pitch),
            whole(w_proj), whole(w_qkv), whole(vecs),
        ],
        out_specs=[blocks(count, length, width), fixed(width, 3 * width), fixed(8, width)],
        out_shape=[
            sds((images, length, width), F32),
            sds((width, 3 * width), BF),
            sds((8, width), F32),
        ],
        scratch_shapes=[
            pltpu.VMEM((rows, width), BF), pltpu.VMEM((rows, 3 * width), BF),
            pltpu.VMEM((width, 3 * width), F32), pltpu.VMEM((8, width), F32),
        ],
        compiler_params=params,
        name="attention_backward",
    )(inputs, grad_resid, packed, probs, w_proj, w_qkv, vecs)
    return outputs, grad_inputs, d_fc1, d_fc2t, d_proj, d_qkv, d_vec, d_vec2, d_b1


def local(
    inputs, cotangent, gain_one, shift_one, w_qkv, b_query, b_value, w_proj, b_proj,
    gain_two, shift_two, w_fc1, b_fc1, w_fc2, b_fc2,
):
    def gather(piece):
        return lax.all_gather(piece, "group", axis=0, tiled=True)

    width = inputs.shape[2]
    members = lax.axis_size("group")
    share = width // members
    small = jnp.concatenate(
        [gain_one, shift_one, b_query, b_value, b_proj, gain_two, shift_two, b_fc2, b_fc1]
    ).reshape(-1, share)
    small = lax.all_gather(small, "group", axis=0)
    vecs = small[:, :8].transpose(1, 0, 2).reshape(8, width)
    bias_fc1 = small[:, 8:].reshape(1, -1)
    bias_qkv = jnp.concatenate([vecs[2], jnp.zeros_like(vecs[2]), vecs[3]]).reshape(1, -1)
    outputs, grad_inputs, d_fc1, d_fc2t, d_proj, d_qkv, d_vec, d_vec2, d_b1 = compute(
        inputs, cotangent, gather(w_qkv), gather(w_proj), gather(w_fc1), gather(w_fc2), vecs, bias_qkv, bias_fc1
    )
    token_total = inputs.shape[0] * inputs.shape[1] * lax.axis_size("replica") * members
    factor = float(token_total) ** (-0.5)
    big = jnp.concatenate([d_qkv, d_proj, d_fc1, d_fc2t], axis=1)
    position = lax.axis_index("group")
    flat = jnp.concatenate([d_vec[:4].reshape(-1), d_vec2[:4].reshape(-1), d_b1.reshape(-1)])
    big, flat = lax.psum((big, flat), ("replica", "group"))
    big = big.astype(F32) * factor
    flat = flat * factor
    cut = [3 * width, 4 * width, 4 * width + w_fc1.shape[1]]

    def rows(block):
        return lax.dynamic_slice_in_dim(block, position * (block.shape[0] // members), block.shape[0] // members, 0)

    g_qkv, g_proj, g_fc1 = (rows(big[:, a:b]) for a, b in zip([0] + cut, cut))
    g_fc2 = rows(big[:, cut[2] :].T)
    names = ["b_proj", "gain_two", "shift_two", "b_fc2", "b_query", "b_value", "gain_one", "shift_one"]
    got = {name: rows(flat[k * width : (k + 1) * width]) for k, name in enumerate(names)}
    g_b1 = rows(flat[8 * width :])
    return (
        outputs, grad_inputs, got["gain_one"], got["shift_one"], g_qkv, got["b_query"], got["b_value"],
        g_proj, got["b_proj"], got["gain_two"], got["shift_two"], g_fc1, g_b1, g_fc2, got["b_fc2"],
    )


def solution(mesh):
    images = P(("replica", "group"), None, None)
    line, table = P("group"), P("group", None)
    params = (line, line, table, line, line, table, line, line, line, table, line, table, line)
    return jax.shard_map(
        local, mesh=mesh, in_specs=(images, images) + params, out_specs=(images, images) + params, check_vma=False
    )
```

```python
import functools

import jax
import jax.numpy as jnp
from jax import lax
from jax.experimental import pallas as pl
from jax.experimental.pallas import tpu as pltpu
from jax.sharding import PartitionSpec as P

HEADS = 6
EPS = 1e-06
BF = jnp.bfloat16
F32 = jnp.float32
LOG2E = 1.4426950408889634
VMEM_LIMIT = 60 * 1024 * 1024
MESH = pl.DeviceIdType.MESH
LANES = 128
QUAD = 4


def dot(left, right):
    return jnp.dot(left, right, preferred_element_type=F32)


def dot_lt(left, right):
    return lax.dot_general(left, right, (((0,), (0,)), ((), ())), preferred_element_type=F32)


def dot_rt(left, right):
    return lax.dot_general(left, right, (((1,), (1,)), ((), ())), preferred_element_type=F32)


def row_stats(rows):
    centre = jnp.mean(rows, axis=-1, keepdims=True)
    centered = rows - centre
    inverse = lax.rsqrt(jnp.mean(centered * centered, axis=-1, keepdims=True) + EPS)
    return centered * inverse, inverse


def norm_back(grad_hidden, normed, inverse, gain):
    grad_normed = grad_hidden * gain
    one = jnp.mean(grad_normed, axis=-1, keepdims=True)
    two = jnp.mean(grad_normed * normed, axis=-1, keepdims=True)
    return inverse * (grad_normed - one - normed * two)


def col_sum(rows):
    return jnp.sum(rows, axis=0, keepdims=True)


def place():
    return lax.axis_index("replica"), lax.axis_index("group")


def greet(partners):
    barrier = pltpu.get_barrier_semaphore()
    for partner in partners:
        pl.semaphore_signal(barrier, inc=1, device_id=partner, device_id_type=MESH)
    pl.semaphore_wait(barrier, len(partners))


def remote(source, target, send, recv, device):
    return pltpu.make_async_remote_copy(
        src_ref=source, dst_ref=target, send_sem=send, recv_sem=recv, device_id=device, device_id_type=MESH
    )


class Gather:
    def __init__(self, shards, wholes, sends, recvs, passes, arrivals):
        self.replica, self.group = place()
        core = lax.rem(self.replica, 2)
        self.across = (self.replica, 1 - self.group)
        self.beside = (self.replica + 1 - 2 * core, self.group)
        self.first, self.second = [], []
        for k, (shard, whole_ref) in enumerate(zip(shards, wholes)):
            rows = shard.shape[0]
            half = rows // 2
            mine = pl.ds(pl.multiple_of(core * half, half), half)
            there = pl.ds(pl.multiple_of(self.group * rows + core * half, half), half)
            here = pl.ds(pl.multiple_of((1 - self.group) * rows + core * half, half), half)
            self.first.append(remote(shard.at[mine], whole_ref.at[there], sends.at[k], recvs.at[k], self.across))
            self.second.append(
                remote(whole_ref.at[here], whole_ref.at[here], passes.at[k], arrivals.at[k], self.beside)
            )


def attention_forward(
    length, pitch, count, late,
    x_ref, wq_hbm, wp_hbm, w1_hbm, w2_hbm, g1, s1, bq, bv, bp, g2, s2, b2, b1,
    packed_ref, probs_ref, att_ref, wq_out, wp_out, w1_out, w2_out, vec_out, b1_out,
    pad_ref, wq, wp, w1, w2, small, wide, vec, bias, b1_full,
    sends, recvs, passes, arrivals, vec_send, vec_recv, own_sem, out_sem,
):
    step = pl.program_id(0)
    width = x_ref.shape[2]
    head_dim = width // HEADS
    pair = 2 * head_dim
    factor = head_dim ** (-0.5) * LOG2E
    shards = (wq_hbm, wp_hbm, w1_hbm, w2_hbm)
    wholes = (wq, wp, w1, w2)
    outs = (wq_out, wp_out, w1_out, w2_out)
    move = Gather(shards, wholes, sends, recvs, passes, arrivals)
    group = move.group
    small_copy = remote(small.at[group], small.at[group], vec_send.at[0], vec_recv.at[0], move.across)
    wide_copy = remote(wide.at[group], wide.at[group], vec_send.at[1], vec_recv.at[1], move.across)
    owns = [
        pltpu.make_async_copy(
            shard, full.at[pl.ds(pl.multiple_of(group * shard.shape[0], shard.shape[0]), shard.shape[0])], own_sem.at[k]
        )
        for k, (shard, full) in enumerate(zip(shards, wholes))
    ]
    flush = [pltpu.make_async_copy(full, out, out_sem.at[k]) for k, (full, out) in enumerate(zip(wholes, outs))]
    last = pl.num_programs(0) - 1

    @pl.when(step == 0)
    def _():
        pad_ref[...] = jnp.zeros_like(pad_ref)
        share = g1.shape[0]
        for k, ref in enumerate((g1, s1, bq, bv, bp, g2, s2, b2)):
            small[group, k : k + 1, 0:share] = ref[...].reshape(1, share).astype(F32)
        wide[group, 0:1, :] = b1[...].reshape(1, b1.shape[0]).astype(F32)
        greet((move.across, move.beside))
        small_copy.start()
        for copy in move.first:
            copy.start()
        wide_copy.start()
        for copy in owns:
            copy.start()
        small_copy.wait()
        for side in range(2):
            vec[:, side * share : (side + 1) * share] = small[side, :, 0:share]
        bias[0:1, 0:width] = vec[2:3, :]
        bias[0:1, width : 2 * width] = jnp.zeros((1, width), F32)
        bias[0:1, 2 * width : 3 * width] = vec[3:4, :]
        vec_out[...] = vec[...]
        move.first[0].wait()
        move.second[0].start()
        owns[0].wait()
        move.second[0].wait()

    @pl.when(step == late)
    def _():
        for k in range(1, 4):
            move.first[k].wait()
            move.second[k].start()
        wide_copy.wait()
        for side in range(2):
            b1_full[0:1, side * b1.shape[0] : (side + 1) * b1.shape[0]] = wide[side, 0:1, :]
        b1_out[...] = b1_full[...]
        for k in range(1, 4):
            owns[k].wait()

    @pl.when(step == late + 2)
    def _():
        for k in range(1, 4):
            move.second[k].wait()
        for copy in flush:
            copy.start()

    gain = vec[0:1, :]
    shift = vec[1:2, :]
    for image in range(count):
        pad_ref[image * pitch : image * pitch + length, :] = x_ref[image]
    normed, _ = row_stats(pad_ref[...].astype(F32))
    hidden = (normed * gain + shift).astype(BF)
    packed = (dot(hidden, wq[...]) + bias[0:1, :]).astype(BF)
    for image in range(count):
        packed_ref[image] = packed[image * pitch : (image + 1) * pitch]
    lane = lax.broadcasted_iota(jnp.int32, (pitch, pair), 1)
    tail = length // 8 * 8
    row = lax.broadcasted_iota(jnp.int32, (pitch - tail, pitch), 0) + tail
    for image in range(count):
        for two in range(HEADS // 2):
            cols = slice(two * pair, (two + 1) * pair)
            query = packed_ref[image, :, two * pair : (two + 1) * pair]
            keys = packed_ref[image, :, width + two * pair : width + (two + 1) * pair]
            values = packed_ref[image, :, 2 * width + two * pair : 2 * width + (two + 1) * pair]
            values_t = values.T
            parts = []
            for side in range(2):
                own = (lane < head_dim) if side == 0 else (lane >= head_dim)
                scores = dot_rt(keys, jnp.where(own, query, jnp.zeros_like(query)))
                low = jnp.where(row < length, scores[tail:], -1e30)
                scores = jnp.concatenate([scores[:tail], low], axis=0)
                top = jnp.max(scores, axis=0, keepdims=True)
                raised = jnp.exp2((scores - top) * factor)
                total = jnp.sum(raised, axis=0, keepdims=True)
                probs = (raised * (1.0 / total)).astype(BF)
                probs_ref[image, 2 * two + side] = probs
                parts.append(dot(values_t[side * head_dim : (side + 1) * head_dim], probs))
            mixed = jnp.concatenate(parts, axis=0)
            att_ref[image, :, cols] = mixed.T.astype(BF)

    @pl.when(step == last)
    def _():
        for copy in flush:
            copy.wait()


def gelu_parts(values):
    half = 0.5 * (1.0 + lax.erf(values * 0.7071067811865476))
    slope = half + values * jnp.exp(-0.5 * values * values) * 0.3989422804014327
    return half, slope


def mlp_both(
    length, pitch, count, chunk,
    x_ref, ct_ref, att_ref, wp_ref, w1_ref, w2_ref, vec_ref, b1_ref,
    y_ref, gr_ref, ga_ref, unit_ref, strip_ref, dvec_ref,
    xpad, ctpad, act_ref, gp_ref, acc1, acc2, accp, accv, accb,
):
    step = pl.program_id(0)
    width = x_ref.shape[2]
    hidden_units = w1_ref.shape[1]

    @pl.when(step == 0)
    def _():
        for ref in (xpad, ctpad, acc1, acc2, accp, accv, accb):
            ref[...] = jnp.zeros_like(ref)

    for image in range(count):
        xpad[image * pitch : image * pitch + length, :] = x_ref[image]
        ctpad[image * pitch : image * pitch + length, :] = ct_ref[image]
    bias_p = vec_ref[4:5, :]
    gain = vec_ref[5:6, :]
    shift = vec_ref[6:7, :]
    bias_2 = vec_ref[7:8, :]
    ct = ctpad[...]
    att = att_ref[...].reshape(count * pitch, width)
    resid = xpad[...].astype(F32) + dot(att, wp_ref[...]) + bias_p
    normed, inverse = row_stats(resid)
    hidden = (normed * gain + shift).astype(BF)
    for start in range(0, hidden_units, chunk):
        cols = slice(start, start + chunk)
        pre = dot(hidden, w1_ref[:, cols]) + b1_ref[0:1, cols]
        half, slope = gelu_parts(pre)
        act_ref[:, cols] = (pre * half).astype(BF)
        grad_pre = dot_rt(ct, w2_ref[cols, :]) * slope
        accb[0:1, cols] += col_sum(grad_pre)
        gp_ref[:, cols] = grad_pre.astype(BF)
    out = resid + dot(act_ref[...], w2_ref[...]) + bias_2
    for image in range(count):
        y_ref[image] = out[image * pitch : image * pitch + length].astype(BF)
    grad_hidden = dot_rt(gp_ref[...], w1_ref[...])
    top = ct.astype(F32)
    grad_resid = top + norm_back(grad_hidden, normed, inverse, gain)
    accv[0:1, :] += col_sum(grad_resid)
    accv[1:2, :] += col_sum(grad_hidden * normed)
    accv[2:3, :] += col_sum(grad_hidden)
    accv[3:4, :] += col_sum(top)
    gr_ref[...] = grad_resid.reshape(gr_ref.shape)
    grad_resid_b = grad_resid.astype(BF)
    ga_ref[...] = dot_rt(grad_resid_b, wp_ref[...]).astype(BF).reshape(ga_ref.shape)
    acc1[...] += dot_lt(hidden, gp_ref[...])
    acc2[...] += dot_lt(ct, act_ref[...])
    accp[...] += dot_lt(att, grad_resid_b)

    @pl.when(step == pl.num_programs(0) - 1)
    def _():
        share = width // 2
        wide = hidden_units // 2
        for side in range(2):
            rows = slice(side * share, (side + 1) * share)
            for strip in range(hidden_units // LANES):
                unit, at = strip // QUAD, strip % QUAD * share
                unit_ref[unit, side, at : at + share, :] = acc1[rows, strip * LANES : (strip + 1) * LANES].astype(BF)
            for strip in range(wide // LANES):
                unit, at = strip // 2 + hidden_units // (QUAD * LANES), strip % 2 * width
                start = side * wide + strip * LANES
                unit_ref[unit, side, at : at + width, :] = acc2[:, start : start + LANES].astype(BF)
            for strip in range(width // LANES):
                strip_ref[strip, side] = accp[rows, strip * LANES : (strip + 1) * LANES].astype(BF)
        dvec_ref[...] = jnp.zeros_like(dvec_ref)
        dvec_ref[0:4, :] = accv[0:4, :]
        for k in range(hidden_units // width):
            dvec_ref[8 + k : 9 + k, :] = accb[0:1, k * width : (k + 1) * width]


def attention_backward(
    length, pitch, count,
    x_ref, gr_ref, ga_ref, q_ref, k_ref, v_ref, probs_ref, wq_ref, vec_ref, strip_ref, dvec_in,
    gx_ref, unit_ref, dvec_ref,
    pad_ref, hid_ref, gp_ref, acc, accv,
):
    phase, block = pl.program_id(0), pl.program_id(1)
    phases, blocks_ = pl.num_programs(0), pl.num_programs(1)
    width = x_ref.shape[2]
    head_dim = width // HEADS
    pair = 2 * head_dim
    factor = head_dim ** (-0.5)
    rows = count * pitch
    here = pl.ds(pl.multiple_of(block * rows, rows), rows)
    gain = vec_ref[0:1, :]
    shift = vec_ref[1:2, :]

    @pl.when(jnp.logical_and(phase == 0, block == 0))
    def _():
        pad_ref[...] = jnp.zeros_like(pad_ref)
        accv[...] = jnp.zeros_like(accv)

    def stats():
        for image in range(count):
            pad_ref[image * pitch : image * pitch + length, :] = x_ref[image]
        return row_stats(pad_ref[...].astype(F32))

    @pl.when(phase == 0)
    def _():
        normed, _ = stats()
        hid_ref[here, :] = (normed * gain + shift).astype(BF)

    @pl.when(phase < phases - 1)
    def _():
        @pl.when(block == 0)
        def _():
            acc[...] = jnp.zeros_like(acc)

        lane = lax.broadcasted_iota(jnp.int32, (pitch, pair), 1)
        sum_q = jnp.zeros((1, pair), F32)
        sum_v = jnp.zeros((1, pair), F32)
        pieces = []
        for image in range(count):
            query = q_ref[image]
            keys = k_ref[image]
            values = v_ref[image]
            grad_out = ga_ref[image]
            keys_t = keys.T
            grad_values = None
            grad_keys = None
            parts = []
            for side in range(2):
                own = (lane < head_dim) if side == 0 else (lane >= head_dim)
                zero = jnp.zeros_like(query)
                grad_side = jnp.where(own, grad_out, zero)
                probs_b = probs_ref[image, side]
                probs = probs_b.astype(F32)
                grad_probs = dot_rt(values, grad_side)
                delta = jnp.sum(probs * grad_probs, axis=0, keepdims=True)
                grad_scores = (probs * (grad_probs - delta)).astype(BF)
                piece_v = dot(probs_b, grad_side)
                piece_k = dot(grad_scores, jnp.where(own, query, zero))
                grad_values = piece_v if grad_values is None else grad_values + piece_v
                grad_keys = piece_k if grad_keys is None else grad_keys + piece_k
                parts.append(dot(keys_t[side * head_dim : (side + 1) * head_dim], grad_scores))
            grad_query = jnp.concatenate(parts, axis=0).T * factor
            grad_keys = grad_keys * factor
            sum_q += col_sum(grad_query)
            sum_v += col_sum(grad_values)
            pieces.append(
                jnp.concatenate([grad_query.astype(BF), grad_keys.astype(BF), grad_values.astype(BF)], axis=1)
            )
        grad_pair = jnp.concatenate(pieces, axis=0)
        gp_ref[phase, here, :] = grad_pair
        accv[phase, 0:1, :] += sum_q
        accv[phase, 1:2, :] += sum_v
        acc[...] += dot_lt(hid_ref[here, :], grad_pair)

        @pl.when(block == blocks_ - 1)
        def _():
            share = width // 2
            for side in range(2):
                for strip in range(3):
                    unit_ref[phase, side, strip * share : (strip + 1) * share, :] = acc[
                        side * share : (side + 1) * share, strip * pair : (strip + 1) * pair
                    ].astype(BF)
                unit_ref[phase, side, 3 * share :, :] = strip_ref[phase, side]

    @pl.when(phase == phases - 1)
    def _():
        @pl.when(block == 0)
        def _():
            dvec_ref[...] = dvec_in[...]
            for two in range(HEADS // 2):
                dvec_ref[4:6, two * pair : (two + 1) * pair] = accv[two, 0:2, :]

        normed, inverse = stats()
        grad_hidden = None
        for two in range(HEADS // 2):
            for third in range(3):
                cols = slice(third * width + two * pair, third * width + (two + 1) * pair)
                piece = (gp_ref[two, here, third * pair : (third + 1) * pair], wq_ref[:, cols])
                grad_hidden = piece if grad_hidden is None else tuple(
                    jnp.concatenate([a, b], axis=1) for a, b in zip(grad_hidden, piece)
                )
        grad_hidden = dot_rt(*grad_hidden)
        dvec_ref[6:7, :] += col_sum(grad_hidden * normed)
        dvec_ref[7:8, :] += col_sum(grad_hidden)
        grad_x = gr_ref[...].reshape(rows, width) + norm_back(grad_hidden, normed, inverse, gain)
        for image in range(count):
            gx_ref[image] = grad_x[image * pitch : image * pitch + length]


class Reduce:
    STAGES = 8

    def __init__(self, source, bufs, out, sends, recvs):
        self.replica, self.group = place()
        self.source, self.out = source, out
        self.r1, self.b1, self.r2, self.b2, self.rx, self.bx, self.rz, self.ez = bufs
        replicas = lax.axis_size("replica")
        self.extra = replicas // 16
        half = out.shape[1] // 2
        self.half, self.quarter, self.piece = half, half // 2, half // 8
        r = self.replica
        self.core = lax.rem(r, 2)
        self.x = lax.rem(r // 2, 2)
        self.z = lax.rem(r // 4, 4)
        self.e = r // 16
        self.sends, self.recvs = sends, recvs
        low = self.core * half
        self.at_core = pl.ds(pl.multiple_of(low, half), half)
        self.at_quarter = pl.ds(pl.multiple_of(low + self.x * self.quarter, self.quarter), self.quarter)
        self.at_piece = pl.ds(
            pl.multiple_of(low + self.x * self.quarter + self.z * self.piece, self.piece), self.piece
        )

    def partners(self):
        return [self.to_core(), self.to_group(), self.to_x()] + [self.to_z(d) for d in (1, 2, 3)] + [
            self.to_e(d) for d in range(1, self.extra)
        ]

    def to_core(self):
        return (self.replica + 1 - 2 * self.core, self.group)

    def to_group(self):
        return (self.replica, 1 - self.group)

    def to_x(self):
        return (self.replica + 2 - 4 * self.x, self.group)

    def z_at(self, hop):
        return lax.rem(self.z + hop, 4)

    def to_z(self, hop):
        return (self.replica + 4 * (self.z_at(hop) - self.z), self.group)

    def to_e(self, hop):
        return (self.replica + 16 * (lax.rem(self.e + hop, self.extra) - self.e), self.group)

    def copy(self, stage, source, target, device, hop=0):
        return remote(source, target, self.sends.at[stage, hop], self.recvs.at[stage, hop], device)

    def copies(self, stage):
        if stage == 0:
            other = pl.ds(pl.multiple_of((1 - self.core) * self.half, self.half), self.half)
            return [self.copy(0, self.source.at[:, :, other], self.r1, self.to_core())]
        if stage == 1:
            return [self.copy(1, self.b1.at[:, 1 - self.group], self.r2, self.to_group())]
        if stage == 2:
            other = pl.ds(pl.multiple_of((1 - self.x) * self.quarter, self.quarter), self.quarter)
            return [self.copy(2, self.b2.at[:, other], self.rx, self.to_x())]
        if stage == 3:
            out = []
            for hop in (1, 2, 3):
                theirs = pl.ds(pl.multiple_of(self.z_at(hop) * self.piece, self.piece), self.piece)
                out.append(self.copy(3, self.bx.at[:, theirs], self.rz.at[hop - 1], self.to_z(hop), hop))
            return out
        if stage == 4:
            return [
                self.copy(4, self.ez.at[self.e], self.ez.at[self.e], self.to_e(hop), hop) for hop in range(1, self.extra)
            ]
        if stage == 5:
            place_ = self.out.at[:, self.at_piece]
            return [self.copy(5, place_, place_, self.to_z(hop), hop) for hop in (1, 2, 3)]
        if stage == 6:
            place_ = self.out.at[:, self.at_quarter]
            return [self.copy(6, place_, place_, self.to_x())]
        place_ = self.out.at[:, self.at_core]
        return [self.copy(7, place_, place_, self.to_core())]

    def start(self, stage):
        for copy in self.copies(stage):
            copy.start()

    def finish(self, stage):
        for copy in self.copies(stage):
            copy.wait()
        if stage == 0:
            self.b1[...] = (self.source[:, :, self.at_core].astype(F32) + self.r1[...].astype(F32)).astype(BF)
        elif stage == 1:
            self.b2[...] = (self.b1[:, self.group].astype(F32) + self.r2[...].astype(F32)).astype(BF)
        elif stage == 2:
            mine = pl.ds(pl.multiple_of(self.x * self.quarter, self.quarter), self.quarter)
            self.bx[...] = (self.b2[:, mine].astype(F32) + self.rx[...].astype(F32)).astype(BF)
        elif stage == 3:
            mine = pl.ds(pl.multiple_of(self.z * self.piece, self.piece), self.piece)
            total = self.bx[:, mine].astype(F32)
            for hop in range(3):
                total = total + self.rz[hop].astype(F32)
            if self.extra > 1:
                self.ez[self.e] = total.astype(BF)
            else:
                self.out[:, self.at_piece] = total.astype(BF)
        elif stage == 4 and self.extra > 1:
            total = self.ez[0].astype(F32)
            for k in range(1, self.extra):
                total = total + self.ez[k].astype(F32)
            self.out[:, self.at_piece] = total.astype(BF)


def reduce_scratch(units, rows, replicas):
    half, extra = rows // 2, max(replicas // 16, 1)
    hops = max(4, extra)
    return [
        pltpu.VMEM((units, 2, half, LANES), BF), pltpu.VMEM((units, 2, half, LANES), BF),
        pltpu.VMEM((units, half, LANES), BF), pltpu.VMEM((units, half, LANES), BF),
        pltpu.VMEM((units, half // 2, LANES), BF), pltpu.VMEM((units, half // 2, LANES), BF),
        pltpu.VMEM((3, units, half // 8, LANES), BF), pltpu.VMEM((extra, units, half // 8, LANES), BF),
        pltpu.SemaphoreType.DMA((Reduce.STAGES, hops)), pltpu.SemaphoreType.DMA((Reduce.STAGES, hops)),
    ]


class ReduceVectors:
    def __init__(self, like, v1, v2, v3, slots_z, slots_e, got, sends, recvs):
        self.like = like
        self.vals, self.slots_z, self.slots_e, self.got, self.sends, self.recvs = (
            (v1, v2, v3), slots_z, slots_e, got, sends, recvs
        )

    def copies(self, stage):
        o = self.like
        if stage < 3:
            device = (o.to_core, o.to_group, o.to_x)[stage]()
            return [remote(self.vals[stage], self.got.at[stage], self.sends.at[stage, 0], self.recvs.at[stage, 0], device)]
        if stage == 3:
            mine = self.slots_z.at[o.z]
            return [
                remote(mine, mine, self.sends.at[3, hop], self.recvs.at[3, hop], o.to_z(hop)) for hop in (1, 2, 3)
            ]
        mine = self.slots_e.at[o.e]
        return [
            remote(mine, mine, self.sends.at[4, hop], self.recvs.at[4, hop], o.to_e(hop)) for hop in range(1, o.extra)
        ]

    def start(self, stage):
        for copy in self.copies(stage):
            copy.start()

    def finish(self, stage, out):
        o = self.like
        for copy in self.copies(stage):
            copy.wait()
        if stage < 2:
            self.vals[stage + 1][...] = self.vals[stage][...] + self.got[stage]
        elif stage == 2:
            self.slots_z[o.z] = self.vals[2][...] + self.got[2]
        elif stage == 3:
            total = self.slots_z[0] + self.slots_z[1] + self.slots_z[2] + self.slots_z[3]
            if o.extra > 1:
                self.slots_e[o.e] = total
            else:
                out[...] = total
        elif o.extra > 1:
            total = self.slots_e[0]
            for k in range(1, o.extra):
                total = total + self.slots_e[k]
            out[...] = total


def vector_scratch(shape, replicas):
    extra = max(replicas // 16, 1)
    hops = max(4, extra)
    return [
        pltpu.VMEM(shape, F32), pltpu.VMEM(shape, F32), pltpu.VMEM(shape, F32),
        pltpu.VMEM((4,) + shape, F32), pltpu.VMEM((extra,) + shape, F32), pltpu.VMEM((3,) + shape, F32),
        pltpu.SemaphoreType.DMA((5, hops)), pltpu.SemaphoreType.DMA((5, hops)),
    ]


REDUCE_REFS = 10


def reduce_all(a_ref, b_ref, vec_ref, a_out, b_out, vec_out, *scratch):
    parts = []
    half = a_ref.shape[0] // 2
    groups = [(a_ref.at[0:half], a_out.at[0:half]), (a_ref.at[half:], a_out.at[half:]), (b_ref, b_out)]
    for k, (source, out) in enumerate(groups):
        refs = scratch[k * REDUCE_REFS : (k + 1) * REDUCE_REFS]
        parts.append(Reduce(source, refs[:8], out, refs[8], refs[9]))
    refs = scratch[3 * REDUCE_REFS :]
    vectors = ReduceVectors(parts[0], *refs)
    refs[0][...] = vec_ref[...]
    greet(parts[0].partners())
    vectors.start(0)
    for part in parts[:1]:
        part.start(0)
    for tick in range(Reduce.STAGES + 2):
        if tick < 2:
            parts[tick + 1].start(0)
        for k in range(3):
            stage = tick - k
            if 0 <= stage < Reduce.STAGES:
                parts[k].finish(stage)
                if stage + 1 < Reduce.STAGES:
                    parts[k].start(stage + 1)
        if tick < 5:
            vectors.finish(tick, vec_out)
            if tick < 4:
                vectors.start(tick + 1)


def unpack(factor, fc_ref, qkv_ref, vec_ref, g1, s1, wq, bq, bv, wp, bp, g2, s2, w1, b1, w2, b2):
    share, width = wp.shape
    group = lax.axis_index("group")
    pair = LANES
    for two in range(qkv_ref.shape[0]):
        for third in range(3):
            wq[:, third * width + two * pair : third * width + (two + 1) * pair] = (
                qkv_ref[two, third * share : (third + 1) * share, :].astype(F32) * factor
            )
        wp[:, two * pair : (two + 1) * pair] = qkv_ref[two, 3 * share :, :].astype(F32) * factor
    strips = w1.shape[1] // LANES
    for strip in range(strips):
        unit, at = strip // QUAD, strip % QUAD * share
        w1[:, strip * LANES : (strip + 1) * LANES] = fc_ref[unit, at : at + share, :].astype(F32) * factor
    for strip in range(w2.shape[0] // LANES):
        unit, at = strip // 2 + strips // QUAD, strip % 2 * width
        w2[strip * LANES : (strip + 1) * LANES, :] = (fc_ref[unit, at : at + width, :].astype(F32) * factor).T
    rows = vec_ref[...] * factor
    mine = jnp.where(group == 0, rows[:, 0:share], rows[:, share:])
    for k, ref in enumerate((bp, g2, s2, b2, bq, bv, g1, s1)):
        ref[...] = mine[k : k + 1, :].reshape(share)
    per = b1.shape[0] // width
    for k in range(per):
        row = jnp.where(group == 0, rows[8 + k : 9 + k, :], rows[8 + per + k : 9 + per + k, :])
        b1[k * width : (k + 1) * width] = row.reshape(width)


def whole(array):
    return pl.BlockSpec(array.shape, lambda *_: (0,) * len(array.shape))


def blocks(count, *rest):
    return pl.BlockSpec((count,) + rest, lambda i: (i,) + (0,) * len(rest))


def fixed(*shape):
    return pl.BlockSpec(shape, lambda *_: (0,) * len(shape))


def params(axes=1, **kw):
    return pltpu.CompilerParams(vmem_limit_bytes=VMEM_LIMIT, dimension_semantics=("arbitrary",) * axes, **kw)


HBM = pl.BlockSpec(memory_space=pl.ANY)
sds = jax.ShapeDtypeStruct


def forward_part(inputs, weights, vectors, pitch, members):
    images, length, width = inputs.shape
    count = 2
    share, wide = vectors[0].shape[0], vectors[-1].shape[0]
    lanes = (share + LANES - 1) // LANES * LANES
    fulls = [(members * w.shape[0], w.shape[1]) for w in weights]
    return pl.pallas_call(
        functools.partial(attention_forward, length, pitch, count, 5),
        grid=(images // count,),
        in_specs=[blocks(count, length, width)] + [HBM] * 4 + [whole(v) for v in vectors],
        out_specs=[
            blocks(count, pitch, 3 * width), blocks(count, HEADS, pitch, pitch), blocks(count, pitch, width),
            HBM, HBM, HBM, HBM, fixed(8, width), fixed(8, members * wide),
        ],
        out_shape=[
            sds((images, pitch, 3 * width), BF), sds((images, HEADS, pitch, pitch), BF), sds((images, pitch, width), BF),
        ] + [sds(full, BF) for full in fulls] + [sds((8, width), F32), sds((8, members * wide), F32)],
        scratch_shapes=[pltpu.VMEM((count * pitch, width), BF)] + [pltpu.VMEM(full, BF) for full in fulls] + [
            pltpu.VMEM((members, 8, lanes), F32), pltpu.VMEM((members, 8, wide), F32),
            pltpu.VMEM((8, width), F32), pltpu.VMEM((8, 3 * width), F32), pltpu.VMEM((8, members * wide), F32),
            pltpu.SemaphoreType.DMA((4,)), pltpu.SemaphoreType.DMA((4,)), pltpu.SemaphoreType.DMA((4,)),
            pltpu.SemaphoreType.DMA((4,)), pltpu.SemaphoreType.DMA((2,)), pltpu.SemaphoreType.DMA((2,)),
            pltpu.SemaphoreType.DMA((4,)), pltpu.SemaphoreType.DMA((4,)),
        ],
        compiler_params=params(collective_id=0, has_side_effects=True),
        name="attention_forward",
    )(inputs, *weights, *vectors)


def middle_part(inputs, cotangent, attended, w_proj, w_fc1, w_fc2, vecs, bias_fc1, pitch):
    images, length, width = inputs.shape
    hidden_units = w_fc1.shape[1]
    count = 2
    rows = count * pitch
    units = 2 * hidden_units // (QUAD * LANES)
    unit_rows = QUAD * width // 2
    unit = (units, 2, unit_rows, LANES)
    strip = (width // LANES, 2, width // 2, LANES)
    return pl.pallas_call(
        functools.partial(mlp_both, length, pitch, count, 256),
        grid=(images // count,),
        in_specs=[blocks(count, length, width), blocks(count, length, width), blocks(count, pitch, width)] + [
            whole(w) for w in (w_proj, w_fc1, w_fc2, vecs, bias_fc1)
        ],
        out_specs=[
            blocks(count, length, width), blocks(count, pitch, width), blocks(count, pitch, width),
            fixed(*unit), fixed(*strip), fixed(16, width),
        ],
        out_shape=[
            sds((images, length, width), BF), sds((images, pitch, width), F32), sds((images, pitch, width), BF),
            sds(unit, BF), sds(strip, BF), sds((16, width), F32),
        ],
        scratch_shapes=[
            pltpu.VMEM((rows, width), BF), pltpu.VMEM((rows, width), BF),
            pltpu.VMEM((rows, hidden_units), BF), pltpu.VMEM((rows, hidden_units), BF),
            pltpu.VMEM((width, hidden_units), F32), pltpu.VMEM((width, hidden_units), F32),
            pltpu.VMEM((width, width), F32), pltpu.VMEM((8, width), F32), pltpu.VMEM((8, hidden_units), F32),
        ],
        compiler_params=params(),
        name="mlp_both",
    )(inputs, cotangent, attended, w_proj, w_fc1, w_fc2, vecs, bias_fc1)


def backward_part(inputs, grad_resid, grad_att, packed, probs, w_qkv, vecs, strips, dvec, pitch):
    images, length, width = inputs.shape
    count = 4
    rows = count * pitch
    steps = images // count
    pairs = HEADS // 2
    pair = width // pairs
    unit = (pairs, 2, QUAD * width // 2, LANES)

    def edge(p, i):
        return jnp.where(jnp.logical_or(p == 0, p == pairs), i, steps - 1)

    def tail(p, i):
        return jnp.where(p == pairs, i, 0)

    def core(p, i):
        return jnp.where(p == pairs, steps - 1, i), jnp.minimum(p, pairs - 1)

    def part(third):
        def index(p, i):
            at, col = core(p, i)
            return at, 0, third * pairs + col

        return pl.BlockSpec((count, pitch, pair), index)

    def probs_at(p, i):
        at, col = core(p, i)
        return at, col, 0, 0

    return pl.pallas_call(
        functools.partial(attention_backward, length, pitch, count),
        grid=(pairs + 1, steps),
        in_specs=[
            pl.BlockSpec((count, length, width), lambda p, i: (edge(p, i), 0, 0)),
            pl.BlockSpec((count, pitch, width), lambda p, i: (tail(p, i), 0, 0)),
            part(0), part(0), part(1), part(2),
            pl.BlockSpec((count, 2, pitch, pitch), probs_at),
            whole(w_qkv), whole(vecs), whole(strips), whole(dvec),
        ],
        out_specs=[
            pl.BlockSpec((count, length, width), lambda p, i: (tail(p, i), 0, 0)), fixed(*unit), fixed(16, width),
        ],
        out_shape=[sds((images, length, width), F32), sds(unit, BF), sds((16, width), F32)],
        scratch_shapes=[
            pltpu.VMEM((rows, width), BF), pltpu.VMEM((images * pitch, width), BF),
            pltpu.VMEM((pairs, images * pitch, 3 * pair), BF), pltpu.VMEM((width, 3 * pair), F32),
            pltpu.VMEM((pairs, 8, pair), F32),
        ],
        compiler_params=params(2),
        name="attention_backward",
    )(inputs, grad_resid, grad_att, packed, packed, packed, probs, w_qkv, vecs, strips, dvec)


def reduce_part(fc_units, qkv_units, dvec, replicas):
    vmem = pl.BlockSpec(memory_space=pltpu.VMEM)
    three, rows = fc_units.shape[0] // 2, fc_units.shape[2]
    scratch = []
    for units in (three, three, qkv_units.shape[0]):
        scratch += reduce_scratch(units, rows, replicas)
    scratch += vector_scratch(dvec.shape, replicas)
    return pl.pallas_call(
        reduce_all,
        in_specs=[vmem] * 3,
        out_specs=[vmem] * 3,
        out_shape=[
            sds((fc_units.shape[0], rows, LANES), BF), sds((qkv_units.shape[0], rows, LANES), BF), sds(dvec.shape, F32),
        ],
        scratch_shapes=scratch,
        compiler_params=pltpu.CompilerParams(vmem_limit_bytes=VMEM_LIMIT, collective_id=1, has_side_effects=True),
        name="reduce_all",
    )(fc_units, qkv_units, dvec)


def local(
    inputs, cotangent, gain_one, shift_one, w_qkv, b_query, b_value, w_proj, b_proj,
    gain_two, shift_two, w_fc1, b_fc1, w_fc2, b_fc2,
):
    images, length, width = inputs.shape
    members = lax.axis_size("group")
    replicas = lax.axis_size("replica")
    pitch = (length + 15) // 16 * 16
    packed, probs, attended, wq, wp, w1, w2, vecs, bias_fc1 = forward_part(
        inputs, (w_qkv, w_proj, w_fc1, w_fc2),
        (gain_one, shift_one, b_query, b_value, b_proj, gain_two, shift_two, b_fc2, b_fc1), pitch, members,
    )
    outputs, grad_resid, grad_att, fc_units, strips, dvec = middle_part(
        inputs, cotangent, attended, wp, w1, w2, vecs, bias_fc1, pitch
    )
    grad_inputs, qkv_units, dvec = backward_part(
        inputs, grad_resid, grad_att, packed, probs, wq, vecs, strips, dvec, pitch
    )
    fc_sum, qkv_sum, vec_sum = reduce_part(fc_units, qkv_units, dvec, replicas)
    factor = float(images * length * replicas * members) ** (-0.5)
    weights = (gain_one, shift_one, w_qkv, b_query, b_value, w_proj, b_proj, gain_two, shift_two, w_fc1, b_fc1, w_fc2, b_fc2)
    grads = pl.pallas_call(
        functools.partial(unpack, factor),
        out_shape=[sds(w.shape, F32) for w in weights],
        compiler_params=pltpu.CompilerParams(vmem_limit_bytes=VMEM_LIMIT),
        name="unpack",
    )(fc_sum, qkv_sum, vec_sum)
    return (outputs, grad_inputs) + tuple(grads)


def solution(mesh):
    images = P(("replica", "group"), None, None)
    line, table = P("group"), P("group", None)
    specs = (line, line, table, line, line, table, line, line, line, table, line, table, line)
    return jax.shard_map(
        local, mesh=mesh, in_specs=(images, images) + specs, out_specs=(images, images) + specs, check_vma=False
    )
```

```python
import functools

import jax
import jax.numpy as jnp
from jax import lax
from jax.experimental import pallas as pl
from jax.experimental.pallas import tpu as pltpu
from jax.sharding import PartitionSpec as P

HEADS = 6
EPS = 1e-06
BF = jnp.bfloat16
F32 = jnp.float32
LOG2E = 1.4426950408889634
VMEM_LIMIT = 60 * 1024 * 1024
MESH = pl.DeviceIdType.MESH
LANES = 128
QUAD = 4


def dot(left, right):
    return jnp.dot(left, right, preferred_element_type=F32)


def dot_lt(left, right):
    return lax.dot_general(left, right, (((0,), (0,)), ((), ())), preferred_element_type=F32)


def dot_rt(left, right):
    return lax.dot_general(left, right, (((1,), (1,)), ((), ())), preferred_element_type=F32)


def row_stats(rows):
    centre = jnp.mean(rows, axis=-1, keepdims=True)
    centered = rows - centre
    inverse = lax.rsqrt(jnp.mean(centered * centered, axis=-1, keepdims=True) + EPS)
    return centered * inverse, inverse


def norm_back(grad_hidden, normed, inverse, gain):
    grad_normed = grad_hidden * gain
    one = jnp.mean(grad_normed, axis=-1, keepdims=True)
    two = jnp.mean(grad_normed * normed, axis=-1, keepdims=True)
    return inverse * (grad_normed - one - normed * two)


def col_sum(rows):
    return jnp.sum(rows, axis=0, keepdims=True)


def place():
    return lax.axis_index("replica"), lax.axis_index("group")


def greet(partners):
    barrier = pltpu.get_barrier_semaphore()
    for partner in partners:
        pl.semaphore_signal(barrier, inc=1, device_id=partner, device_id_type=MESH)
    pl.semaphore_wait(barrier, len(partners))


def remote(source, target, send, recv, device):
    return pltpu.make_async_remote_copy(
        src_ref=source, dst_ref=target, send_sem=send, recv_sem=recv, device_id=device, device_id_type=MESH
    )


class Gather:
    def __init__(self, shards, wholes, sends, recvs, passes, arrivals):
        self.replica, self.group = place()
        core = lax.rem(self.replica, 2)
        self.across = (self.replica, 1 - self.group)
        self.beside = (self.replica + 1 - 2 * core, self.group)
        self.first, self.second = [], []
        for k, (shard, whole_ref) in enumerate(zip(shards, wholes)):
            rows = shard.shape[0]
            half = rows // 2
            mine = pl.ds(pl.multiple_of(core * half, half), half)
            there = pl.ds(pl.multiple_of(self.group * rows + core * half, half), half)
            here = pl.ds(pl.multiple_of((1 - self.group) * rows + core * half, half), half)
            self.first.append(remote(shard.at[mine], whole_ref.at[there], sends.at[k], recvs.at[k], self.across))
            self.second.append(
                remote(whole_ref.at[here], whole_ref.at[here], passes.at[k], arrivals.at[k], self.beside)
            )


def attention_forward(
    length, pitch, count, late,
    x_ref, wq_hbm, wp_hbm, w1_hbm, w2_hbm, g1, s1, bq, bv, bp, g2, s2, b2, b1,
    packed_ref, probs_ref, att_ref, wq_out, wp_out, w1_out, w2_out, vec_out, b1_out,
    pad_ref, wq, wp, w1, w2, small, wide, vec, bias, b1_full,
    sends, recvs, passes, arrivals, vec_send, vec_recv, own_sem, out_sem,
):
    step = pl.program_id(0)
    width = x_ref.shape[2]
    head_dim = width // HEADS
    pair = 2 * head_dim
    factor = head_dim ** (-0.5) * LOG2E
    shards = (wq_hbm, wp_hbm, w1_hbm, w2_hbm)
    wholes = (wq, wp, w1, w2)
    outs = (wq_out, wp_out, w1_out, w2_out)
    move = Gather(shards, wholes, sends, recvs, passes, arrivals)
    group = move.group
    small_copy = remote(small.at[group], small.at[group], vec_send.at[0], vec_recv.at[0], move.across)
    wide_copy = remote(wide.at[group], wide.at[group], vec_send.at[1], vec_recv.at[1], move.across)
    owns = [
        pltpu.make_async_copy(
            shard, full.at[pl.ds(pl.multiple_of(group * shard.shape[0], shard.shape[0]), shard.shape[0])], own_sem.at[k]
        )
        for k, (shard, full) in enumerate(zip(shards, wholes))
    ]
    flush = [pltpu.make_async_copy(full, out, out_sem.at[k]) for k, (full, out) in enumerate(zip(wholes, outs))]
    last = pl.num_programs(0) - 1

    @pl.when(step == 0)
    def _():
        pad_ref[...] = jnp.zeros_like(pad_ref)
        share = g1.shape[0]
        for k, ref in enumerate((g1, s1, bq, bv, bp, g2, s2, b2)):
            small[group, k : k + 1, 0:share] = ref[...].reshape(1, share).astype(F32)
        wide[group, 0:1, :] = b1[...].reshape(1, b1.shape[0]).astype(F32)
        greet((move.across, move.beside))
        small_copy.start()
        for copy in move.first:
            copy.start()
        wide_copy.start()
        for copy in owns:
            copy.start()
        small_copy.wait()
        for side in range(2):
            vec[:, side * share : (side + 1) * share] = small[side, :, 0:share]
        bias[0:1, 0:width] = vec[2:3, :]
        bias[0:1, width : 2 * width] = jnp.zeros((1, width), F32)
        bias[0:1, 2 * width : 3 * width] = vec[3:4, :]
        vec_out[...] = vec[...]
        move.first[0].wait()
        move.second[0].start()
        owns[0].wait()
        move.second[0].wait()

    @pl.when(step == late)
    def _():
        for k in range(1, 4):
            move.first[k].wait()
            move.second[k].start()
        wide_copy.wait()
        for side in range(2):
            b1_full[0:1, side * b1.shape[0] : (side + 1) * b1.shape[0]] = wide[side, 0:1, :]
        b1_out[...] = b1_full[...]
        for k in range(1, 4):
            owns[k].wait()

    @pl.when(step == late + 2)
    def _():
        for k in range(1, 4):
            move.second[k].wait()
        for copy in flush:
            copy.start()

    gain = vec[0:1, :]
    shift = vec[1:2, :]
    for image in range(count):
        pad_ref[image * pitch : image * pitch + length, :] = x_ref[image]
    normed, _ = row_stats(pad_ref[...].astype(F32))
    hidden = (normed * gain + shift).astype(BF)
    packed = (dot(hidden, wq[...]) + bias[0:1, :]).astype(BF)
    for image in range(count):
        packed_ref[image] = packed[image * pitch : (image + 1) * pitch]
    lane = lax.broadcasted_iota(jnp.int32, (pitch, pair), 1)
    tail = length // 8 * 8
    row = lax.broadcasted_iota(jnp.int32, (pitch - tail, pitch), 0) + tail
    for image in range(count):
        for two in range(HEADS // 2):
            cols = slice(two * pair, (two + 1) * pair)
            query = packed_ref[image, :, two * pair : (two + 1) * pair]
            keys = packed_ref[image, :, width + two * pair : width + (two + 1) * pair]
            values = packed_ref[image, :, 2 * width + two * pair : 2 * width + (two + 1) * pair]
            values_t = values.T
            parts = []
            for side in range(2):
                own = (lane < head_dim) if side == 0 else (lane >= head_dim)
                scores = dot_rt(keys, jnp.where(own, query, jnp.zeros_like(query)))
                low = jnp.where(row < length, scores[tail:], -1e30)
                scores = jnp.concatenate([scores[:tail], low], axis=0)
                top = jnp.max(scores, axis=0, keepdims=True)
                raised = jnp.exp2((scores - top) * factor)
                total = jnp.sum(raised, axis=0, keepdims=True)
                probs = (raised * (1.0 / total)).astype(BF)
                probs_ref[image, 2 * two + side] = probs
                parts.append(dot(values_t[side * head_dim : (side + 1) * head_dim], probs))
            mixed = jnp.concatenate(parts, axis=0)
            att_ref[image, :, cols] = mixed.T.astype(BF)

    @pl.when(step == last)
    def _():
        for copy in flush:
            copy.wait()


def gelu_parts(values):
    half = 0.5 * (1.0 + lax.erf(values * 0.7071067811865476))
    slope = half + values * jnp.exp(-0.5 * values * values) * 0.3989422804014327
    return half, slope


def mlp_both(
    length, pitch, count, chunk,
    x_ref, ct_ref, att_ref, wp_ref, w1_ref, w2_ref, vec_ref, b1_ref,
    y_ref, gr_ref, ga_ref, unit_ref, strip_ref, dvec_ref,
    xpad, ctpad, act_ref, gp_ref, acc1, acc2, accp, accv, accb,
):
    step = pl.program_id(0)
    width = x_ref.shape[2]
    hidden_units = w1_ref.shape[1]

    @pl.when(step == 0)
    def _():
        for ref in (xpad, ctpad, acc1, acc2, accp, accv, accb):
            ref[...] = jnp.zeros_like(ref)

    for image in range(count):
        xpad[image * pitch : image * pitch + length, :] = x_ref[image]
        ctpad[image * pitch : image * pitch + length, :] = ct_ref[image]
    bias_p = vec_ref[4:5, :]
    gain = vec_ref[5:6, :]
    shift = vec_ref[6:7, :]
    bias_2 = vec_ref[7:8, :]
    ct = ctpad[...]
    att = att_ref[...].reshape(count * pitch, width)
    resid = xpad[...].astype(F32) + dot(att, wp_ref[...]) + bias_p
    normed, inverse = row_stats(resid)
    hidden = (normed * gain + shift).astype(BF)
    for start in range(0, hidden_units, chunk):
        cols = slice(start, start + chunk)
        pre = dot(hidden, w1_ref[:, cols]) + b1_ref[0:1, cols]
        half, slope = gelu_parts(pre)
        act_ref[:, cols] = (pre * half).astype(BF)
        grad_pre = dot_rt(ct, w2_ref[cols, :]) * slope
        accb[0:1, cols] += col_sum(grad_pre)
        gp_ref[:, cols] = grad_pre.astype(BF)
    out = resid + dot(act_ref[...], w2_ref[...]) + bias_2
    for image in range(count):
        y_ref[image] = out[image * pitch : image * pitch + length].astype(BF)
    grad_hidden = dot_rt(gp_ref[...], w1_ref[...])
    top = ct.astype(F32)
    grad_resid = top + norm_back(grad_hidden, normed, inverse, gain)
    accv[0:1, :] += col_sum(grad_resid)
    accv[1:2, :] += col_sum(grad_hidden * normed)
    accv[2:3, :] += col_sum(grad_hidden)
    accv[3:4, :] += col_sum(top)
    gr_ref[...] = grad_resid.reshape(gr_ref.shape)
    grad_resid_b = grad_resid.astype(BF)
    ga_ref[...] = dot_rt(grad_resid_b, wp_ref[...]).astype(BF).reshape(ga_ref.shape)
    acc1[...] += dot_lt(hidden, gp_ref[...])
    acc2[...] += dot_lt(ct, act_ref[...])
    accp[...] += dot_lt(att, grad_resid_b)

    @pl.when(step == pl.num_programs(0) - 1)
    def _():
        share = width // 2
        wide = hidden_units // 2
        for side in range(2):
            rows = slice(side * share, (side + 1) * share)
            for strip in range(hidden_units // LANES):
                unit, at = strip // QUAD, strip % QUAD * share
                unit_ref[unit, side, at : at + share, :] = acc1[rows, strip * LANES : (strip + 1) * LANES].astype(BF)
            for strip in range(wide // LANES):
                unit, at = strip // 2 + hidden_units // (QUAD * LANES), strip % 2 * width
                start = side * wide + strip * LANES
                unit_ref[unit, side, at : at + width, :] = acc2[:, start : start + LANES].astype(BF)
            for strip in range(width // LANES):
                strip_ref[strip, side] = accp[rows, strip * LANES : (strip + 1) * LANES].astype(BF)
        dvec_ref[...] = jnp.zeros_like(dvec_ref)
        dvec_ref[0:4, :] = accv[0:4, :]
        for k in range(hidden_units // width):
            dvec_ref[8 + k : 9 + k, :] = accb[0:1, k * width : (k + 1) * width]


def phases_of(heads):
    return heads // 2


def schedule(total, steps):
    plan = {}

    def put(at, *work):
        plan.setdefault(at if at < total else -1, []).append(work)

    def chain(name, starts):
        for k, at in enumerate(starts):
            put(at, name, ORDER[k - 1] if k else None, ORDER[k] if k < len(ORDER) else None)

    plan[0] = [("greet", None, None)]
    chain("a", (0, 1, 4, 6, 8, 10, 12, 14))
    chain("b", (0, 3, 7, 9, 11, 13, 15, 16))
    chain(0, (steps, 7, 9, 10, 12, 13, 14, 15))
    chain(1, (2 * steps, 11, 13, 14, 15, 16, 17, 18))
    chain(2, (3 * steps, 16, 17, 18, 19, total, total, total))
    return plan


ORDER = (0, 1, 2, 3, 5, 6, 7)


class Ticks:
    def __init__(self, parts, vectors, vec_out, flushes, vec_flush):
        self.parts, self.vectors, self.vec_out, self.flushes, self.vec_flush = parts, vectors, vec_out, flushes, vec_flush

    def run(self, work):
        for name, done, start in work:
            if name == "greet":
                greet(self.parts["a"].partners())
                continue
            part = self.parts[name]
            if done is not None:
                self.finish(name, part, done)
            if start is not None:
                part.start(start)

    def finish(self, name, part, done):
        part.finish(done)
        if done == 3 and part.extra > 1:
            part.start(4)
            part.finish(4)
        if done == ORDER[-1]:
            self.flushes[name].start()

    def close(self, work):
        vectors, pending = self.vectors, list(work)
        vectors.start(0)
        for stage in range(5):
            if pending:
                self.run([pending.pop(0)])
            vectors.finish(stage, self.vec_out)
            if stage < 4:
                vectors.start(stage + 1)
        self.run(pending)
        self.vec_flush.start()
        for copy in list(self.flushes.values()) + [self.vec_flush]:
            copy.wait()


def make_ticks(fc_ref, unit_ref, dvec_ref, fc_out, qkv_out, vec_out, fc_hbm, qkv_hbm, vec_hbm, flush_sem, scratch):
    three = fc_ref.shape[0] // 2
    pairs = unit_ref.shape[0]
    sources = {"a": (fc_ref, fc_out, fc_hbm, 0, three), "b": (fc_ref, fc_out, fc_hbm, three, three)}
    for k in range(pairs):
        sources[k] = (unit_ref, qkv_out, qkv_hbm, k, 1)
    parts, flushes = {}, {}
    for k, (name, (source, out, hbm, at, size)) in enumerate(sources.items()):
        refs = scratch[k * REDUCE_REFS : (k + 1) * REDUCE_REFS]
        mine = pl.ds(at, size)
        parts[name] = Reduce(source.at[mine], refs[:8], out.at[mine], refs[8], refs[9])
        flushes[name] = pltpu.make_async_copy(out.at[mine], hbm.at[mine], flush_sem.at[k])
    vectors = ReduceVectors(parts["a"], *scratch[len(sources) * REDUCE_REFS :], first=dvec_ref)
    vec_flush = pltpu.make_async_copy(vec_out, vec_hbm, flush_sem.at[len(sources)])
    return Ticks(parts, vectors, vec_out, flushes, vec_flush)


def attention_backward(
    length, pitch, count, steps,
    x_ref, gr_ref, ga_ref, q_ref, k_ref, v_ref, probs_ref, wq_ref, vec_ref, strip_ref, dvec_in, fc_ref,
    gx_ref, fc_hbm, qkv_hbm, vec_hbm,
    pad_ref, hid_ref, gp_ref, acc, accv, unit_ref, dvec_ref, fc_out, qkv_out, vec_out, flush_sem, *scratch,
):
    phase, block = pl.program_id(0), pl.program_id(1)
    phases, blocks_ = pl.num_programs(0), pl.num_programs(1)
    step = phase * blocks_ + block
    ticks = make_ticks(
        fc_ref, unit_ref, dvec_ref, fc_out, qkv_out, vec_out, fc_hbm, qkv_hbm, vec_hbm, flush_sem, scratch
    )
    plan = schedule((phases_of(HEADS) + 1) * steps, steps)
    for at, work in plan.items():
        if at >= 0:
            @pl.when(step == at)
            def _(work=work):
                ticks.run(work)
    width = x_ref.shape[2]
    head_dim = width // HEADS
    pair = 2 * head_dim
    factor = head_dim ** (-0.5)
    rows = count * pitch
    here = pl.ds(pl.multiple_of(block * rows, rows), rows)
    gain = vec_ref[0:1, :]
    shift = vec_ref[1:2, :]

    @pl.when(jnp.logical_and(phase == 0, block == 0))
    def _():
        pad_ref[...] = jnp.zeros_like(pad_ref)
        accv[...] = jnp.zeros_like(accv)

    def stats():
        for image in range(count):
            pad_ref[image * pitch : image * pitch + length, :] = x_ref[image]
        return row_stats(pad_ref[...].astype(F32))

    @pl.when(phase == 0)
    def _():
        normed, _ = stats()
        hid_ref[here, :] = (normed * gain + shift).astype(BF)

    @pl.when(phase < phases - 1)
    def _():
        @pl.when(block == 0)
        def _():
            acc[...] = jnp.zeros_like(acc)

        lane = lax.broadcasted_iota(jnp.int32, (pitch, pair), 1)
        sum_q = jnp.zeros((1, pair), F32)
        sum_v = jnp.zeros((1, pair), F32)
        pieces = []
        for image in range(count):
            query = q_ref[image]
            keys = k_ref[image]
            values = v_ref[image]
            grad_out = ga_ref[image]
            keys_t = keys.T
            grad_values = None
            grad_keys = None
            parts = []
            for side in range(2):
                own = (lane < head_dim) if side == 0 else (lane >= head_dim)
                zero = jnp.zeros_like(query)
                grad_side = jnp.where(own, grad_out, zero)
                probs_b = probs_ref[image, side]
                probs = probs_b.astype(F32)
                grad_probs = dot_rt(values, grad_side)
                delta = jnp.sum(probs * grad_probs, axis=0, keepdims=True)
                grad_scores = (probs * (grad_probs - delta)).astype(BF)
                piece_v = dot(probs_b, grad_side)
                piece_k = dot(grad_scores, jnp.where(own, query, zero))
                grad_values = piece_v if grad_values is None else grad_values + piece_v
                grad_keys = piece_k if grad_keys is None else grad_keys + piece_k
                parts.append(dot(keys_t[side * head_dim : (side + 1) * head_dim], grad_scores))
            grad_query = jnp.concatenate(parts, axis=0).T * factor
            grad_keys = grad_keys * factor
            sum_q += col_sum(grad_query)
            sum_v += col_sum(grad_values)
            pieces.append(
                jnp.concatenate([grad_query.astype(BF), grad_keys.astype(BF), grad_values.astype(BF)], axis=1)
            )
        grad_pair = jnp.concatenate(pieces, axis=0)
        gp_ref[phase, here, :] = grad_pair
        accv[phase, 0:1, :] += sum_q
        accv[phase, 1:2, :] += sum_v
        acc[...] += dot_lt(hid_ref[here, :], grad_pair)

        @pl.when(block == blocks_ - 1)
        def _():
            share = width // 2
            for side in range(2):
                for strip in range(3):
                    unit_ref[phase, side, strip * share : (strip + 1) * share, :] = acc[
                        side * share : (side + 1) * share, strip * pair : (strip + 1) * pair
                    ].astype(BF)
                unit_ref[phase, side, 3 * share :, :] = strip_ref[phase, side]

    @pl.when(phase == phases - 1)
    def _():
        @pl.when(block == 0)
        def _():
            dvec_ref[...] = dvec_in[...]
            for two in range(HEADS // 2):
                dvec_ref[4:6, two * pair : (two + 1) * pair] = accv[two, 0:2, :]

        normed, inverse = stats()
        grad_hidden = None
        for two in range(HEADS // 2):
            for third in range(3):
                cols = slice(third * width + two * pair, third * width + (two + 1) * pair)
                piece = (gp_ref[two, here, third * pair : (third + 1) * pair], wq_ref[:, cols])
                grad_hidden = piece if grad_hidden is None else tuple(
                    jnp.concatenate([a, b], axis=1) for a, b in zip(grad_hidden, piece)
                )
        grad_hidden = dot_rt(*grad_hidden)
        dvec_ref[6:7, :] += col_sum(grad_hidden * normed)
        dvec_ref[7:8, :] += col_sum(grad_hidden)
        grad_x = gr_ref[...].reshape(rows, width) + norm_back(grad_hidden, normed, inverse, gain)
        for image in range(count):
            gx_ref[image] = grad_x[image * pitch : image * pitch + length]

        @pl.when(block == blocks_ - 1)
        def _():
            ticks.close(plan.get(-1, []))


class Reduce:
    STAGES = 8

    def __init__(self, source, bufs, out, sends, recvs):
        self.replica, self.group = place()
        self.source, self.out = source, out
        self.r1, self.b1, self.r2, self.b2, self.rx, self.bx, self.rz, self.ez = bufs
        replicas = lax.axis_size("replica")
        self.extra = replicas // 16
        half = out.shape[1] // 2
        self.half, self.quarter, self.piece = half, half // 2, half // 8
        r = self.replica
        self.core = lax.rem(r, 2)
        self.x = lax.rem(r // 2, 2)
        self.z = lax.rem(r // 4, 4)
        self.e = r // 16
        self.sends, self.recvs = sends, recvs
        low = self.core * half
        self.at_core = pl.ds(pl.multiple_of(low, half), half)
        self.at_quarter = pl.ds(pl.multiple_of(low + self.x * self.quarter, self.quarter), self.quarter)
        self.at_piece = pl.ds(
            pl.multiple_of(low + self.x * self.quarter + self.z * self.piece, self.piece), self.piece
        )

    def partners(self):
        return [self.to_core(), self.to_group(), self.to_x()] + [self.to_z(d) for d in (1, 2, 3)] + [
            self.to_e(d) for d in range(1, self.extra)
        ]

    def to_core(self):
        return (self.replica + 1 - 2 * self.core, self.group)

    def to_group(self):
        return (self.replica, 1 - self.group)

    def to_x(self):
        return (self.replica + 2 - 4 * self.x, self.group)

    def z_at(self, hop):
        return lax.rem(self.z + hop, 4)

    def to_z(self, hop):
        return (self.replica + 4 * (self.z_at(hop) - self.z), self.group)

    def to_e(self, hop):
        return (self.replica + 16 * (lax.rem(self.e + hop, self.extra) - self.e), self.group)

    def copy(self, stage, source, target, device, hop=0):
        return remote(source, target, self.sends.at[stage, hop], self.recvs.at[stage, hop], device)

    def copies(self, stage):
        if stage == 0:
            other = pl.ds(pl.multiple_of((1 - self.core) * self.half, self.half), self.half)
            return [self.copy(0, self.source.at[:, :, other], self.r1, self.to_core())]
        if stage == 1:
            return [self.copy(1, self.b1.at[:, 1 - self.group], self.r2, self.to_group())]
        if stage == 2:
            other = pl.ds(pl.multiple_of((1 - self.x) * self.quarter, self.quarter), self.quarter)
            return [self.copy(2, self.b2.at[:, other], self.rx, self.to_x())]
        if stage == 3:
            out = []
            for hop in (1, 2, 3):
                theirs = pl.ds(pl.multiple_of(self.z_at(hop) * self.piece, self.piece), self.piece)
                out.append(self.copy(3, self.bx.at[:, theirs], self.rz.at[hop - 1], self.to_z(hop), hop))
            return out
        if stage == 4:
            return [
                self.copy(4, self.ez.at[self.e], self.ez.at[self.e], self.to_e(hop), hop) for hop in range(1, self.extra)
            ]
        if stage == 5:
            place_ = self.out.at[:, self.at_piece]
            return [self.copy(5, place_, place_, self.to_z(hop), hop) for hop in (1, 2, 3)]
        if stage == 6:
            place_ = self.out.at[:, self.at_quarter]
            return [self.copy(6, place_, place_, self.to_x())]
        place_ = self.out.at[:, self.at_core]
        return [self.copy(7, place_, place_, self.to_core())]

    def start(self, stage):
        for copy in self.copies(stage):
            copy.start()

    def finish(self, stage):
        for copy in self.copies(stage):
            copy.wait()
        if stage == 0:
            self.b1[...] = (self.source[:, :, self.at_core].astype(F32) + self.r1[...].astype(F32)).astype(BF)
        elif stage == 1:
            self.b2[...] = (self.b1[:, self.group].astype(F32) + self.r2[...].astype(F32)).astype(BF)
        elif stage == 2:
            mine = pl.ds(pl.multiple_of(self.x * self.quarter, self.quarter), self.quarter)
            self.bx[...] = (self.b2[:, mine].astype(F32) + self.rx[...].astype(F32)).astype(BF)
        elif stage == 3:
            mine = pl.ds(pl.multiple_of(self.z * self.piece, self.piece), self.piece)
            total = self.bx[:, mine].astype(F32)
            for hop in range(3):
                total = total + self.rz[hop].astype(F32)
            if self.extra > 1:
                self.ez[self.e] = total.astype(BF)
            else:
                self.out[:, self.at_piece] = total.astype(BF)
        elif stage == 4 and self.extra > 1:
            total = self.ez[0].astype(F32)
            for k in range(1, self.extra):
                total = total + self.ez[k].astype(F32)
            self.out[:, self.at_piece] = total.astype(BF)


def reduce_scratch(units, rows, replicas):
    half, extra = rows // 2, max(replicas // 16, 1)
    hops = max(4, extra)
    return [
        pltpu.VMEM((units, 2, half, LANES), BF), pltpu.VMEM((units, 2, half, LANES), BF),
        pltpu.VMEM((units, half, LANES), BF), pltpu.VMEM((units, half, LANES), BF),
        pltpu.VMEM((units, half // 2, LANES), BF), pltpu.VMEM((units, half // 2, LANES), BF),
        pltpu.VMEM((3, units, half // 8, LANES), BF), pltpu.VMEM((extra, units, half // 8, LANES), BF),
        pltpu.SemaphoreType.DMA((Reduce.STAGES, hops)), pltpu.SemaphoreType.DMA((Reduce.STAGES, hops)),
    ]


class ReduceVectors:
    def __init__(self, like, v2, v3, slots_z, slots_e, got, sends, recvs, first):
        self.like = like
        self.vals, self.slots_z, self.slots_e, self.got, self.sends, self.recvs = (
            (first, v2, v3), slots_z, slots_e, got, sends, recvs
        )

    def copies(self, stage):
        o = self.like
        if stage < 3:
            device = (o.to_core, o.to_group, o.to_x)[stage]()
            return [remote(self.vals[stage], self.got.at[stage], self.sends.at[stage, 0], self.recvs.at[stage, 0], device)]
        if stage == 3:
            mine = self.slots_z.at[o.z]
            return [
                remote(mine, mine, self.sends.at[3, hop], self.recvs.at[3, hop], o.to_z(hop)) for hop in (1, 2, 3)
            ]
        mine = self.slots_e.at[o.e]
        return [
            remote(mine, mine, self.sends.at[4, hop], self.recvs.at[4, hop], o.to_e(hop)) for hop in range(1, o.extra)
        ]

    def start(self, stage):
        for copy in self.copies(stage):
            copy.start()

    def finish(self, stage, out):
        o = self.like
        for copy in self.copies(stage):
            copy.wait()
        if stage < 2:
            self.vals[stage + 1][...] = self.vals[stage][...] + self.got[stage]
        elif stage == 2:
            self.slots_z[o.z] = self.vals[2][...] + self.got[2]
        elif stage == 3:
            total = self.slots_z[0] + self.slots_z[1] + self.slots_z[2] + self.slots_z[3]
            if o.extra > 1:
                self.slots_e[o.e] = total
            else:
                out[...] = total
        elif o.extra > 1:
            total = self.slots_e[0]
            for k in range(1, o.extra):
                total = total + self.slots_e[k]
            out[...] = total


def vector_scratch(shape, replicas):
    extra = max(replicas // 16, 1)
    hops = max(4, extra)
    return [
        pltpu.VMEM(shape, F32), pltpu.VMEM(shape, F32),
        pltpu.VMEM((4,) + shape, F32), pltpu.VMEM((extra,) + shape, F32), pltpu.VMEM((3,) + shape, F32),
        pltpu.SemaphoreType.DMA((5, hops)), pltpu.SemaphoreType.DMA((5, hops)),
    ]


REDUCE_REFS = 10


def unpack(factor, fc_ref, qkv_ref, vec_ref, g1, s1, wq, bq, bv, wp, bp, g2, s2, w1, b1, w2, b2):
    share, width = wp.shape
    group = lax.axis_index("group")
    pair = LANES
    for two in range(qkv_ref.shape[0]):
        for third in range(3):
            wq[:, third * width + two * pair : third * width + (two + 1) * pair] = (
                qkv_ref[two, third * share : (third + 1) * share, :].astype(F32) * factor
            )
        wp[:, two * pair : (two + 1) * pair] = qkv_ref[two, 3 * share :, :].astype(F32) * factor
    strips = w1.shape[1] // LANES
    for strip in range(strips):
        unit, at = strip // QUAD, strip % QUAD * share
        w1[:, strip * LANES : (strip + 1) * LANES] = fc_ref[unit, at : at + share, :].astype(F32) * factor
    for strip in range(w2.shape[0] // LANES):
        unit, at = strip // 2 + strips // QUAD, strip % 2 * width
        w2[strip * LANES : (strip + 1) * LANES, :] = (fc_ref[unit, at : at + width, :].astype(F32) * factor).T
    rows = vec_ref[...] * factor
    mine = jnp.where(group == 0, rows[:, 0:share], rows[:, share:])
    for k, ref in enumerate((bp, g2, s2, b2, bq, bv, g1, s1)):
        ref[...] = mine[k : k + 1, :].reshape(share)
    per = b1.shape[0] // width
    for k in range(per):
        row = jnp.where(group == 0, rows[8 + k : 9 + k, :], rows[8 + per + k : 9 + per + k, :])
        b1[k * width : (k + 1) * width] = row.reshape(width)


def whole(array):
    return pl.BlockSpec(array.shape, lambda *_: (0,) * len(array.shape))


def blocks(count, *rest):
    return pl.BlockSpec((count,) + rest, lambda i: (i,) + (0,) * len(rest))


def fixed(*shape):
    return pl.BlockSpec(shape, lambda *_: (0,) * len(shape))


def params(axes=1, **kw):
    return pltpu.CompilerParams(vmem_limit_bytes=VMEM_LIMIT, dimension_semantics=("arbitrary",) * axes, **kw)


HBM = pl.BlockSpec(memory_space=pl.ANY)
sds = jax.ShapeDtypeStruct


def forward_part(inputs, weights, vectors, pitch, members):
    images, length, width = inputs.shape
    count = 2
    share, wide = vectors[0].shape[0], vectors[-1].shape[0]
    lanes = (share + LANES - 1) // LANES * LANES
    fulls = [(members * w.shape[0], w.shape[1]) for w in weights]
    return pl.pallas_call(
        functools.partial(attention_forward, length, pitch, count, 5),
        grid=(images // count,),
        in_specs=[blocks(count, length, width)] + [HBM] * 4 + [whole(v) for v in vectors],
        out_specs=[
            blocks(count, pitch, 3 * width), blocks(count, HEADS, pitch, pitch), blocks(count, pitch, width),
            HBM, HBM, HBM, HBM, fixed(8, width), fixed(8, members * wide),
        ],
        out_shape=[
            sds((images, pitch, 3 * width), BF), sds((images, HEADS, pitch, pitch), BF), sds((images, pitch, width), BF),
        ] + [sds(full, BF) for full in fulls] + [sds((8, width), F32), sds((8, members * wide), F32)],
        scratch_shapes=[pltpu.VMEM((count * pitch, width), BF)] + [pltpu.VMEM(full, BF) for full in fulls] + [
            pltpu.VMEM((members, 8, lanes), F32), pltpu.VMEM((members, 8, wide), F32),
            pltpu.VMEM((8, width), F32), pltpu.VMEM((8, 3 * width), F32), pltpu.VMEM((8, members * wide), F32),
            pltpu.SemaphoreType.DMA((4,)), pltpu.SemaphoreType.DMA((4,)), pltpu.SemaphoreType.DMA((4,)),
            pltpu.SemaphoreType.DMA((4,)), pltpu.SemaphoreType.DMA((2,)), pltpu.SemaphoreType.DMA((2,)),
            pltpu.SemaphoreType.DMA((4,)), pltpu.SemaphoreType.DMA((4,)),
        ],
        compiler_params=params(collective_id=0, has_side_effects=True),
        name="attention_forward",
    )(inputs, *weights, *vectors)


def middle_part(inputs, cotangent, attended, w_proj, w_fc1, w_fc2, vecs, bias_fc1, pitch):
    images, length, width = inputs.shape
    hidden_units = w_fc1.shape[1]
    count = 2
    rows = count * pitch
    units = 2 * hidden_units // (QUAD * LANES)
    unit_rows = QUAD * width // 2
    unit = (units, 2, unit_rows, LANES)
    strip = (width // LANES, 2, width // 2, LANES)
    return pl.pallas_call(
        functools.partial(mlp_both, length, pitch, count, 256),
        grid=(images // count,),
        in_specs=[blocks(count, length, width), blocks(count, length, width), blocks(count, pitch, width)] + [
            whole(w) for w in (w_proj, w_fc1, w_fc2, vecs, bias_fc1)
        ],
        out_specs=[
            blocks(count, length, width), blocks(count, pitch, width), blocks(count, pitch, width),
            fixed(*unit), fixed(*strip), fixed(16, width),
        ],
        out_shape=[
            sds((images, length, width), BF), sds((images, pitch, width), F32), sds((images, pitch, width), BF),
            sds(unit, BF), sds(strip, BF), sds((16, width), F32),
        ],
        scratch_shapes=[
            pltpu.VMEM((rows, width), BF), pltpu.VMEM((rows, width), BF),
            pltpu.VMEM((rows, hidden_units), BF), pltpu.VMEM((rows, hidden_units), BF),
            pltpu.VMEM((width, hidden_units), F32), pltpu.VMEM((width, hidden_units), F32),
            pltpu.VMEM((width, width), F32), pltpu.VMEM((8, width), F32), pltpu.VMEM((8, hidden_units), F32),
        ],
        compiler_params=params(),
        name="mlp_both",
    )(inputs, cotangent, attended, w_proj, w_fc1, w_fc2, vecs, bias_fc1)


def backward_part(inputs, grad_resid, grad_att, packed, probs, w_qkv, vecs, strips, dvec, fc_units, pitch, replicas):
    images, length, width = inputs.shape
    count = 4
    rows = count * pitch
    steps = images // count
    pairs = HEADS // 2
    pair = width // pairs
    unit_rows = QUAD * width // 2
    unit = (pairs, 2, unit_rows, LANES)
    fc_sum, qkv_sum = (fc_units.shape[0], unit_rows, LANES), (pairs, unit_rows, LANES)
    scratch = []
    for units in (fc_units.shape[0] // 2,) * 2 + (1,) * pairs:
        scratch += reduce_scratch(units, unit_rows, replicas)
    scratch += vector_scratch(dvec.shape, replicas)

    def edge(p, i):
        return jnp.where(jnp.logical_or(p == 0, p == pairs), i, steps - 1)

    def tail(p, i):
        return jnp.where(p == pairs, i, 0)

    def core(p, i):
        return jnp.where(p == pairs, steps - 1, i), jnp.minimum(p, pairs - 1)

    def part(third):
        def index(p, i):
            at, col = core(p, i)
            return at, 0, third * pairs + col

        return pl.BlockSpec((count, pitch, pair), index)

    def probs_at(p, i):
        at, col = core(p, i)
        return at, col, 0, 0

    return pl.pallas_call(
        functools.partial(attention_backward, length, pitch, count, steps),
        grid=(pairs + 1, steps),
        in_specs=[
            pl.BlockSpec((count, length, width), lambda p, i: (edge(p, i), 0, 0)),
            pl.BlockSpec((count, pitch, width), lambda p, i: (tail(p, i), 0, 0)),
            part(0), part(0), part(1), part(2),
            pl.BlockSpec((count, 2, pitch, pitch), probs_at),
            whole(w_qkv), whole(vecs), whole(strips), whole(dvec), whole(fc_units),
        ],
        out_specs=[pl.BlockSpec((count, length, width), lambda p, i: (tail(p, i), 0, 0)), HBM, HBM, HBM],
        out_shape=[sds((images, length, width), F32), sds(fc_sum, BF), sds(qkv_sum, BF), sds(dvec.shape, F32)],
        scratch_shapes=[
            pltpu.VMEM((rows, width), BF), pltpu.VMEM((images * pitch, width), BF),
            pltpu.VMEM((pairs, images * pitch, 3 * pair), BF), pltpu.VMEM((width, 3 * pair), F32),
            pltpu.VMEM((pairs, 8, pair), F32), pltpu.VMEM(unit, BF), pltpu.VMEM(dvec.shape, F32),
            pltpu.VMEM(fc_sum, BF), pltpu.VMEM(qkv_sum, BF), pltpu.VMEM(dvec.shape, F32),
            pltpu.SemaphoreType.DMA((pairs + 3,)),
        ] + scratch,
        compiler_params=params(2, collective_id=1, has_side_effects=True),
        name="attention_backward",
    )(inputs, grad_resid, grad_att, packed, packed, packed, probs, w_qkv, vecs, strips, dvec, fc_units)


def local(
    inputs, cotangent, gain_one, shift_one, w_qkv, b_query, b_value, w_proj, b_proj,
    gain_two, shift_two, w_fc1, b_fc1, w_fc2, b_fc2,
):
    images, length, width = inputs.shape
    members = lax.axis_size("group")
    replicas = lax.axis_size("replica")
    pitch = (length + 15) // 16 * 16
    packed, probs, attended, wq, wp, w1, w2, vecs, bias_fc1 = forward_part(
        inputs, (w_qkv, w_proj, w_fc1, w_fc2),
        (gain_one, shift_one, b_query, b_value, b_proj, gain_two, shift_two, b_fc2, b_fc1), pitch, members,
    )
    outputs, grad_resid, grad_att, fc_units, strips, dvec = middle_part(
        inputs, cotangent, attended, wp, w1, w2, vecs, bias_fc1, pitch
    )
    grad_inputs, fc_sum, qkv_sum, vec_sum = backward_part(
        inputs, grad_resid, grad_att, packed, probs, wq, vecs, strips, dvec, fc_units, pitch, replicas
    )
    factor = float(images * length * replicas * members) ** (-0.5)
    weights = (gain_one, shift_one, w_qkv, b_query, b_value, w_proj, b_proj, gain_two, shift_two, w_fc1, b_fc1, w_fc2, b_fc2)
    grads = pl.pallas_call(
        functools.partial(unpack, factor),
        out_shape=[sds(w.shape, F32) for w in weights],
        compiler_params=pltpu.CompilerParams(vmem_limit_bytes=VMEM_LIMIT),
        name="unpack",
    )(fc_sum, qkv_sum, vec_sum)
    return (outputs, grad_inputs) + tuple(grads)


def solution(mesh):
    images = P(("replica", "group"), None, None)
    line, table = P("group"), P("group", None)
    specs = (line, line, table, line, line, table, line, line, line, table, line, table, line)
    return jax.shard_map(
        local, mesh=mesh, in_specs=(images, images) + specs, out_specs=(images, images) + specs, check_vma=False
    )
```

```python
import functools

import jax
import jax.numpy as jnp
from jax import lax
from jax.experimental import pallas as pl
from jax.experimental.pallas import tpu as pltpu
from jax.sharding import PartitionSpec as P

HEADS = 6
EPS = 1e-06
BF = jnp.bfloat16
F32 = jnp.float32
LOG2E = 1.4426950408889634
VMEM_LIMIT = 60 * 1024 * 1024
MESH = pl.DeviceIdType.MESH
LANES = 128
QUAD = 4


def dot(left, right):
    return jnp.dot(left, right, preferred_element_type=F32)


def dot_lt(left, right):
    return lax.dot_general(left, right, (((0,), (0,)), ((), ())), preferred_element_type=F32)


def dot_rt(left, right):
    return lax.dot_general(left, right, (((1,), (1,)), ((), ())), preferred_element_type=F32)


def row_stats(rows):
    centre = jnp.mean(rows, axis=-1, keepdims=True)
    centered = rows - centre
    inverse = lax.rsqrt(jnp.mean(centered * centered, axis=-1, keepdims=True) + EPS)
    return centered * inverse, inverse


def norm_back(grad_hidden, normed, inverse, gain):
    grad_normed = grad_hidden * gain
    one = jnp.mean(grad_normed, axis=-1, keepdims=True)
    two = jnp.mean(grad_normed * normed, axis=-1, keepdims=True)
    return inverse * (grad_normed - one - normed * two)


def col_sum(rows):
    return jnp.sum(rows, axis=0, keepdims=True)


def place():
    return lax.axis_index("replica"), lax.axis_index("group")


def greet(partners):
    barrier = pltpu.get_barrier_semaphore()
    for partner in partners:
        pl.semaphore_signal(barrier, inc=1, device_id=partner, device_id_type=MESH)
    pl.semaphore_wait(barrier, len(partners))


def remote(source, target, send, recv, device):
    return pltpu.make_async_remote_copy(
        src_ref=source, dst_ref=target, send_sem=send, recv_sem=recv, device_id=device, device_id_type=MESH
    )


class Gather:
    def __init__(self, shards, wholes, sends, recvs, passes, arrivals):
        self.replica, self.group = place()
        core = lax.rem(self.replica, 2)
        self.across = (self.replica, 1 - self.group)
        self.beside = (self.replica + 1 - 2 * core, self.group)
        self.first, self.second = [], []
        for k, (shard, whole_ref) in enumerate(zip(shards, wholes)):
            rows = shard.shape[0]
            half = rows // 2
            mine = pl.ds(pl.multiple_of(core * half, half), half)
            there = pl.ds(pl.multiple_of(self.group * rows + core * half, half), half)
            here = pl.ds(pl.multiple_of((1 - self.group) * rows + core * half, half), half)
            self.first.append(remote(shard.at[mine], whole_ref.at[there], sends.at[k], recvs.at[k], self.across))
            self.second.append(
                remote(whole_ref.at[here], whole_ref.at[here], passes.at[k], arrivals.at[k], self.beside)
            )


def pipeline(items, *stages):
    for tick in range(len(items) + len(stages) - 1):
        for late, stage in enumerate(stages):
            if 0 <= tick - late < len(items):
                stage(items[tick - late])


def attention_forward(
    length, pitch, count, late,
    x_ref, wq_hbm, wp_hbm, w1_hbm, w2_hbm, g1, s1, bq, bv, bp, g2, s2, b2, b1,
    qt_ref, kt_ref, v_ref, exp_ref, inv_ref, att_ref, wq_out, wp_out, w1_out, w2_out, vec_out, b1_out,
    pad_ref, wq, wp, w1, w2, small, wide, vec, b1_full, wqt, bias_q, k_ref,
    sends, recvs, passes, arrivals, vec_send, vec_recv, own_sem, out_sem,
):
    step = pl.program_id(0)
    width = x_ref.shape[2]
    head_dim = width // HEADS
    factor = head_dim ** (-0.5) * LOG2E
    shards = (wq_hbm, wp_hbm, w1_hbm, w2_hbm)
    wholes = (wq, wp, w1, w2)
    outs = (wq_out, wp_out, w1_out, w2_out)
    move = Gather(shards, wholes, sends, recvs, passes, arrivals)
    group = move.group
    small_copy = remote(small.at[group], small.at[group], vec_send.at[0], vec_recv.at[0], move.across)
    wide_copy = remote(wide.at[group], wide.at[group], vec_send.at[1], vec_recv.at[1], move.across)
    owns = [
        pltpu.make_async_copy(
            shard, full.at[pl.ds(pl.multiple_of(group * shard.shape[0], shard.shape[0]), shard.shape[0])], own_sem.at[k]
        )
        for k, (shard, full) in enumerate(zip(shards, wholes))
    ]
    flush = [pltpu.make_async_copy(full, out, out_sem.at[k]) for k, (full, out) in enumerate(zip(wholes, outs))]
    last = pl.num_programs(0) - 1

    @pl.when(step == 0)
    def _():
        pad_ref[...] = jnp.zeros_like(pad_ref)
        share = g1.shape[0]
        for k, ref in enumerate((g1, s1, bq, bv, bp, g2, s2, b2)):
            small[group, k : k + 1, 0:share] = ref[...].reshape(1, share).astype(F32)
        wide[group, 0:1, :] = b1[...].reshape(1, b1.shape[0]).astype(F32)
        greet((move.across, move.beside))
        small_copy.start()
        for copy in move.first:
            copy.start()
        wide_copy.start()
        for copy in owns:
            copy.start()
        small_copy.wait()
        for side in range(2):
            vec[:, side * share : (side + 1) * share] = small[side, :, 0:share]
        vec_out[...] = vec[...]
        bias_q[...] = jnp.broadcast_to(vec[...].T[:, 2:3], bias_q.shape)
        move.first[0].wait()
        move.second[0].start()
        owns[0].wait()
        move.second[0].wait()
        wqt[...] = wq[:, 0:width].T

    @pl.when(step == late)
    def _():
        for k in range(1, 4):
            move.first[k].wait()
            move.second[k].start()
        wide_copy.wait()
        for side in range(2):
            b1_full[0:1, side * b1.shape[0] : (side + 1) * b1.shape[0]] = wide[side, 0:1, :]
        b1_out[...] = b1_full[...]
        for k in range(1, 4):
            owns[k].wait()

    @pl.when(step == late + 1)
    def _():
        for k in range(1, 4):
            move.second[k].wait()
        for copy in flush:
            copy.start()

    gain = vec[0:1, :]
    shift = vec[1:2, :]
    for image in range(count):
        pad_ref[image * pitch : image * pitch + length, :] = x_ref[image]
    normed, _ = row_stats(pad_ref[...].astype(F32))
    hidden = (normed * gain + shift).astype(BF)
    keys_all = dot(hidden, wq[:, width : 2 * width]).astype(BF)
    values_all = (dot(hidden, wq[:, 2 * width :]) + vec[3:4, :]).astype(BF)
    for image in range(count):
        rows = slice(image * pitch, (image + 1) * pitch)
        k_ref[image] = keys_all[rows]
        v_ref[image] = values_all[rows]
        qt_ref[image] = ((dot_rt(wqt[...], hidden[rows]) + bias_q[...]) * factor).astype(BF)
    tail = length // 8 * 8
    row = lax.broadcasted_iota(jnp.int32, (pitch - tail, pitch), 0) + tail
    zero = jnp.zeros((head_dim, pitch), BF)
    ones = jnp.ones((16, pitch), BF)
    kept = {}

    def score(item):
        image, two, side = item
        cols = slice(two * LANES, (two + 1) * LANES)
        if side == 0:
            kt_ref[image, cols, :] = k_ref[image, :, cols].T
            kept["vt", image, two] = v_ref[image, :, cols].T
        at = two * LANES + side * head_dim
        own = qt_ref[image, at : at + head_dim, :]
        full = jnp.concatenate([own, zero] if side == 0 else [zero, own], axis=0)
        kept[item] = dot(k_ref[image, :, cols], full)

    def soften(item):
        image, two, side = item
        scores = kept.pop(item)
        low = jnp.where(row < length, scores[tail:], -1e30)
        scores = jnp.concatenate([scores[:tail], low], axis=0)
        top = jnp.max(scores, axis=0, keepdims=True)
        raised = jnp.exp2(scores - top).astype(BF)
        exp_ref[image, 2 * two + side] = raised
        kept[item] = raised

    def mix(item):
        image, two, side = item
        own = kept["vt", image, two][side * head_dim : (side + 1) * head_dim]
        mixed = dot(jnp.concatenate([own, ones], axis=0), kept.pop(item))
        inverse = 1.0 / mixed[head_dim : head_dim + 1]
        at = two * LANES + side * head_dim
        inv_ref[image, 2 * two + side : 2 * two + side + 1, :] = inverse
        att_ref[image, at : at + head_dim, :] = (mixed[:head_dim] * inverse).astype(BF)

    items = [(image, two, side) for image in range(count) for two in range(HEADS // 2) for side in range(2)]
    pipeline(items, score, soften, mix)

    @pl.when(step == last)
    def _():
        for copy in flush:
            copy.wait()


def gelu_parts(values):
    half = 0.5 * (1.0 + lax.erf(values * 0.7071067811865476))
    slope = half + values * jnp.exp(-0.5 * values * values) * 0.3989422804014327
    return half, slope


def mlp_both(
    length, pitch, count, chunk,
    x_ref, ct_ref, att_ref, wp_ref, w1_ref, w2_ref, vec_ref, b1_ref,
    y_ref, gr_ref, ga_ref, unit_ref, strip_ref, dvec_ref,
    xpad, ctpad, att_s, act_ref, gp_ref, w2t, acc1, acc2, accp, accv, accb,
):
    step = pl.program_id(0)
    width = x_ref.shape[2]
    hidden_units = w1_ref.shape[1]

    @pl.when(step == 0)
    def _():
        for ref in (xpad, ctpad, acc1, acc2, accp, accv, accb):
            ref[...] = jnp.zeros_like(ref)
        w2t[...] = w2_ref[...].T

    for image in range(count):
        att_s[image * pitch : (image + 1) * pitch, :] = att_ref[image].T
        xpad[image * pitch : image * pitch + length, :] = x_ref[image]
        ctpad[image * pitch : image * pitch + length, :] = ct_ref[image]
    bias_p = vec_ref[4:5, :]
    gain = vec_ref[5:6, :]
    shift = vec_ref[6:7, :]
    bias_2 = vec_ref[7:8, :]
    ct = ctpad[...]
    att = att_s[...]
    resid = xpad[...].astype(F32) + dot(att, wp_ref[...]) + bias_p
    normed, inverse = row_stats(resid)
    hidden = (normed * gain + shift).astype(BF)
    for start in range(0, hidden_units, chunk):
        cols = slice(start, start + chunk)
        pre = dot(hidden, w1_ref[:, cols]) + b1_ref[0:1, cols]
        half, slope = gelu_parts(pre)
        act_ref[:, cols] = (pre * half).astype(BF)
        grad_pre = dot_rt(ct, w2_ref[cols, :]) * slope
        accb[0:1, cols] += col_sum(grad_pre)
        gp_ref[:, cols] = grad_pre.astype(BF)
    out = resid + dot_rt(w2t[...], act_ref[...]).T + bias_2
    for image in range(count):
        y_ref[image] = out[image * pitch : image * pitch + length].astype(BF)
    grad_hidden = dot_rt(w1_ref[...], gp_ref[...]).T
    top = ct.astype(F32)
    grad_resid = top + norm_back(grad_hidden, normed, inverse, gain)
    accv[0:1, :] += col_sum(grad_resid)
    accv[1:2, :] += col_sum(grad_hidden * normed)
    accv[2:3, :] += col_sum(grad_hidden)
    accv[3:4, :] += col_sum(top)
    grad_resid_b = grad_resid.astype(BF)
    for image in range(count):
        rows = slice(image * pitch, (image + 1) * pitch)
        gr_ref[image] = grad_resid[rows]
        ga_ref[image] = dot_rt(wp_ref[...], grad_resid_b[rows]).astype(BF)
    acc1[...] += dot_lt(hidden, gp_ref[...])
    acc2[...] += dot_lt(ct, act_ref[...])
    accp[...] += dot_lt(att, grad_resid_b)

    @pl.when(step == pl.num_programs(0) - 1)
    def _():
        share = width // 2
        wide = hidden_units // 2
        for side in range(2):
            rows = slice(side * share, (side + 1) * share)
            for strip in range(hidden_units // LANES):
                unit, at = strip // QUAD, strip % QUAD * share
                unit_ref[unit, side, at : at + share, :] = acc1[rows, strip * LANES : (strip + 1) * LANES].astype(BF)
            for strip in range(wide // LANES):
                unit, at = strip // 2 + hidden_units // (QUAD * LANES), strip % 2 * width
                start = side * wide + strip * LANES
                unit_ref[unit, side, at : at + width, :] = acc2[:, start : start + LANES].astype(BF)
            for strip in range(width // LANES):
                strip_ref[strip, side] = accp[rows, strip * LANES : (strip + 1) * LANES].astype(BF)
        dvec_ref[...] = jnp.zeros_like(dvec_ref)
        dvec_ref[0:4, :] = accv[0:4, :]
        for k in range(hidden_units // width):
            dvec_ref[8 + k : 9 + k, :] = accb[0:1, k * width : (k + 1) * width]


def phases_of(heads):
    return heads // 2


def schedule(total, steps):
    plan = {}

    def put(at, *work):
        plan.setdefault(at if at < total else -1, []).append(work)

    def chain(name, starts):
        for k, at in enumerate(starts):
            put(at, name, ORDER[k - 1] if k else None, ORDER[k] if k < len(ORDER) else None)

    plan[0] = [("greet", None, None)]
    chain("a", (0, 1, 4, 6, 8, 10, 12, 14))
    chain("b", (0, 3, 7, 9, 11, 13, 15, 16))
    chain(0, (steps, 7, 9, 10, 12, 13, 14, 15))
    chain(1, (2 * steps, 11, 13, 14, 15, 16, 17, 18))
    chain(2, (3 * steps, 16, 17, 18, 19, total, total, total))
    return plan


ORDER = (0, 1, 2, 3, 5, 6, 7)


class Ticks:
    def __init__(self, parts, vectors, vec_out, flushes, vec_flush):
        self.parts, self.vectors, self.vec_out, self.flushes, self.vec_flush = parts, vectors, vec_out, flushes, vec_flush

    def run(self, work):
        for name, done, start in work:
            if name == "greet":
                greet(self.parts["a"].partners())
                continue
            part = self.parts[name]
            if done is not None:
                self.finish(name, part, done)
            if start is not None:
                part.start(start)

    def finish(self, name, part, done):
        part.finish(done)
        if done == 3 and part.extra > 1:
            part.start(4)
            part.finish(4)
        if done == ORDER[-1]:
            self.flushes[name].start()

    def close(self, work):
        vectors, pending = self.vectors, list(work)
        vectors.start(0)
        for stage in range(5):
            if pending:
                self.run([pending.pop(0)])
            vectors.finish(stage, self.vec_out)
            if stage < 4:
                vectors.start(stage + 1)
        self.run(pending)
        self.vec_flush.start()
        for copy in list(self.flushes.values()) + [self.vec_flush]:
            copy.wait()


def make_ticks(fc_ref, unit_ref, dvec_ref, fc_out, qkv_out, vec_out, fc_hbm, qkv_hbm, vec_hbm, flush_sem, scratch):
    three = fc_ref.shape[0] // 2
    pairs = unit_ref.shape[0]
    sources = {"a": (fc_ref, fc_out, fc_hbm, 0, three), "b": (fc_ref, fc_out, fc_hbm, three, three)}
    for k in range(pairs):
        sources[k] = (unit_ref, qkv_out, qkv_hbm, k, 1)
    parts, flushes = {}, {}
    for k, (name, (source, out, hbm, at, size)) in enumerate(sources.items()):
        refs = scratch[k * REDUCE_REFS : (k + 1) * REDUCE_REFS]
        mine = pl.ds(at, size)
        parts[name] = Reduce(source.at[mine], refs[:8], out.at[mine], refs[8], refs[9])
        flushes[name] = pltpu.make_async_copy(out.at[mine], hbm.at[mine], flush_sem.at[k])
    vectors = ReduceVectors(parts["a"], *scratch[len(sources) * REDUCE_REFS :], first=dvec_ref)
    vec_flush = pltpu.make_async_copy(vec_out, vec_hbm, flush_sem.at[len(sources)])
    return Ticks(parts, vectors, vec_out, flushes, vec_flush)


def attention_backward(
    length, pitch, count, steps,
    x_ref, gr_ref, ga_ref, qt_ref, kt_ref, v_ref, exp_ref, inv_ref, wq_ref, vec_ref, strip_ref, dvec_in, fc_ref,
    gx_ref, fc_hbm, qkv_hbm, vec_hbm,
    pad_ref, hid_ref, gp_ref, wperm, acc, accv, unit_ref, dvec_ref, fc_out, qkv_out, vec_out, flush_sem, *scratch,
):
    phase, block = pl.program_id(0), pl.program_id(1)
    phases, blocks_ = pl.num_programs(0), pl.num_programs(1)
    step = phase * blocks_ + block
    ticks = make_ticks(
        fc_ref, unit_ref, dvec_ref, fc_out, qkv_out, vec_out, fc_hbm, qkv_hbm, vec_hbm, flush_sem, scratch
    )
    plan = schedule((phases_of(HEADS) + 1) * steps, steps)
    for at, work in plan.items():
        if at >= 0:
            @pl.when(step == at)
            def _(work=work):
                ticks.run(work)
    width = x_ref.shape[2]
    head_dim = width // HEADS
    pair = 2 * head_dim
    factor = head_dim ** (-0.5)
    rows = count * pitch
    first = block * count
    gain = vec_ref[0:1, :]
    shift = vec_ref[1:2, :]

    @pl.when(jnp.logical_and(phase == 0, block == 0))
    def _():
        pad_ref[...] = jnp.zeros_like(pad_ref)
        for two in range(HEADS // 2):
            for third in range(3):
                to, at = (3 * two + third) * pair, third * width + two * pair
                wperm[:, to : to + pair] = wq_ref[:, at : at + pair]

    def stats():
        for image in range(count):
            pad_ref[image * pitch : image * pitch + length, :] = x_ref[image]
        return row_stats(pad_ref[...].astype(F32))

    @pl.when(phase == 0)
    def _():
        normed, _ = stats()
        hidden = (normed * gain + shift).astype(BF)
        for image in range(count):
            hid_ref[first + image, 0:width, :] = hidden[image * pitch : (image + 1) * pitch].T
            hid_ref[first + image, width:, :] = jnp.ones((16, pitch), BF)

    @pl.when(phase < phases - 1)
    def _():
        @pl.when(block == 0)
        def _():
            acc[...] = jnp.zeros_like(acc)

        zero = jnp.zeros((head_dim, pitch), BF)
        kept = {}

        def probe(item):
            image, side = item
            own = slice(side * head_dim, (side + 1) * head_dim)
            inverse = inv_ref[image, pl.ds(2 * phase + side, 1), :]
            grad_out = (ga_ref[image, own, :].astype(F32) * inverse).astype(BF)
            full = jnp.concatenate([grad_out, zero] if side == 0 else [zero, grad_out], axis=0)
            kept[item] = (dot(v_ref[image], full), grad_out, inverse)

        def soften(item):
            image, side = item
            grad_probs, grad_out, inverse = kept[item]
            raised = exp_ref[image, side].astype(F32)
            delta = jnp.sum(raised * grad_probs, axis=0, keepdims=True) * inverse
            kept[item] = ((raised * (grad_probs - delta)).astype(BF), grad_out)

        def spread(item):
            image, side = item
            scores, grad_out = kept.pop(item)
            own = slice(side * head_dim, (side + 1) * head_dim)
            grad_q = dot(kt_ref[image, own, :], scores) * factor
            grad_k = dot_rt(qt_ref[image, own, :], scores) * (1.0 / LOG2E)
            grad_v = dot_rt(grad_out, exp_ref[image, side])
            for third, part in enumerate((grad_q, grad_k, grad_v)):
                at = third * pair + side * head_dim
                gp_ref[phase, first + image, at : at + head_dim, :] = part.astype(BF)

        def gather(item):
            image, side = item
            if side == 1:
                acc[...] += dot_rt(hid_ref[first + image], gp_ref[phase, first + image])

        items = [(image, side) for image in range(count) for side in range(2)]
        pipeline(items, probe, soften, spread, gather)

        @pl.when(block == blocks_ - 1)
        def _():
            share = width // 2
            for side in range(2):
                for strip in range(3):
                    unit_ref[phase, side, strip * share : (strip + 1) * share, :] = acc[
                        side * share : (side + 1) * share, strip * pair : (strip + 1) * pair
                    ].astype(BF)
                unit_ref[phase, side, 3 * share :, :] = strip_ref[phase, side]
            accv[phase] = acc[width : width + 8, :]

    @pl.when(phase == phases - 1)
    def _():
        @pl.when(block == 0)
        def _():
            dvec_ref[...] = dvec_in[...]
            for two in range(HEADS // 2):
                cols = slice(two * pair, (two + 1) * pair)
                dvec_ref[4:5, cols] = accv[two, 0:1, 0:pair]
                dvec_ref[5:6, cols] = accv[two, 0:1, 2 * pair : 3 * pair]

        normed, inverse = stats()
        sum_n = jnp.zeros((1, width), F32)
        sum_h = jnp.zeros((1, width), F32)
        for image in range(count):
            at = slice(image * pitch, (image + 1) * pitch)
            packed = jnp.concatenate([gp_ref[two, first + image] for two in range(HEADS // 2)], axis=0)
            grad_hidden = dot(wperm[...], packed).T
            sum_n += col_sum(grad_hidden * normed[at])
            sum_h += col_sum(grad_hidden)
            grad_x = gr_ref[image] + norm_back(grad_hidden, normed[at], inverse[at], gain)
            gx_ref[image] = grad_x[:length]
        dvec_ref[6:7, :] += sum_n
        dvec_ref[7:8, :] += sum_h

        @pl.when(block == blocks_ - 1)
        def _():
            ticks.close(plan.get(-1, []))


class Reduce:
    STAGES = 8

    def __init__(self, source, bufs, out, sends, recvs):
        self.replica, self.group = place()
        self.source, self.out = source, out
        self.r1, self.b1, self.r2, self.b2, self.rx, self.bx, self.rz, self.ez = bufs
        replicas = lax.axis_size("replica")
        self.extra = replicas // 16
        half = out.shape[1] // 2
        self.half, self.quarter, self.piece = half, half // 2, half // 8
        r = self.replica
        self.core = lax.rem(r, 2)
        self.x = lax.rem(r // 2, 2)
        self.z = lax.rem(r // 4, 4)
        self.e = r // 16
        self.sends, self.recvs = sends, recvs
        low = self.core * half
        self.at_core = pl.ds(pl.multiple_of(low, half), half)
        self.at_quarter = pl.ds(pl.multiple_of(low + self.x * self.quarter, self.quarter), self.quarter)
        self.at_piece = pl.ds(
            pl.multiple_of(low + self.x * self.quarter + self.z * self.piece, self.piece), self.piece
        )

    def partners(self):
        return [self.to_core(), self.to_group(), self.to_x()] + [self.to_z(d) for d in (1, 2, 3)] + [
            self.to_e(d) for d in range(1, self.extra)
        ]

    def to_core(self):
        return (self.replica + 1 - 2 * self.core, self.group)

    def to_group(self):
        return (self.replica, 1 - self.group)

    def to_x(self):
        return (self.replica + 2 - 4 * self.x, self.group)

    def z_at(self, hop):
        return lax.rem(self.z + hop, 4)

    def to_z(self, hop):
        return (self.replica + 4 * (self.z_at(hop) - self.z), self.group)

    def to_e(self, hop):
        return (self.replica + 16 * (lax.rem(self.e + hop, self.extra) - self.e), self.group)

    def copy(self, stage, source, target, device, hop=0):
        return remote(source, target, self.sends.at[stage, hop], self.recvs.at[stage, hop], device)

    def copies(self, stage):
        if stage == 0:
            other = pl.ds(pl.multiple_of((1 - self.core) * self.half, self.half), self.half)
            return [self.copy(0, self.source.at[:, :, other], self.r1, self.to_core())]
        if stage == 1:
            return [self.copy(1, self.b1.at[:, 1 - self.group], self.r2, self.to_group())]
        if stage == 2:
            other = pl.ds(pl.multiple_of((1 - self.x) * self.quarter, self.quarter), self.quarter)
            return [self.copy(2, self.b2.at[:, other], self.rx, self.to_x())]
        if stage == 3:
            out = []
            for hop in (1, 2, 3):
                theirs = pl.ds(pl.multiple_of(self.z_at(hop) * self.piece, self.piece), self.piece)
                out.append(self.copy(3, self.bx.at[:, theirs], self.rz.at[hop - 1], self.to_z(hop), hop))
            return out
        if stage == 4:
            return [
                self.copy(4, self.ez.at[self.e], self.ez.at[self.e], self.to_e(hop), hop) for hop in range(1, self.extra)
            ]
        if stage == 5:
            place_ = self.out.at[:, self.at_piece]
            return [self.copy(5, place_, place_, self.to_z(hop), hop) for hop in (1, 2, 3)]
        if stage == 6:
            place_ = self.out.at[:, self.at_quarter]
            return [self.copy(6, place_, place_, self.to_x())]
        place_ = self.out.at[:, self.at_core]
        return [self.copy(7, place_, place_, self.to_core())]

    def start(self, stage):
        for copy in self.copies(stage):
            copy.start()

    def finish(self, stage):
        for copy in self.copies(stage):
            copy.wait()
        if stage == 0:
            self.b1[...] = (self.source[:, :, self.at_core].astype(F32) + self.r1[...].astype(F32)).astype(BF)
        elif stage == 1:
            self.b2[...] = (self.b1[:, self.group].astype(F32) + self.r2[...].astype(F32)).astype(BF)
        elif stage == 2:
            mine = pl.ds(pl.multiple_of(self.x * self.quarter, self.quarter), self.quarter)
            self.bx[...] = (self.b2[:, mine].astype(F32) + self.rx[...].astype(F32)).astype(BF)
        elif stage == 3:
            mine = pl.ds(pl.multiple_of(self.z * self.piece, self.piece), self.piece)
            total = self.bx[:, mine].astype(F32)
            for hop in range(3):
                total = total + self.rz[hop].astype(F32)
            if self.extra > 1:
                self.ez[self.e] = total.astype(BF)
            else:
                self.out[:, self.at_piece] = total.astype(BF)
        elif stage == 4 and self.extra > 1:
            total = self.ez[0].astype(F32)
            for k in range(1, self.extra):
                total = total + self.ez[k].astype(F32)
            self.out[:, self.at_piece] = total.astype(BF)


def reduce_scratch(units, rows, replicas):
    half, extra = rows // 2, max(replicas // 16, 1)
    hops = max(4, extra)
    return [
        pltpu.VMEM((units, 2, half, LANES), BF), pltpu.VMEM((units, 2, half, LANES), BF),
        pltpu.VMEM((units, half, LANES), BF), pltpu.VMEM((units, half, LANES), BF),
        pltpu.VMEM((units, half // 2, LANES), BF), pltpu.VMEM((units, half // 2, LANES), BF),
        pltpu.VMEM((3, units, half // 8, LANES), BF), pltpu.VMEM((extra, units, half // 8, LANES), BF),
        pltpu.SemaphoreType.DMA((Reduce.STAGES, hops)), pltpu.SemaphoreType.DMA((Reduce.STAGES, hops)),
    ]


class ReduceVectors:
    def __init__(self, like, v2, v3, slots_z, slots_e, got, sends, recvs, first):
        self.like = like
        self.vals, self.slots_z, self.slots_e, self.got, self.sends, self.recvs = (
            (first, v2, v3), slots_z, slots_e, got, sends, recvs
        )

    def copies(self, stage):
        o = self.like
        if stage < 3:
            device = (o.to_core, o.to_group, o.to_x)[stage]()
            return [remote(self.vals[stage], self.got.at[stage], self.sends.at[stage, 0], self.recvs.at[stage, 0], device)]
        if stage == 3:
            mine = self.slots_z.at[o.z]
            return [
                remote(mine, mine, self.sends.at[3, hop], self.recvs.at[3, hop], o.to_z(hop)) for hop in (1, 2, 3)
            ]
        mine = self.slots_e.at[o.e]
        return [
            remote(mine, mine, self.sends.at[4, hop], self.recvs.at[4, hop], o.to_e(hop)) for hop in range(1, o.extra)
        ]

    def start(self, stage):
        for copy in self.copies(stage):
            copy.start()

    def finish(self, stage, out):
        o = self.like
        for copy in self.copies(stage):
            copy.wait()
        if stage < 2:
            self.vals[stage + 1][...] = self.vals[stage][...] + self.got[stage]
        elif stage == 2:
            self.slots_z[o.z] = self.vals[2][...] + self.got[2]
        elif stage == 3:
            total = self.slots_z[0] + self.slots_z[1] + self.slots_z[2] + self.slots_z[3]
            if o.extra > 1:
                self.slots_e[o.e] = total
            else:
                out[...] = total
        elif o.extra > 1:
            total = self.slots_e[0]
            for k in range(1, o.extra):
                total = total + self.slots_e[k]
            out[...] = total


def vector_scratch(shape, replicas):
    extra = max(replicas // 16, 1)
    hops = max(4, extra)
    return [
        pltpu.VMEM(shape, F32), pltpu.VMEM(shape, F32),
        pltpu.VMEM((4,) + shape, F32), pltpu.VMEM((extra,) + shape, F32), pltpu.VMEM((3,) + shape, F32),
        pltpu.SemaphoreType.DMA((5, hops)), pltpu.SemaphoreType.DMA((5, hops)),
    ]


REDUCE_REFS = 10


def unpack(factor, fc_ref, qkv_ref, vec_ref, g1, s1, wq, bq, bv, wp, bp, g2, s2, w1, b1, w2, b2):
    share, width = wp.shape
    group = lax.axis_index("group")
    pair = LANES
    for two in range(qkv_ref.shape[0]):
        for third in range(3):
            wq[:, third * width + two * pair : third * width + (two + 1) * pair] = (
                qkv_ref[two, third * share : (third + 1) * share, :].astype(F32) * factor
            )
        wp[:, two * pair : (two + 1) * pair] = qkv_ref[two, 3 * share :, :].astype(F32) * factor
    strips = w1.shape[1] // LANES
    for strip in range(strips):
        unit, at = strip // QUAD, strip % QUAD * share
        w1[:, strip * LANES : (strip + 1) * LANES] = fc_ref[unit, at : at + share, :].astype(F32) * factor
    for strip in range(w2.shape[0] // LANES):
        unit, at = strip // 2 + strips // QUAD, strip % 2 * width
        w2[strip * LANES : (strip + 1) * LANES, :] = (fc_ref[unit, at : at + width, :].astype(F32) * factor).T
    rows = vec_ref[...] * factor
    mine = jnp.where(group == 0, rows[:, 0:share], rows[:, share:])
    for k, ref in enumerate((bp, g2, s2, b2, bq, bv, g1, s1)):
        ref[...] = mine[k : k + 1, :].reshape(share)
    per = b1.shape[0] // width
    for k in range(per):
        row = jnp.where(group == 0, rows[8 + k : 9 + k, :], rows[8 + per + k : 9 + per + k, :])
        b1[k * width : (k + 1) * width] = row.reshape(width)


def whole(array):
    return pl.BlockSpec(array.shape, lambda *_: (0,) * len(array.shape))


def blocks(count, *rest):
    return pl.BlockSpec((count,) + rest, lambda i: (i,) + (0,) * len(rest))


def fixed(*shape):
    return pl.BlockSpec(shape, lambda *_: (0,) * len(shape))


def params(axes=1, **kw):
    return pltpu.CompilerParams(vmem_limit_bytes=VMEM_LIMIT, dimension_semantics=("arbitrary",) * axes, **kw)


HBM = pl.BlockSpec(memory_space=pl.ANY)
sds = jax.ShapeDtypeStruct


def forward_part(inputs, weights, vectors, pitch, members):
    images, length, width = inputs.shape
    count = 2
    share, wide = vectors[0].shape[0], vectors[-1].shape[0]
    lanes = (share + LANES - 1) // LANES * LANES
    fulls = [(members * w.shape[0], w.shape[1]) for w in weights]
    turned = (images, width, pitch)
    return pl.pallas_call(
        functools.partial(attention_forward, length, pitch, count, 5),
        grid=(images // count,),
        in_specs=[blocks(count, length, width)] + [HBM] * 4 + [whole(v) for v in vectors],
        out_specs=[
            blocks(count, width, pitch), blocks(count, width, pitch), blocks(count, pitch, width),
            blocks(count, HEADS, pitch, pitch), blocks(count, 8, pitch), blocks(count, width, pitch),
            HBM, HBM, HBM, HBM, fixed(8, width), fixed(8, members * wide),
        ],
        out_shape=[
            sds(turned, BF), sds(turned, BF), sds((images, pitch, width), BF),
            sds((images, HEADS, pitch, pitch), BF), sds((images, 8, pitch), F32), sds(turned, BF),
        ] + [sds(full, BF) for full in fulls] + [sds((8, width), F32), sds((8, members * wide), F32)],
        scratch_shapes=[pltpu.VMEM((count * pitch, width), BF)] + [pltpu.VMEM(full, BF) for full in fulls] + [
            pltpu.VMEM((members, 8, lanes), F32), pltpu.VMEM((members, 8, wide), F32),
            pltpu.VMEM((8, width), F32), pltpu.VMEM((8, members * wide), F32),
            pltpu.VMEM((width, width), BF), pltpu.VMEM((width, pitch), F32), pltpu.VMEM((count, pitch, width), BF),
            pltpu.SemaphoreType.DMA((4,)), pltpu.SemaphoreType.DMA((4,)), pltpu.SemaphoreType.DMA((4,)),
            pltpu.SemaphoreType.DMA((4,)), pltpu.SemaphoreType.DMA((2,)), pltpu.SemaphoreType.DMA((2,)),
            pltpu.SemaphoreType.DMA((4,)), pltpu.SemaphoreType.DMA((4,)),
        ],
        compiler_params=params(collective_id=0, has_side_effects=True),
        name="attention_forward",
    )(inputs, *weights, *vectors)


def middle_part(inputs, cotangent, attended, w_proj, w_fc1, w_fc2, vecs, bias_fc1, pitch):
    images, length, width = inputs.shape
    hidden_units = w_fc1.shape[1]
    count = 5
    rows = count * pitch
    units = 2 * hidden_units // (QUAD * LANES)
    unit_rows = QUAD * width // 2
    unit = (units, 2, unit_rows, LANES)
    strip = (width // LANES, 2, width // 2, LANES)
    return pl.pallas_call(
        functools.partial(mlp_both, length, pitch, count, 256),
        grid=(images // count,),
        in_specs=[blocks(count, length, width), blocks(count, length, width), blocks(count, width, pitch)] + [
            whole(w) for w in (w_proj, w_fc1, w_fc2, vecs, bias_fc1)
        ],
        out_specs=[
            blocks(count, length, width), blocks(count, pitch, width), blocks(count, width, pitch),
            fixed(*unit), fixed(*strip), fixed(16, width),
        ],
        out_shape=[
            sds((images, length, width), BF), sds((images, pitch, width), F32), sds((images, width, pitch), BF),
            sds(unit, BF), sds(strip, BF), sds((16, width), F32),
        ],
        scratch_shapes=[
            pltpu.VMEM((rows, width), BF), pltpu.VMEM((rows, width), BF), pltpu.VMEM((rows, width), BF),
            pltpu.VMEM((rows, hidden_units), BF), pltpu.VMEM((rows, hidden_units), BF),
            pltpu.VMEM((width, hidden_units), BF),
            pltpu.VMEM((width, hidden_units), F32), pltpu.VMEM((width, hidden_units), F32),
            pltpu.VMEM((width, width), F32), pltpu.VMEM((8, width), F32), pltpu.VMEM((8, hidden_units), F32),
        ],
        compiler_params=params(),
        name="mlp_both",
    )(inputs, cotangent, attended, w_proj, w_fc1, w_fc2, vecs, bias_fc1)


def backward_part(inputs, grad_resid, grad_att, qt, kt, values, raised, inverse, w_qkv, vecs, strips, dvec, fc_units, pitch, replicas):
    images, length, width = inputs.shape
    count = 4
    rows = count * pitch
    steps = images // count
    pairs = HEADS // 2
    pair = width // pairs
    unit_rows = QUAD * width // 2
    unit = (pairs, 2, unit_rows, LANES)
    fc_sum, qkv_sum = (fc_units.shape[0], unit_rows, LANES), (pairs, unit_rows, LANES)
    scratch = []
    for units in (fc_units.shape[0] // 2,) * 2 + (1,) * pairs:
        scratch += reduce_scratch(units, unit_rows, replicas)
    scratch += vector_scratch(dvec.shape, replicas)

    def edge(p, i):
        return jnp.where(jnp.logical_or(p == 0, p == pairs), i, steps - 1)

    def tail(p, i):
        return jnp.where(p == pairs, i, 0)

    def core(p, i):
        return jnp.where(p == pairs, steps - 1, i), jnp.minimum(p, pairs - 1)

    def turned(p, i):
        at, row = core(p, i)
        return at, row, 0

    def plain(p, i):
        at, col = core(p, i)
        return at, 0, col

    def exp_at(p, i):
        at, col = core(p, i)
        return at, col, 0, 0

    strip = pl.BlockSpec((count, pair, pitch), turned)
    return pl.pallas_call(
        functools.partial(attention_backward, length, pitch, count, steps),
        grid=(pairs + 1, steps),
        in_specs=[
            pl.BlockSpec((count, length, width), lambda p, i: (edge(p, i), 0, 0)),
            pl.BlockSpec((count, pitch, width), lambda p, i: (tail(p, i), 0, 0)),
            strip, strip, strip, pl.BlockSpec((count, pitch, pair), plain),
            pl.BlockSpec((count, 2, pitch, pitch), exp_at),
            pl.BlockSpec((count, 8, pitch), lambda p, i: (core(p, i)[0], 0, 0)),
            whole(w_qkv), whole(vecs), whole(strips), whole(dvec), whole(fc_units),
        ],
        out_specs=[pl.BlockSpec((count, length, width), lambda p, i: (tail(p, i), 0, 0)), HBM, HBM, HBM],
        out_shape=[sds((images, length, width), F32), sds(fc_sum, BF), sds(qkv_sum, BF), sds(dvec.shape, F32)],
        scratch_shapes=[
            pltpu.VMEM((rows, width), BF), pltpu.VMEM((images, width + 16, pitch), BF),
            pltpu.VMEM((pairs, images, 3 * pair, pitch), BF), pltpu.VMEM((width, 3 * width), BF),
            pltpu.VMEM((width + 16, 3 * pair), F32), pltpu.VMEM((pairs, 8, 3 * pair), F32), pltpu.VMEM(unit, BF), pltpu.VMEM(dvec.shape, F32),
            pltpu.VMEM(fc_sum, BF), pltpu.VMEM(qkv_sum, BF), pltpu.VMEM(dvec.shape, F32),
            pltpu.SemaphoreType.DMA((pairs + 3,)),
        ] + scratch,
        compiler_params=params(2, collective_id=1, has_side_effects=True),
        name="attention_backward",
    )(inputs, grad_resid, grad_att, qt, kt, values, raised, inverse, w_qkv, vecs, strips, dvec, fc_units)


def local(
    inputs, cotangent, gain_one, shift_one, w_qkv, b_query, b_value, w_proj, b_proj,
    gain_two, shift_two, w_fc1, b_fc1, w_fc2, b_fc2,
):
    images, length, width = inputs.shape
    members = lax.axis_size("group")
    replicas = lax.axis_size("replica")
    pitch = (length + 7) // 8 * 8
    qt, kt, values, raised, inverse, attended, wq, wp, w1, w2, vecs, bias_fc1 = forward_part(
        inputs, (w_qkv, w_proj, w_fc1, w_fc2),
        (gain_one, shift_one, b_query, b_value, b_proj, gain_two, shift_two, b_fc2, b_fc1), pitch, members,
    )
    outputs, grad_resid, grad_att, fc_units, strips, dvec = middle_part(
        inputs, cotangent, attended, wp, w1, w2, vecs, bias_fc1, pitch
    )
    grad_inputs, fc_sum, qkv_sum, vec_sum = backward_part(
        inputs, grad_resid, grad_att, qt, kt, values, raised, inverse, wq, vecs, strips, dvec, fc_units, pitch, replicas
    )
    factor = float(images * length * replicas * members) ** (-0.5)
    weights = (gain_one, shift_one, w_qkv, b_query, b_value, w_proj, b_proj, gain_two, shift_two, w_fc1, b_fc1, w_fc2, b_fc2)
    grads = pl.pallas_call(
        functools.partial(unpack, factor),
        out_shape=[sds(w.shape, F32) for w in weights],
        compiler_params=pltpu.CompilerParams(vmem_limit_bytes=VMEM_LIMIT),
        name="unpack",
    )(fc_sum, qkv_sum, vec_sum)
    return (outputs, grad_inputs) + tuple(grads)


def solution(mesh):
    images = P(("replica", "group"), None, None)
    line, table = P("group"), P("group", None)
    specs = (line, line, table, line, line, table, line, line, line, table, line, table, line)
    return jax.shard_map(
        local, mesh=mesh, in_specs=(images, images) + specs, out_specs=(images, images) + specs, check_vma=False
    )
```

```python
import functools

import jax
import jax.numpy as jnp
from jax import lax
from jax.experimental import pallas as pl
from jax.experimental.pallas import tpu as pltpu
from jax.sharding import PartitionSpec as P

HEADS = 6
EPS = 1e-06
BF = jnp.bfloat16
F32 = jnp.float32
LOG2E = 1.4426950408889634
VMEM_LIMIT = 60 * 1024 * 1024
MESH = pl.DeviceIdType.MESH
LANES = 128
QUAD = 4


def dot(left, right):
    return jnp.dot(left, right, preferred_element_type=F32)


def dot_lt(left, right):
    return lax.dot_general(left, right, (((0,), (0,)), ((), ())), preferred_element_type=F32)


def dot_rt(left, right):
    return lax.dot_general(left, right, (((1,), (1,)), ((), ())), preferred_element_type=F32)


def row_stats(rows):
    centre = jnp.mean(rows, axis=-1, keepdims=True)
    centered = rows - centre
    inverse = lax.rsqrt(jnp.mean(centered * centered, axis=-1, keepdims=True) + EPS)
    return centered * inverse, inverse


def norm_back(grad_hidden, normed, inverse, gain):
    grad_normed = grad_hidden * gain
    one = jnp.mean(grad_normed, axis=-1, keepdims=True)
    two = jnp.mean(grad_normed * normed, axis=-1, keepdims=True)
    return inverse * (grad_normed - one - normed * two)


def col_sum(rows):
    return jnp.sum(rows, axis=0, keepdims=True)


def place():
    return lax.axis_index("replica"), lax.axis_index("group")


def greet(partners):
    barrier = pltpu.get_barrier_semaphore()
    for partner in partners:
        pl.semaphore_signal(barrier, inc=1, device_id=partner, device_id_type=MESH)
    pl.semaphore_wait(barrier, len(partners))


def remote(source, target, send, recv, device):
    return pltpu.make_async_remote_copy(
        src_ref=source, dst_ref=target, send_sem=send, recv_sem=recv, device_id=device, device_id_type=MESH
    )


class Gather:
    def __init__(self, shards, wholes, sends, recvs, passes, arrivals):
        self.replica, self.group = place()
        core = lax.rem(self.replica, 2)
        self.across = (self.replica, 1 - self.group)
        self.beside = (self.replica + 1 - 2 * core, self.group)
        self.first, self.second = [], []
        for k, (shard, whole_ref) in enumerate(zip(shards, wholes)):
            rows = shard.shape[0]
            half = rows // 2
            mine = pl.ds(pl.multiple_of(core * half, half), half)
            there = pl.ds(pl.multiple_of(self.group * rows + core * half, half), half)
            here = pl.ds(pl.multiple_of((1 - self.group) * rows + core * half, half), half)
            self.first.append(remote(shard.at[mine], whole_ref.at[there], sends.at[k], recvs.at[k], self.across))
            self.second.append(
                remote(whole_ref.at[here], whole_ref.at[here], passes.at[k], arrivals.at[k], self.beside)
            )


def pipeline(items, *stages):
    for tick in range(len(items) + len(stages) - 1):
        for late, stage in enumerate(stages):
            if 0 <= tick - late < len(items):
                stage(items[tick - late])


def attention_forward(
    length, pitch, count, late,
    x_ref, wq_hbm, wp_hbm, w1_hbm, w2_hbm, g1, s1, bq, bv, bp, g2, s2, b2, b1,
    qt_ref, kt_ref, v_ref, exp_ref, inv_ref, att_ref, nt_ref, wq_out, wp_out, w1_out, w2_out, vec_out, b1_out,
    normed_ref, wq, wp, w1, w2, small, wide, vec, b1_full, wqt, bias_q, k_ref,
    sends, recvs, passes, arrivals, vec_send, vec_recv, own_sem, out_sem,
):
    step = pl.program_id(0)
    width = x_ref.shape[2]
    head_dim = width // HEADS
    factor = head_dim ** (-0.5) * LOG2E
    shards = (wq_hbm, wp_hbm, w1_hbm, w2_hbm)
    wholes = (wq, wp, w1, w2)
    outs = (wq_out, wp_out, w1_out, w2_out)
    move = Gather(shards, wholes, sends, recvs, passes, arrivals)
    group = move.group
    small_copy = remote(small.at[group], small.at[group], vec_send.at[0], vec_recv.at[0], move.across)
    wide_copy = remote(wide.at[group], wide.at[group], vec_send.at[1], vec_recv.at[1], move.across)
    owns = [
        pltpu.make_async_copy(
            shard, full.at[pl.ds(pl.multiple_of(group * shard.shape[0], shard.shape[0]), shard.shape[0])], own_sem.at[k]
        )
        for k, (shard, full) in enumerate(zip(shards, wholes))
    ]
    flush = [pltpu.make_async_copy(full, out, out_sem.at[k]) for k, (full, out) in enumerate(zip(wholes, outs))]
    last = pl.num_programs(0) - 1

    @pl.when(step == 0)
    def _():
        share = g1.shape[0]
        for k, ref in enumerate((g1, s1, bq, bv, bp, g2, s2, b2)):
            small[group, k : k + 1, 0:share] = ref[...].reshape(1, share).astype(F32)
        wide[group, 0:1, :] = b1[...].reshape(1, b1.shape[0]).astype(F32)
        greet((move.across, move.beside))
        small_copy.start()
        for copy in move.first:
            copy.start()
        wide_copy.start()
        for copy in owns:
            copy.start()
        tail_ = length // 8 * 8

        @pl.loop(0, x_ref.shape[0])
        def _(image):
            normed_ref[image, tail_:, :] = jnp.zeros((pitch - tail_, width), F32)
            normed_ref[image, 0:length, :] = row_stats(x_ref[image].astype(F32))[0]

        small_copy.wait()
        for side in range(2):
            vec[:, side * share : (side + 1) * share] = small[side, :, 0:share]
        vec_out[...] = vec[...]
        bias_q[...] = jnp.broadcast_to(vec[...].T[:, 2:3], bias_q.shape)
        move.first[0].wait()
        move.second[0].start()
        owns[0].wait()
        move.second[0].wait()
        wqt[...] = wq[:, 0:width].T

    @pl.when(step == late)
    def _():
        for k in range(1, 4):
            move.first[k].wait()
            move.second[k].start()
        wide_copy.wait()
        for side in range(2):
            b1_full[0:1, side * b1.shape[0] : (side + 1) * b1.shape[0]] = wide[side, 0:1, :]
        b1_out[...] = b1_full[...]
        for k in range(1, 4):
            owns[k].wait()

    @pl.when(step == late + 1)
    def _():
        for k in range(1, 4):
            move.second[k].wait()
        for copy in flush:
            copy.start()

    gain = vec[0:1, :]
    shift = vec[1:2, :]
    normed = normed_ref[pl.ds(step * count, count)].reshape(count * pitch, width)
    hidden = (normed * gain + shift).astype(BF)
    keys_all = dot(hidden, wq[:, width : 2 * width]).astype(BF)
    values_all = (dot(hidden, wq[:, 2 * width :]) + vec[3:4, :]).astype(BF)
    for image in range(count):
        rows = slice(image * pitch, (image + 1) * pitch)
        nt_ref[image, 0:width, :] = normed[rows].astype(BF).T
        nt_ref[image, width:, :] = jnp.ones((16, pitch), BF)
        k_ref[image] = keys_all[rows]
        v_ref[image] = values_all[rows]
        qt_ref[image] = ((dot_rt(wqt[...], hidden[rows]) + bias_q[...]) * factor).astype(BF)
    tail = length // 8 * 8
    row = lax.broadcasted_iota(jnp.int32, (pitch - tail, pitch), 0) + tail
    zero = jnp.zeros((head_dim, pitch), BF)
    ones = jnp.ones((16, pitch), BF)
    kept = {}

    def score(item):
        image, two, side = item
        cols = slice(two * LANES, (two + 1) * LANES)
        if side == 0:
            kt_ref[image, cols, :] = k_ref[image, :, cols].T
            kept["vt", image, two] = v_ref[image, :, cols].T
        at = two * LANES + side * head_dim
        own = qt_ref[image, at : at + head_dim, :]
        full = jnp.concatenate([own, zero] if side == 0 else [zero, own], axis=0)
        kept[item] = dot(k_ref[image, :, cols], full)

    def soften(item):
        image, two, side = item
        scores = kept.pop(item)
        low = jnp.where(row < length, scores[tail:], -1e30)
        scores = jnp.concatenate([scores[:tail], low], axis=0)
        top = jnp.max(scores, axis=0, keepdims=True)
        raised = jnp.exp2(scores - top).astype(BF)
        exp_ref[image, 2 * two + side] = raised
        kept[item] = raised

    def mix(item):
        image, two, side = item
        own = kept["vt", image, two][side * head_dim : (side + 1) * head_dim]
        mixed = dot(jnp.concatenate([own, ones], axis=0), kept.pop(item))
        inverse = 1.0 / mixed[head_dim : head_dim + 1]
        at = two * LANES + side * head_dim
        inv_ref[image, 2 * two + side : 2 * two + side + 1, :] = inverse
        att_ref[image, at : at + head_dim, :] = (mixed[:head_dim] * inverse).astype(BF)

    items = [(image, two, side) for image in range(count) for two in range(HEADS // 2) for side in range(2)]
    pipeline(items, score, soften, mix)

    @pl.when(step == last)
    def _():
        for copy in flush:
            copy.wait()


def gelu_parts(values):
    half = 0.5 * (1.0 + lax.erf(values * 0.7071067811865476))
    slope = half + values * jnp.exp(-0.5 * values * values) * 0.3989422804014327
    return half, slope


def mlp_both(
    length, pitch, count, chunk,
    x_ref, ct_ref, att_ref, wp_ref, w1_ref, w2_ref, vec_ref, b1_ref,
    y_ref, gr_ref, ga_ref, unit_ref, strip_ref, dvec_ref,
    xpad, ctpad, att_s, act_ref, gp_ref, w2t, acc1, acc2, accp, accv, accb,
):
    step = pl.program_id(0)
    width = x_ref.shape[2]
    hidden_units = w1_ref.shape[1]

    @pl.when(step == 0)
    def _():
        for ref in (xpad, ctpad, acc1, acc2, accp, accv, accb):
            ref[...] = jnp.zeros_like(ref)
        w2t[...] = w2_ref[...].T

    for image in range(count):
        att_s[image * pitch : (image + 1) * pitch, :] = att_ref[image].T
        xpad[image * pitch : image * pitch + length, :] = x_ref[image]
        ctpad[image * pitch : image * pitch + length, :] = ct_ref[image]
    bias_p = vec_ref[4:5, :]
    gain = vec_ref[5:6, :]
    shift = vec_ref[6:7, :]
    bias_2 = vec_ref[7:8, :]
    ct = ctpad[...]
    att = att_s[...]
    resid = xpad[...].astype(F32) + dot(att, wp_ref[...]) + bias_p
    normed, inverse = row_stats(resid)
    hidden = (normed * gain + shift).astype(BF)
    for start in range(0, hidden_units, chunk):
        cols = slice(start, start + chunk)
        pre = dot(hidden, w1_ref[:, cols]) + b1_ref[0:1, cols]
        half, slope = gelu_parts(pre)
        act_ref[:, cols] = (pre * half).astype(BF)
        grad_pre = dot_rt(ct, w2_ref[cols, :]) * slope
        accb[0:1, cols] += col_sum(grad_pre)
        gp_ref[:, cols] = grad_pre.astype(BF)
    out = resid + dot_rt(w2t[...], act_ref[...]).T + bias_2
    for image in range(count):
        y_ref[image] = out[image * pitch : image * pitch + length].astype(BF)
    grad_hidden = dot_rt(w1_ref[...], gp_ref[...]).T
    top = ct.astype(F32)
    grad_resid = top + norm_back(grad_hidden, normed, inverse, gain)
    accv[0:1, :] += col_sum(grad_resid)
    accv[1:2, :] += col_sum(grad_hidden * normed)
    accv[2:3, :] += col_sum(grad_hidden)
    accv[3:4, :] += col_sum(top)
    grad_resid_b = grad_resid.astype(BF)
    for image in range(count):
        rows = slice(image * pitch, (image + 1) * pitch)
        gr_ref[image] = grad_resid[rows]
        ga_ref[image] = dot_rt(wp_ref[...], grad_resid_b[rows]).astype(BF)
    acc1[...] += dot_lt(hidden, gp_ref[...])
    acc2[...] += dot_lt(ct, act_ref[...])
    accp[...] += dot_lt(att, grad_resid_b)

    @pl.when(step == pl.num_programs(0) - 1)
    def _():
        share = width // 2
        wide = hidden_units // 2
        for side in range(2):
            rows = slice(side * share, (side + 1) * share)
            for strip in range(hidden_units // LANES):
                unit, at = strip // QUAD, strip % QUAD * share
                unit_ref[unit, side, at : at + share, :] = acc1[rows, strip * LANES : (strip + 1) * LANES].astype(BF)
            for strip in range(wide // LANES):
                unit, at = strip // 2 + hidden_units // (QUAD * LANES), strip % 2 * width
                start = side * wide + strip * LANES
                unit_ref[unit, side, at : at + width, :] = acc2[:, start : start + LANES].astype(BF)
            for strip in range(width // LANES):
                strip_ref[strip, side] = accp[rows, strip * LANES : (strip + 1) * LANES].astype(BF)
        dvec_ref[...] = jnp.zeros_like(dvec_ref)
        dvec_ref[0:4, :] = accv[0:4, :]
        for k in range(hidden_units // width):
            dvec_ref[8 + k : 9 + k, :] = accb[0:1, k * width : (k + 1) * width]


CHAINS = {
    "a": (0, 1, 3, 5, 7, 9, 11, 12),
    "b": (0, 1, 3, 5, 7, 9, 11, 12),
    "c": (0, 3, 5, 7, 9, 11, 13, 14),
    0: (4, 5, 8, 10, 12, 13, 14, 15),
    1: (8, 9, 11, 13, 14, 15, 16, 16),
    2: (12, 13, 14, 16, 16, 16),
    "v": (12, 13, 14, 15, 16),
}
SWAPPED = ("b", 0)
SHORT = (2,)


def schedule(total):
    plan = {0: [("greet", None, None)]}
    for name, starts in CHAINS.items():
        order = order_of(name)
        for k, at in enumerate(starts):
            work = (name, order[k - 1] if k else None, order[k] if k < len(order) else None)
            plan.setdefault(at if at < total else -1, []).append(work)
    return plan


def order_of(name):
    if name == "v":
        return (0, 1, 2, 3)
    return (0, 1, 3, 5, 7) if name in SHORT else (0, 1, 2, 3, 5, 6, 7)


class Ticks:
    def __init__(self, parts, flushes):
        self.parts, self.flushes = parts, flushes

    def run(self, work):
        for name, done, start in work:
            if name == "greet":
                greet(self.parts["a"].partners())
                continue
            part = self.parts[name]
            if done is not None:
                part.finish(done)
                if done == 3 and part.extra > 1:
                    part.start(4)
                    part.finish(4)
                if done == order_of(name)[-1]:
                    self.flushes[name].start()
            if start is not None:
                part.start(start)

    def close(self, work):
        pending = list(work)
        while pending:
            names, later = set(), []
            for item in pending:
                if item[0] in names:
                    later.append(item)
                else:
                    names.add(item[0])
                    self.run([item])
            pending = later
        for copy in self.flushes.values():
            copy.wait()


def make_ticks(fc_ref, unit_ref, dvec_ref, fc_out, qkv_out, vec_out, fc_hbm, qkv_hbm, vec_hbm, flush_sem, scratch):
    third = fc_ref.shape[0] // 3
    pairs = unit_ref.shape[0]
    sources = {name: (fc_ref, fc_out, fc_hbm, k * third, third) for k, name in enumerate("abc")}
    for k in range(pairs):
        sources[k] = (unit_ref, qkv_out, qkv_hbm, k, 1)
    parts, flushes = {}, {}
    for k, (name, (source, out, hbm, at, size)) in enumerate(sources.items()):
        refs = scratch[k * REDUCE_REFS : (k + 1) * REDUCE_REFS]
        mine = pl.ds(at, size)
        parts[name] = Reduce(source.at[mine], refs[:8], out.at[mine], refs[8], refs[9], name)
        flushes[name] = pltpu.make_async_copy(out.at[mine], hbm.at[mine], flush_sem.at[k])
    parts["v"] = ReduceVectors(parts["a"], *scratch[len(sources) * REDUCE_REFS :], first=dvec_ref, out=vec_out)
    flushes["v"] = pltpu.make_async_copy(vec_out, vec_hbm, flush_sem.at[len(sources)])
    return Ticks(parts, flushes)


def attention_backward(
    length, pitch, count, steps,
    x_ref, gr_ref, ga_ref, qt_ref, kt_ref, v_ref, exp_ref, inv_ref, nt_ref, wq_ref, vec_ref, strip_ref, dvec_in, fc_ref,
    gx_ref, fc_hbm, qkv_hbm, vec_hbm,
    pad_ref, gp_ref, wperm, acc, accv, unit_ref, dvec_ref, fc_out, qkv_out, vec_out, flush_sem, *scratch,
):
    phase, block = pl.program_id(0), pl.program_id(1)
    phases, blocks_ = pl.num_programs(0), pl.num_programs(1)
    step = phase * blocks_ + block
    ticks = make_ticks(
        fc_ref, unit_ref, dvec_ref, fc_out, qkv_out, vec_out, fc_hbm, qkv_hbm, vec_hbm, flush_sem, scratch
    )
    plan = schedule((HEADS // 2 + 1) * steps)
    for at, work in plan.items():
        if at >= 0:
            @pl.when(step == at)
            def _(work=work):
                ticks.run(work)
    width = x_ref.shape[2]
    head_dim = width // HEADS
    pair = 2 * head_dim
    factor = head_dim ** (-0.5)
    rows = count * pitch
    first = block * count
    gain = vec_ref[0:1, :]

    @pl.when(jnp.logical_and(phase == 0, block == 0))
    def _():
        pad_ref[...] = jnp.zeros_like(pad_ref)
        for two in range(HEADS // 2):
            for third in range(3):
                to, at = (3 * two + third) * pair, third * width + two * pair
                wperm[:, to : to + pair] = wq_ref[:, at : at + pair]

    def stats():
        for image in range(count):
            pad_ref[image * pitch : image * pitch + length, :] = x_ref[image]
        return row_stats(pad_ref[...].astype(F32))

    @pl.when(phase < phases - 1)
    def _():
        @pl.when(block == 0)
        def _():
            acc[...] = jnp.zeros_like(acc)

        zero = jnp.zeros((head_dim, pitch), BF)
        kept = {}

        def probe(item):
            image, side = item
            own = slice(side * head_dim, (side + 1) * head_dim)
            inverse = inv_ref[image, pl.ds(2 * phase + side, 1), :]
            grad_out = (ga_ref[image, own, :].astype(F32) * inverse).astype(BF)
            full = jnp.concatenate([grad_out, zero] if side == 0 else [zero, grad_out], axis=0)
            kept[item] = (dot(v_ref[image], full), grad_out, inverse)

        def soften(item):
            image, side = item
            grad_probs, grad_out, inverse = kept[item]
            raised = exp_ref[image, side].astype(F32)
            delta = jnp.sum(raised * grad_probs, axis=0, keepdims=True) * inverse
            kept[item] = ((raised * (grad_probs - delta)).astype(BF), grad_out)

        def spread(item):
            image, side = item
            scores, grad_out = kept.pop(item)
            own = slice(side * head_dim, (side + 1) * head_dim)
            grad_q = dot(kt_ref[image, own, :], scores) * factor
            grad_k = dot_rt(qt_ref[image, own, :], scores) * (1.0 / LOG2E)
            grad_v = dot_rt(grad_out, exp_ref[image, side])
            for third, part in enumerate((grad_q, grad_k, grad_v)):
                at = third * pair + side * head_dim
                gp_ref[phase, first + image, at : at + head_dim, :] = part.astype(BF)

        def gather(item):
            image, side = item
            if side == 1:
                acc[...] += dot_rt(nt_ref[image], gp_ref[phase, first + image])

        items = [(image, side) for image in range(count) for side in range(2)]
        pipeline(items, probe, soften, spread, gather)

        @pl.when(block == blocks_ - 1)
        def _():
            share = width // 2
            for side in range(2):
                for strip in range(3):
                    unit_ref[phase, side, strip * share : (strip + 1) * share, :] = acc[
                        side * share : (side + 1) * share, strip * pair : (strip + 1) * pair
                    ].astype(BF)
                unit_ref[phase, side, 3 * share :, :] = strip_ref[phase, side]
            accv[phase] = acc[width : width + 8, :]

            @pl.when(phase == phases - 2)
            def _():
                dvec_ref[...] = dvec_in[...]
                for two in range(HEADS // 2):
                    for third in range(3):
                        dvec_ref[4 + third : 5 + third, two * pair : (two + 1) * pair] = accv[
                            two, 0:1, third * pair : (third + 1) * pair
                        ]

    @pl.when(phase == phases - 1)
    def _():
        normed, inverse = stats()
        for image in range(count):
            at = slice(image * pitch, (image + 1) * pitch)
            packed = jnp.concatenate([gp_ref[two, first + image] for two in range(HEADS // 2)], axis=0)
            grad_hidden = dot(wperm[...], packed).T
            grad_x = gr_ref[image] + norm_back(grad_hidden, normed[at], inverse[at], gain)
            gx_ref[image] = grad_x[:length].astype(BF)

        @pl.when(block == blocks_ - 1)
        def _():
            ticks.close(plan.get(-1, []))


SLOTS = {False: (0, 1, 2, 3, 11, 6, 9, 10), True: (0, 1, 0, 2, 17, 9, 0, 16)}


class Reduce:
    def __init__(self, source, bufs, out, sends, recvs, name):
        self.replica, self.group = place()
        self.swapped, self.short = name in SWAPPED, name in SHORT
        self.source, self.out = source, out
        self.r1, self.b1, self.r2, self.b2, self.rx, self.bx, self.rz, self.ez = bufs
        replicas = lax.axis_size("replica")
        self.extra = replicas // 16
        half = out.shape[1] // 2
        self.half, self.quarter, self.piece = half, half // 2, half // 8
        r = self.replica
        self.core = lax.rem(r, 2)
        self.x = lax.rem(r // 2, 2)
        self.z = lax.rem(r // 4, 4)
        self.e = r // 16
        self.m = lax.rem(r // 2, 8)
        self.sends, self.recvs = sends, recvs
        low = self.core * half
        self.at_core = pl.ds(pl.multiple_of(low, half), half)
        self.at_quarter = pl.ds(pl.multiple_of(low + self.x * self.quarter, self.quarter), self.quarter)
        self.at_piece = pl.ds(
            pl.multiple_of(low + self.x * self.quarter + self.z * self.piece, self.piece), self.piece
        )

    def partners(self):
        return [self.to_core(), self.to_group()] + [self.to_m(d) for d in range(1, 8)] + [
            self.to_e(d) for d in range(1, self.extra)
        ]

    def to_core(self):
        return (self.replica + 1 - 2 * self.core, self.group)

    def to_group(self):
        return (self.replica, 1 - self.group)

    def to_x(self):
        return (self.replica + 2 - 4 * self.x, self.group)

    def z_at(self, hop):
        return lax.rem(self.z + hop, 4)

    def to_z(self, hop):
        return (self.replica + 4 * (self.z_at(hop) - self.z), self.group)

    def m_at(self, hop):
        return lax.rem(self.m + hop, 8)

    def to_m(self, hop):
        return (self.replica + 2 * (self.m_at(hop) - self.m), self.group)

    def row_of(self, m):
        start = lax.rem(m, 2) * self.quarter + m // 2 * self.piece
        return pl.ds(pl.multiple_of(start, self.piece), self.piece)

    def to_e(self, hop):
        return (self.replica + 16 * (lax.rem(self.e + hop, self.extra) - self.e), self.group)

    def copy(self, stage, source, target, device, hop=0):
        at = SLOTS[self.short][stage] + hop - (stage in (3, 5)) - (stage == 4)
        return remote(source, target, self.sends.at[at], self.recvs.at[at], device)

    def copies(self, stage):
        if stage == 0:
            other = pl.ds(pl.multiple_of((1 - self.core) * self.half, self.half), self.half)
            return [self.copy(0, self.source.at[:, :, other], self.r1, self.to_core())]
        if stage == 1 and self.swapped:
            other = pl.ds(pl.multiple_of((1 - self.x) * self.quarter, self.quarter), self.quarter)
            return [self.copy(1, self.b1.at[:, :, other], self.r2, self.to_x())]
        if stage == 2 and self.swapped:
            return [self.copy(2, self.b2.at[:, 1 - self.group], self.rx, self.to_group())]
        if stage == 1:
            return [self.copy(1, self.b1.at[:, 1 - self.group], self.r2, self.to_group())]
        if stage == 2:
            other = pl.ds(pl.multiple_of((1 - self.x) * self.quarter, self.quarter), self.quarter)
            return [self.copy(2, self.b2.at[:, other], self.rx, self.to_x())]
        if stage == 3 and self.short:
            return [
                self.copy(3, self.b2.at[:, self.row_of(self.m_at(hop))], self.rz.at[hop - 1], self.to_m(hop), hop)
                for hop in range(1, 8)
            ]
        if stage == 5 and self.short:
            place_ = self.out.at[:, self.at_piece]
            return [self.copy(5, place_, place_, self.to_m(hop), hop) for hop in range(1, 8)]
        if stage == 3:
            out = []
            for hop in (1, 2, 3):
                theirs = pl.ds(pl.multiple_of(self.z_at(hop) * self.piece, self.piece), self.piece)
                out.append(self.copy(3, self.bx.at[:, theirs], self.rz.at[hop - 1], self.to_z(hop), hop))
            return out
        if stage == 4:
            return [
                self.copy(4, self.ez.at[self.e], self.ez.at[self.e], self.to_e(hop), hop) for hop in range(1, self.extra)
            ]
        if stage == 5:
            place_ = self.out.at[:, self.at_piece]
            return [self.copy(5, place_, place_, self.to_z(hop), hop) for hop in (1, 2, 3)]
        if stage == 6:
            place_ = self.out.at[:, self.at_quarter]
            return [self.copy(6, place_, place_, self.to_x())]
        place_ = self.out.at[:, self.at_core]
        return [self.copy(7, place_, place_, self.to_core())]

    def start(self, stage):
        for copy in self.copies(stage):
            copy.start()

    def finish(self, stage):
        for copy in self.copies(stage):
            copy.wait()
        if stage == 0:
            self.b1[...] = self.source[:, :, self.at_core] + self.r1[...]
        elif stage == 1 and self.swapped:
            mine = pl.ds(pl.multiple_of(self.x * self.quarter, self.quarter), self.quarter)
            self.b2[...] = self.b1[:, :, mine] + self.r2[...]
        elif stage == 2 and self.swapped:
            self.bx[...] = self.b2[:, self.group] + self.rx[...]
        elif stage == 1:
            self.b2[...] = self.b1[:, self.group] + self.r2[...]
        elif stage == 2:
            mine = pl.ds(pl.multiple_of(self.x * self.quarter, self.quarter), self.quarter)
            self.bx[...] = self.b2[:, mine] + self.rx[...]
        elif stage == 3:
            mine = pl.ds(pl.multiple_of(self.z * self.piece, self.piece), self.piece)
            own = self.b2.at[:, self.row_of(self.m)] if self.short else self.bx.at[:, mine]
            total = own[...].astype(F32)
            for hop in range(self.rz.shape[0]):
                total = total + self.rz[hop].astype(F32)
            if self.extra > 1:
                self.ez[self.e] = total.astype(BF)
            else:
                self.out[:, self.at_piece] = total.astype(BF)
        elif stage == 4 and self.extra > 1:
            total = self.ez[0].astype(F32)
            for k in range(1, self.extra):
                total = total + self.ez[k].astype(F32)
            self.out[:, self.at_piece] = total.astype(BF)


def reduce_scratch(units, rows, replicas, name):
    half, extra = rows // 2, max(replicas // 16, 1)
    sems = SLOTS[name in SHORT][4] + extra - 1
    second = (units, 2, half // 2, LANES) if name in SWAPPED else (units, half, LANES)
    return [
        pltpu.VMEM((units, 2, half, LANES), BF), pltpu.VMEM((units, 2, half, LANES), BF),
        pltpu.VMEM(second, BF), pltpu.VMEM(second, BF),
        pltpu.VMEM((units, half // 2, LANES), BF), pltpu.VMEM((units, half // 2, LANES), BF),
        pltpu.VMEM((7 if name in SHORT else 3, units, half // 8, LANES), BF), pltpu.VMEM((extra, units, half // 8, LANES), BF),
        pltpu.SemaphoreType.DMA((sems,)), pltpu.SemaphoreType.DMA((sems,)),
    ]


class ReduceVectors:
    def __init__(self, like, v2, v3, slots_z, slots_e, got, sends, recvs, first, out):
        self.like, self.out, self.extra = like, out, like.extra
        self.vals, self.slots_z, self.slots_e, self.got, self.sends, self.recvs = (
            (first, v2, v3), slots_z, slots_e, got, sends, recvs
        )

    def copies(self, stage):
        o = self.like
        if stage < 3:
            device = (o.to_core, o.to_group, o.to_x)[stage]()
            return [remote(self.vals[stage], self.got.at[stage], self.sends.at[stage], self.recvs.at[stage], device)]
        if stage == 3:
            mine = self.slots_z.at[o.z]
            return [
                remote(mine, mine, self.sends.at[2 + hop], self.recvs.at[2 + hop], o.to_z(hop)) for hop in (1, 2, 3)
            ]
        mine = self.slots_e.at[o.e]
        return [
            remote(mine, mine, self.sends.at[5 + hop], self.recvs.at[5 + hop], o.to_e(hop)) for hop in range(1, o.extra)
        ]

    def start(self, stage):
        for copy in self.copies(stage):
            copy.start()

    def finish(self, stage):
        o, out = self.like, self.out
        for copy in self.copies(stage):
            copy.wait()
        if stage < 2:
            self.vals[stage + 1][...] = self.vals[stage][...] + self.got[stage]
        elif stage == 2:
            self.slots_z[o.z] = self.vals[2][...] + self.got[2]
        elif stage == 3:
            total = self.slots_z[0] + self.slots_z[1] + self.slots_z[2] + self.slots_z[3]
            if o.extra > 1:
                self.slots_e[o.e] = total
            else:
                out[...] = total
        elif o.extra > 1:
            total = self.slots_e[0]
            for k in range(1, o.extra):
                total = total + self.slots_e[k]
            out[...] = total


def vector_scratch(shape, replicas):
    extra = max(replicas // 16, 1)
    return [
        pltpu.VMEM(shape, F32), pltpu.VMEM(shape, F32),
        pltpu.VMEM((4,) + shape, F32), pltpu.VMEM((extra,) + shape, F32), pltpu.VMEM((3,) + shape, F32),
        pltpu.SemaphoreType.DMA((5 + extra,)), pltpu.SemaphoreType.DMA((5 + extra,)),
    ]


REDUCE_REFS = 10


def unpack(factor, gx_in, fc_ref, qkv_ref, vec_ref, w_ref, gain_ref, shift_ref, gx_out, g1, s1, wq, bq, bv, wp, bp, g2, s2, w1, b1, w2, b2):
    gx_out[...] = gx_in[...].astype(F32)

    @pl.when(pl.program_id(0) == 0)
    def _():
        share, width = wp.shape
        group = lax.axis_index("group")
        pair = LANES
        column = [
            jnp.broadcast_to(ref[...].reshape(1, share).astype(F32), (8, share)).T[:, 0:1] for ref in (gain_ref, shift_ref)
        ]
        sum_g = jnp.zeros((share, pair), F32)
        sum_s = jnp.zeros((share, pair), F32)
        for two in range(qkv_ref.shape[0]):
            for third in range(3):
                cols = slice(third * width + two * pair, third * width + (two + 1) * pair)
                cross = qkv_ref[two, third * share : (third + 1) * share, :].astype(F32)
                total = vec_ref[4 + third : 5 + third, two * pair : (two + 1) * pair]
                weight = w_ref[:, cols].astype(F32)
                sum_g += weight * cross
                sum_s += weight * total
                wq[:, cols] = (column[0] * cross + column[1] * total) * factor
            wp[:, two * pair : (two + 1) * pair] = qkv_ref[two, 3 * share :, :].astype(F32) * factor
        for ref, total in ((g1, sum_g), (s1, sum_s)):
            ref[...] = (col_sum(total.T) * factor).reshape(share)
        strips = w1.shape[1] // LANES
        for strip in range(strips):
            unit, at = strip // QUAD, strip % QUAD * share
            w1[:, strip * LANES : (strip + 1) * LANES] = fc_ref[unit, at : at + share, :].astype(F32) * factor
        for strip in range(w2.shape[0] // LANES):
            unit, at = strip // 2 + strips // QUAD, strip % 2 * width
            w2[strip * LANES : (strip + 1) * LANES, :] = (fc_ref[unit, at : at + width, :].astype(F32) * factor).T
        rows = vec_ref[...] * factor
        mine = jnp.where(group == 0, rows[:, 0:share], rows[:, share:])
        for k, ref in enumerate((bp, g2, s2, b2, bq, None, bv)):
            if ref is not None:
                ref[...] = mine[k : k + 1, :].reshape(share)
        per = b1.shape[0] // width
        for k in range(per):
            row = jnp.where(group == 0, rows[8 + k : 9 + k, :], rows[8 + per + k : 9 + per + k, :])
            b1[k * width : (k + 1) * width] = row.reshape(width)


def whole(array):
    return pl.BlockSpec(array.shape, lambda *_: (0,) * len(array.shape))


def blocks(count, *rest):
    return pl.BlockSpec((count,) + rest, lambda i: (i,) + (0,) * len(rest))


def fixed(*shape):
    return pl.BlockSpec(shape, lambda *_: (0,) * len(shape))


def params(axes=1, **kw):
    return pltpu.CompilerParams(vmem_limit_bytes=VMEM_LIMIT, dimension_semantics=("arbitrary",) * axes, **kw)


HBM = pl.BlockSpec(memory_space=pl.ANY)
sds = jax.ShapeDtypeStruct


def forward_part(inputs, weights, vectors, pitch, members):
    images, length, width = inputs.shape
    count = 4
    share, wide = vectors[0].shape[0], vectors[-1].shape[0]
    lanes = (share + LANES - 1) // LANES * LANES
    fulls = [(members * w.shape[0], w.shape[1]) for w in weights]
    turned = (images, width, pitch)
    return pl.pallas_call(
        functools.partial(attention_forward, length, pitch, count, 2),
        grid=(images // count,),
        in_specs=[whole(inputs)] + [HBM] * 4 + [whole(v) for v in vectors],
        out_specs=[
            blocks(count, width, pitch), blocks(count, width, pitch), blocks(count, pitch, width),
            blocks(count, HEADS, pitch, pitch), blocks(count, 8, pitch), blocks(count, width, pitch),
            blocks(count, width + 16, pitch), HBM, HBM, HBM, HBM, fixed(8, width), fixed(8, members * wide),
        ],
        out_shape=[
            sds(turned, BF), sds(turned, BF), sds((images, pitch, width), BF),
            sds((images, HEADS, pitch, pitch), BF), sds((images, 8, pitch), F32), sds(turned, BF),
            sds((images, width + 16, pitch), BF),
        ] + [sds(full, BF) for full in fulls] + [sds((8, width), F32), sds((8, members * wide), F32)],
        scratch_shapes=[pltpu.VMEM((images, pitch, width), F32)] + [pltpu.VMEM(full, BF) for full in fulls] + [
            pltpu.VMEM((members, 8, lanes), F32), pltpu.VMEM((members, 8, wide), F32),
            pltpu.VMEM((8, width), F32), pltpu.VMEM((8, members * wide), F32),
            pltpu.VMEM((width, width), BF), pltpu.VMEM((width, pitch), F32), pltpu.VMEM((count, pitch, width), BF),
            pltpu.SemaphoreType.DMA((4,)), pltpu.SemaphoreType.DMA((4,)), pltpu.SemaphoreType.DMA((4,)),
            pltpu.SemaphoreType.DMA((4,)), pltpu.SemaphoreType.DMA((2,)), pltpu.SemaphoreType.DMA((2,)),
            pltpu.SemaphoreType.DMA((4,)), pltpu.SemaphoreType.DMA((4,)),
        ],
        compiler_params=params(collective_id=0, has_side_effects=True),
        name="attention_forward",
    )(inputs, *weights, *vectors)


def middle_part(inputs, cotangent, attended, w_proj, w_fc1, w_fc2, vecs, bias_fc1, pitch):
    images, length, width = inputs.shape
    hidden_units = w_fc1.shape[1]
    count = 5
    rows = count * pitch
    units = 2 * hidden_units // (QUAD * LANES)
    unit_rows = QUAD * width // 2
    unit = (units, 2, unit_rows, LANES)
    strip = (width // LANES, 2, width // 2, LANES)
    return pl.pallas_call(
        functools.partial(mlp_both, length, pitch, count, 256),
        grid=(images // count,),
        in_specs=[blocks(count, length, width), blocks(count, length, width), blocks(count, width, pitch)] + [
            whole(w) for w in (w_proj, w_fc1, w_fc2, vecs, bias_fc1)
        ],
        out_specs=[
            blocks(count, length, width), blocks(count, pitch, width), blocks(count, width, pitch),
            fixed(*unit), fixed(*strip), fixed(16, width),
        ],
        out_shape=[
            sds((images, length, width), BF), sds((images, pitch, width), F32), sds((images, width, pitch), BF),
            sds(unit, BF), sds(strip, BF), sds((16, width), F32),
        ],
        scratch_shapes=[
            pltpu.VMEM((rows, width), BF), pltpu.VMEM((rows, width), BF), pltpu.VMEM((rows, width), BF),
            pltpu.VMEM((rows, hidden_units), BF), pltpu.VMEM((rows, hidden_units), BF),
            pltpu.VMEM((width, hidden_units), BF),
            pltpu.VMEM((width, hidden_units), F32), pltpu.VMEM((width, hidden_units), F32),
            pltpu.VMEM((width, width), F32), pltpu.VMEM((8, width), F32), pltpu.VMEM((8, hidden_units), F32),
        ],
        compiler_params=params(),
        name="mlp_both",
    )(inputs, cotangent, attended, w_proj, w_fc1, w_fc2, vecs, bias_fc1)


def backward_part(inputs, grad_resid, grad_att, qt, kt, values, raised, inverse, turned_x, w_qkv, vecs, strips, dvec, fc_units, pitch, replicas):
    images, length, width = inputs.shape
    count = 5
    rows = count * pitch
    steps = images // count
    pairs = HEADS // 2
    pair = width // pairs
    unit_rows = QUAD * width // 2
    unit = (pairs, 2, unit_rows, LANES)
    fc_sum, qkv_sum = (fc_units.shape[0], unit_rows, LANES), (pairs, unit_rows, LANES)
    scratch = []
    for name in [name for name in CHAINS if name != "v"]:
        units = 1 if name in range(pairs) else fc_units.shape[0] // 3
        scratch += reduce_scratch(units, unit_rows, replicas, name)
    scratch += vector_scratch(dvec.shape, replicas)

    def edge(p, i):
        return jnp.where(p == pairs, i, 0)

    def tail(p, i):
        return jnp.where(p == pairs, i, 0)

    def core(p, i):
        return jnp.where(p == pairs, steps - 1, i), jnp.minimum(p, pairs - 1)

    def turned(p, i):
        at, row = core(p, i)
        return at, row, 0

    def plain(p, i):
        at, col = core(p, i)
        return at, 0, col

    def exp_at(p, i):
        at, col = core(p, i)
        return at, col, 0, 0

    strip = pl.BlockSpec((count, pair, pitch), turned)
    return pl.pallas_call(
        functools.partial(attention_backward, length, pitch, count, steps),
        grid=(pairs + 1, steps),
        in_specs=[
            pl.BlockSpec((count, length, width), lambda p, i: (edge(p, i), 0, 0)),
            pl.BlockSpec((count, pitch, width), lambda p, i: (tail(p, i), 0, 0)),
            strip, strip, strip, pl.BlockSpec((count, pitch, pair), plain),
            pl.BlockSpec((count, 2, pitch, pitch), exp_at),
            pl.BlockSpec((count, 8, pitch), lambda p, i: (core(p, i)[0], 0, 0)),
            pl.BlockSpec((count, width + 16, pitch), lambda p, i: (core(p, i)[0], 0, 0)),
            whole(w_qkv), whole(vecs), whole(strips), whole(dvec), whole(fc_units),
        ],
        out_specs=[pl.BlockSpec((count, length, width), lambda p, i: (tail(p, i), 0, 0)), HBM, HBM, HBM],
        out_shape=[sds((images, length, width), BF), sds(fc_sum, BF), sds(qkv_sum, BF), sds(dvec.shape, F32)],
        scratch_shapes=[
            pltpu.VMEM((rows, width), BF),
            pltpu.VMEM((pairs, images, 3 * pair, pitch), BF), pltpu.VMEM((width, 3 * width), BF),
            pltpu.VMEM((width + 16, 3 * pair), F32), pltpu.VMEM((pairs, 8, 3 * pair), F32), pltpu.VMEM(unit, BF), pltpu.VMEM(dvec.shape, F32),
            pltpu.VMEM(fc_sum, BF), pltpu.VMEM(qkv_sum, BF), pltpu.VMEM(dvec.shape, F32),
            pltpu.SemaphoreType.DMA((len(CHAINS) + 1,)),
        ] + scratch,
        compiler_params=params(2, collective_id=1, has_side_effects=True),
        name="attention_backward",
    )(inputs, grad_resid, grad_att, qt, kt, values, raised, inverse, turned_x, w_qkv, vecs, strips, dvec, fc_units)


def local(
    inputs, cotangent, gain_one, shift_one, w_qkv, b_query, b_value, w_proj, b_proj,
    gain_two, shift_two, w_fc1, b_fc1, w_fc2, b_fc2,
):
    images, length, width = inputs.shape
    members = lax.axis_size("group")
    replicas = lax.axis_size("replica")
    pitch = (length + 7) // 8 * 8
    qt, kt, values, raised, inverse, attended, turned_x, wq, wp, w1, w2, vecs, bias_fc1 = forward_part(
        inputs, (w_qkv, w_proj, w_fc1, w_fc2),
        (gain_one, shift_one, b_query, b_value, b_proj, gain_two, shift_two, b_fc2, b_fc1), pitch, members,
    )
    outputs, grad_resid, grad_att, fc_units, strips, dvec = middle_part(
        inputs, cotangent, attended, wp, w1, w2, vecs, bias_fc1, pitch
    )
    grad_inputs, fc_sum, qkv_sum, vec_sum = backward_part(
        inputs, grad_resid, grad_att, qt, kt, values, raised, inverse, turned_x, wq, vecs, strips, dvec, fc_units,
        pitch, replicas
    )
    factor = float(images * length * replicas * members) ** (-0.5)
    weights = (gain_one, shift_one, w_qkv, b_query, b_value, w_proj, b_proj, gain_two, shift_two, w_fc1, b_fc1, w_fc2, b_fc2)
    grad_inputs, *grads = pl.pallas_call(
        functools.partial(unpack, factor),
        grid=(4,),
        in_specs=[blocks(images // 4, length, width), whole(fc_sum), whole(qkv_sum), whole(vec_sum)] + [
            whole(w) for w in (w_qkv, gain_one, shift_one)
        ],
        out_specs=[blocks(images // 4, length, width)] + [whole(w) for w in weights],
        out_shape=[sds(inputs.shape, F32)] + [sds(w.shape, F32) for w in weights],
        compiler_params=params(),
        name="unpack",
    )(grad_inputs, fc_sum, qkv_sum, vec_sum, w_qkv, gain_one, shift_one)
    return (outputs, grad_inputs) + tuple(grads)


def solution(mesh):
    images = P(("replica", "group"), None, None)
    line, table = P("group"), P("group", None)
    specs = (line, line, table, line, line, table, line, line, line, table, line, table, line)
    return jax.shard_map(
        local, mesh=mesh, in_specs=(images, images) + specs, out_specs=(images, images) + specs, check_vma=False
    )
```

```python
import functools

import jax
import jax.numpy as jnp
from jax import lax
from jax.experimental import pallas as pl
from jax.experimental.pallas import tpu as pltpu
from jax.sharding import PartitionSpec as P

HEADS = 6
EPS = 1e-06
BF = jnp.bfloat16
F32 = jnp.float32
LOG2E = 1.4426950408889634
VMEM_LIMIT = 60 * 1024 * 1024
MESH = pl.DeviceIdType.MESH
LANES = 128
QUAD = 4


def dot(left, right):
    return jnp.dot(left, right, preferred_element_type=F32)


def dot_lt(left, right):
    return lax.dot_general(left, right, (((0,), (0,)), ((), ())), preferred_element_type=F32)


def dot_rt(left, right):
    return lax.dot_general(left, right, (((1,), (1,)), ((), ())), preferred_element_type=F32)


def row_stats(rows):
    centre = jnp.mean(rows, axis=-1, keepdims=True)
    centered = rows - centre
    inverse = lax.rsqrt(jnp.mean(centered * centered, axis=-1, keepdims=True) + EPS)
    return centered * inverse, inverse


def norm_back(grad_hidden, normed, inverse, gain):
    grad_normed = grad_hidden * gain
    one = jnp.mean(grad_normed, axis=-1, keepdims=True)
    two = jnp.mean(grad_normed * normed, axis=-1, keepdims=True)
    return inverse * (grad_normed - one - normed * two)


def col_sum(rows):
    return jnp.sum(rows, axis=0, keepdims=True)


def place():
    return lax.axis_index("replica"), lax.axis_index("group")


def greet(partners):
    barrier = pltpu.get_barrier_semaphore()
    for partner in partners:
        pl.semaphore_signal(barrier, inc=1, device_id=partner, device_id_type=MESH)
    pl.semaphore_wait(barrier, len(partners))


def remote(source, target, send, recv, device):
    return pltpu.make_async_remote_copy(
        src_ref=source, dst_ref=target, send_sem=send, recv_sem=recv, device_id=device, device_id_type=MESH
    )


class Gather:
    def __init__(self, shards, wholes, sends, recvs, passes, arrivals):
        self.replica, self.group = place()
        core = lax.rem(self.replica, 2)
        self.across = (self.replica, 1 - self.group)
        self.beside = (self.replica + 1 - 2 * core, self.group)
        self.first, self.second = [], []
        for k, (shard, whole_ref) in enumerate(zip(shards, wholes)):
            rows = shard.shape[0]
            half = rows // 2
            mine = pl.ds(pl.multiple_of(core * half, half), half)
            there = pl.ds(pl.multiple_of(self.group * rows + core * half, half), half)
            here = pl.ds(pl.multiple_of((1 - self.group) * rows + core * half, half), half)
            self.first.append(remote(shard.at[mine], whole_ref.at[there], sends.at[k], recvs.at[k], self.across))
            self.second.append(
                remote(whole_ref.at[here], whole_ref.at[here], passes.at[k], arrivals.at[k], self.beside)
            )


def pipeline(items, *stages):
    for tick in range(len(items) + len(stages) - 1):
        for late, stage in enumerate(stages):
            if 0 <= tick - late < len(items):
                stage(items[tick - late])


def attention_forward(
    length, pitch, count, late,
    x_ref, wq_hbm, wp_hbm, w1_hbm, w2_hbm, g1, s1, bq, bv, bp, g2, s2, b2, b1,
    qt_ref, kt_ref, v_ref, exp_ref, inv_ref, att_ref, nt_ref, wq_out, wp_out, w1_out, w2_out, vec_out, b1_out,
    normed_ref, wq, wp, w1, w2, small, wide, vec, b1_full, wqt, bias_q, k_ref,
    sends, recvs, passes, arrivals, vec_send, vec_recv, own_sem, out_sem,
):
    step = pl.program_id(0)
    width = x_ref.shape[2]
    head_dim = width // HEADS
    factor = head_dim ** (-0.5) * LOG2E
    shards = (wq_hbm, wp_hbm, w1_hbm, w2_hbm)
    wholes = (wq, wp, w1, w2)
    outs = (wq_out, wp_out, w1_out, w2_out)
    move = Gather(shards, wholes, sends, recvs, passes, arrivals)
    group = move.group
    small_copy = remote(small.at[group], small.at[group], vec_send.at[0], vec_recv.at[0], move.across)
    wide_copy = remote(wide.at[group], wide.at[group], vec_send.at[1], vec_recv.at[1], move.across)
    owns = [
        pltpu.make_async_copy(
            shard, full.at[pl.ds(pl.multiple_of(group * shard.shape[0], shard.shape[0]), shard.shape[0])], own_sem.at[k]
        )
        for k, (shard, full) in enumerate(zip(shards, wholes))
    ]
    flush = [pltpu.make_async_copy(full, out, out_sem.at[k]) for k, (full, out) in enumerate(zip(wholes, outs))]
    last = pl.num_programs(0) - 1

    @pl.when(step == 0)
    def _():
        share = g1.shape[0]
        for k, ref in enumerate((g1, s1, bq, bv, bp, g2, s2, b2)):
            small[group, k : k + 1, 0:share] = ref[...].reshape(1, share).astype(F32)
        wide[group, 0:1, :] = b1[...].reshape(1, b1.shape[0]).astype(F32)
        greet((move.across, move.beside))
        small_copy.start()
        for copy in move.first:
            copy.start()
        wide_copy.start()
        for copy in owns:
            copy.start()
        tail_ = length // 8 * 8

        @pl.loop(0, x_ref.shape[0])
        def _(image):
            normed_ref[image, tail_:, :] = jnp.zeros((pitch - tail_, width), F32)
            normed_ref[image, 0:length, :] = row_stats(x_ref[image].astype(F32))[0]

        small_copy.wait()
        for side in range(2):
            vec[:, side * share : (side + 1) * share] = small[side, :, 0:share]
        vec_out[...] = vec[...]
        bias_q[...] = jnp.broadcast_to(vec[...].T[:, 2:3], bias_q.shape)
        move.first[0].wait()
        move.second[0].start()
        owns[0].wait()
        move.second[0].wait()
        wqt[...] = wq[:, 0:width].T

    @pl.when(step == late)
    def _():
        for k in range(1, 4):
            move.first[k].wait()
            move.second[k].start()
        wide_copy.wait()
        for side in range(2):
            b1_full[0:1, side * b1.shape[0] : (side + 1) * b1.shape[0]] = wide[side, 0:1, :]
        b1_out[...] = b1_full[...]
        for k in range(1, 4):
            owns[k].wait()

    @pl.when(step == late + 1)
    def _():
        for k in range(1, 4):
            move.second[k].wait()
        for copy in flush:
            copy.start()

    gain = vec[0:1, :]
    shift = vec[1:2, :]
    normed = normed_ref[pl.ds(step * count, count)].reshape(count * pitch, width)
    hidden = (normed * gain + shift).astype(BF)
    keys_all = dot(hidden, wq[:, width : 2 * width]).astype(BF)
    values_all = (dot(hidden, wq[:, 2 * width :]) + vec[3:4, :]).astype(BF)
    for image in range(count):
        rows = slice(image * pitch, (image + 1) * pitch)
        nt_ref[image, 0:width, :] = normed[rows].astype(BF).T
        nt_ref[image, width:, :] = jnp.ones((16, pitch), BF)
        k_ref[image] = keys_all[rows]
        v_ref[image] = values_all[rows]
        qt_ref[image] = ((dot_rt(wqt[...], hidden[rows]) + bias_q[...]) * factor).astype(BF)
    tail = length // 8 * 8
    row = lax.broadcasted_iota(jnp.int32, (pitch - tail, pitch), 0) + tail
    zero = jnp.zeros((head_dim, pitch), BF)
    ones = jnp.ones((16, pitch), BF)
    kept = {}

    def score(item):
        image, two, side = item
        cols = slice(two * LANES, (two + 1) * LANES)
        if side == 0:
            kt_ref[image, cols, :] = k_ref[image, :, cols].T
            kept["vt", image, two] = v_ref[image, :, cols].T
        at = two * LANES + side * head_dim
        own = qt_ref[image, at : at + head_dim, :]
        full = jnp.concatenate([own, zero] if side == 0 else [zero, own], axis=0)
        kept[item] = dot(k_ref[image, :, cols], full)

    def soften(item):
        image, two, side = item
        scores = kept.pop(item)
        low = jnp.where(row < length, scores[tail:], -1e30)
        scores = jnp.concatenate([scores[:tail], low], axis=0)
        top = jnp.max(scores, axis=0, keepdims=True)
        raised = jnp.exp2(scores - top).astype(BF)
        exp_ref[image, 2 * two + side] = raised
        kept[item] = raised

    def mix(item):
        image, two, side = item
        own = kept["vt", image, two][side * head_dim : (side + 1) * head_dim]
        mixed = dot(jnp.concatenate([own, ones], axis=0), kept.pop(item))
        inverse = 1.0 / mixed[head_dim : head_dim + 1]
        at = two * LANES + side * head_dim
        inv_ref[image, 2 * two + side : 2 * two + side + 1, :] = inverse
        att_ref[image, at : at + head_dim, :] = (mixed[:head_dim] * inverse).astype(BF)

    items = [(image, two, side) for image in range(count) for two in range(HEADS // 2) for side in range(2)]
    pipeline(items, score, soften, mix)

    @pl.when(step == last)
    def _():
        for copy in flush:
            copy.wait()


def gelu_parts(values):
    half = 0.5 * (1.0 + lax.erf(values * 0.7071067811865476))
    slope = half + values * jnp.exp(-0.5 * values * values) * 0.3989422804014327
    return half, slope


def mlp_both(
    length, pitch, count, chunk,
    x_ref, ct_ref, att_ref, wp_ref, w1_ref, w2_ref, vec_ref, b1_ref,
    y_ref, gr_ref, ga_ref, unit_ref, strip_ref, dvec_ref,
    xpad, ctpad, att_s, act_ref, gp_ref, w2t, acc1, acc2, accp, accv, accb,
):
    step = pl.program_id(0)
    width = x_ref.shape[2]
    hidden_units = w1_ref.shape[1]

    @pl.when(step == 0)
    def _():
        for ref in (xpad, ctpad, acc1, acc2, accp, accv, accb):
            ref[...] = jnp.zeros_like(ref)
        w2t[...] = w2_ref[...].T

    for image in range(count):
        att_s[image * pitch : (image + 1) * pitch, :] = att_ref[image].T
        xpad[image * pitch : image * pitch + length, :] = x_ref[image]
        ctpad[image * pitch : image * pitch + length, :] = ct_ref[image]
    bias_p = vec_ref[4:5, :]
    gain = vec_ref[5:6, :]
    shift = vec_ref[6:7, :]
    bias_2 = vec_ref[7:8, :]
    ct = ctpad[...]
    att = att_s[...]
    resid = xpad[...].astype(F32) + dot(att, wp_ref[...]) + bias_p
    normed, inverse = row_stats(resid)
    hidden = (normed * gain + shift).astype(BF)
    for start in range(0, hidden_units, chunk):
        cols = slice(start, start + chunk)
        pre = dot(hidden, w1_ref[:, cols]) + b1_ref[0:1, cols]
        half, slope = gelu_parts(pre)
        act_ref[:, cols] = (pre * half).astype(BF)
        grad_pre = dot_rt(ct, w2_ref[cols, :]) * slope
        accb[0:1, cols] += col_sum(grad_pre)
        gp_ref[:, cols] = grad_pre.astype(BF)
    out = resid + dot_rt(w2t[...], act_ref[...]).T + bias_2
    for image in range(count):
        y_ref[image] = out[image * pitch : image * pitch + length].astype(BF)
    grad_hidden = dot_rt(w1_ref[...], gp_ref[...]).T
    top = ct.astype(F32)
    grad_resid = top + norm_back(grad_hidden, normed, inverse, gain)
    accv[0:1, :] += col_sum(grad_resid)
    accv[1:2, :] += col_sum(grad_hidden * normed)
    accv[2:3, :] += col_sum(grad_hidden)
    accv[3:4, :] += col_sum(top)
    grad_resid_b = grad_resid.astype(BF)
    for image in range(count):
        rows = slice(image * pitch, (image + 1) * pitch)
        gr_ref[image] = grad_resid[rows]
        ga_ref[image] = dot_rt(wp_ref[...], grad_resid_b[rows]).astype(BF)
    acc1[...] += dot_lt(hidden, gp_ref[...])
    acc2[...] += dot_lt(ct, act_ref[...])
    accp[...] += dot_lt(att, grad_resid_b)

    @pl.when(step == pl.num_programs(0) - 1)
    def _():
        share = width // 2
        wide = hidden_units // 2
        for side in range(2):
            rows = slice(side * share, (side + 1) * share)
            for strip in range(hidden_units // LANES):
                unit, at = strip // QUAD, strip % QUAD * share
                unit_ref[unit, side, at : at + share, :] = acc1[rows, strip * LANES : (strip + 1) * LANES].astype(BF)
            for strip in range(wide // LANES):
                unit, at = strip // 2 + hidden_units // (QUAD * LANES), strip % 2 * width
                start = side * wide + strip * LANES
                unit_ref[unit, side, at : at + width, :] = acc2[:, start : start + LANES].astype(BF)
            for strip in range(width // LANES):
                strip_ref[strip, side] = accp[rows, strip * LANES : (strip + 1) * LANES].astype(BF)
        dvec_ref[...] = jnp.zeros_like(dvec_ref)
        dvec_ref[0:4, :] = accv[0:4, :]
        for k in range(hidden_units // width):
            dvec_ref[8 + k : 9 + k, :] = accb[0:1, k * width : (k + 1) * width]


CHAINS = {
    "a": (0, 1, 4, 6, 8, 11, 13, 14),
    "b": (0, 1, 4, 6, 8, 11, 13, 14),
    "c": (0, 4, 7, 9, 11, 13, 15, 16),
    0: (4, 5, 8, 10, 12, 13, 14, 15),
    1: (8, 9, 11, 13, 14, 15, 16, 16),
    2: (12, 13, 14, 16, 16, 16),
    "v": (12, 13, 14, 15, 16),
}
SWAPPED = ("b", 0)
SHORT = (2,)


def schedule(total):
    plan = {0: [("greet", None, None)]}
    for name, starts in CHAINS.items():
        order = order_of(name)
        for k, at in enumerate(starts):
            work = (name, order[k - 1] if k else None, order[k] if k < len(order) else None)
            plan.setdefault(at if at < total else -1, []).append(work)
    return plan


def order_of(name):
    if name == "v":
        return (0, 1, 2, 3)
    return (0, 1, 3, 5, 7) if name in SHORT else (0, 1, 2, 3, 5, 6, 7)


class Ticks:
    def __init__(self, parts, flushes):
        self.parts, self.flushes = parts, flushes

    def run(self, work):
        for name, done, start in work:
            if name == "greet":
                greet(self.parts["a"].partners())
                continue
            part = self.parts[name]
            if done is not None:
                part.finish(done)
                if done == 3 and part.extra > 1:
                    part.start(4)
                    part.finish(4)
                if done == order_of(name)[-1]:
                    self.flushes[name].start()
            if start is not None:
                part.start(start)

    def close(self, work):
        pending = list(work)
        while pending:
            names, later = set(), []
            for item in pending:
                if item[0] in names:
                    later.append(item)
                else:
                    names.add(item[0])
                    self.run([item])
            pending = later
        for copy in self.flushes.values():
            copy.wait()


def make_ticks(fc_ref, unit_ref, dvec_ref, fc_out, qkv_out, vec_out, fc_hbm, qkv_hbm, vec_hbm, flush_sem, scratch):
    third = fc_ref.shape[0] // 3
    pairs = unit_ref.shape[0]
    sources = {name: (fc_ref, fc_out, fc_hbm, k * third, third) for k, name in enumerate("abc")}
    for k in range(pairs):
        sources[k] = (unit_ref, qkv_out, qkv_hbm, k, 1)
    parts, flushes = {}, {}
    for k, (name, (source, out, hbm, at, size)) in enumerate(sources.items()):
        refs = scratch[k * REDUCE_REFS : (k + 1) * REDUCE_REFS]
        mine = pl.ds(at, size)
        parts[name] = Reduce(source.at[mine], refs[:8], out.at[mine], refs[8], refs[9], name)
        flushes[name] = pltpu.make_async_copy(out.at[mine], hbm.at[mine], flush_sem.at[k])
    parts["v"] = ReduceVectors(parts["a"], *scratch[len(sources) * REDUCE_REFS :], first=dvec_ref, out=vec_out)
    flushes["v"] = pltpu.make_async_copy(vec_out, vec_hbm, flush_sem.at[len(sources)])
    return Ticks(parts, flushes)


def attention_backward(
    length, pitch, count, steps,
    x_ref, gr_ref, ga_ref, qt_ref, kt_ref, v_ref, exp_ref, inv_ref, nt_ref, wq_ref, vec_ref, strip_ref, dvec_in, fc_ref,
    gx_ref, fc_hbm, qkv_hbm, vec_hbm,
    pad_ref, gp_ref, wperm, acc, accv, unit_ref, dvec_ref, fc_out, qkv_out, vec_out, flush_sem, *scratch,
):
    phase, block = pl.program_id(0), pl.program_id(1)
    phases, blocks_ = pl.num_programs(0), pl.num_programs(1)
    step = phase * blocks_ + block
    ticks = make_ticks(
        fc_ref, unit_ref, dvec_ref, fc_out, qkv_out, vec_out, fc_hbm, qkv_hbm, vec_hbm, flush_sem, scratch
    )
    plan = schedule((HEADS // 2 + 1) * steps)
    for at, work in plan.items():
        if at >= 0:
            @pl.when(step == at)
            def _(work=work):
                ticks.run(work)
    width = x_ref.shape[2]
    head_dim = width // HEADS
    pair = 2 * head_dim
    factor = head_dim ** (-0.5)
    rows = count * pitch
    first = block * count
    gain = vec_ref[0:1, :]

    @pl.when(jnp.logical_and(phase == 0, block == 0))
    def _():
        pad_ref[...] = jnp.zeros_like(pad_ref)
        for two in range(HEADS // 2):
            for third in range(3):
                to, at = (3 * two + third) * pair, third * width + two * pair
                wperm[:, to : to + pair] = wq_ref[:, at : at + pair]

    def stats():
        for image in range(count):
            pad_ref[image * pitch : image * pitch + length, :] = x_ref[image]
        return row_stats(pad_ref[...].astype(F32))

    @pl.when(phase < phases - 1)
    def _():
        @pl.when(block == 0)
        def _():
            acc[...] = jnp.zeros_like(acc)

        zero = jnp.zeros((head_dim, pitch), BF)
        kept = {}

        def probe(item):
            image, side = item
            own = slice(side * head_dim, (side + 1) * head_dim)
            inverse = inv_ref[image, pl.ds(2 * phase + side, 1), :]
            grad_out = (ga_ref[image, own, :].astype(F32) * inverse).astype(BF)
            full = jnp.concatenate([grad_out, zero] if side == 0 else [zero, grad_out], axis=0)
            kept[item] = (dot(v_ref[image], full), grad_out, inverse)

        def soften(item):
            image, side = item
            grad_probs, grad_out, inverse = kept[item]
            raised = exp_ref[image, side].astype(F32)
            delta = jnp.sum(raised * grad_probs, axis=0, keepdims=True) * inverse
            kept[item] = ((raised * (grad_probs - delta)).astype(BF), grad_out)

        def spread(item):
            image, side = item
            scores, grad_out = kept.pop(item)
            own = slice(side * head_dim, (side + 1) * head_dim)
            grad_q = dot(kt_ref[image, own, :], scores) * factor
            grad_k = dot_rt(qt_ref[image, own, :], scores) * (1.0 / LOG2E)
            grad_v = dot_rt(grad_out, exp_ref[image, side])
            for third, part in enumerate((grad_q, grad_k, grad_v)):
                at = third * pair + side * head_dim
                gp_ref[phase, first + image, at : at + head_dim, :] = part.astype(BF)

        def gather(item):
            image, side = item
            if side == 1:
                acc[...] += dot_rt(nt_ref[image], gp_ref[phase, first + image])

        items = [(image, side) for image in range(count) for side in range(2)]
        pipeline(items, probe, soften, spread, gather)

        @pl.when(block == blocks_ - 1)
        def _():
            share = width // 2
            for side in range(2):
                for strip in range(3):
                    unit_ref[phase, side, strip * share : (strip + 1) * share, :] = acc[
                        side * share : (side + 1) * share, strip * pair : (strip + 1) * pair
                    ].astype(BF)
                unit_ref[phase, side, 3 * share :, :] = strip_ref[phase, side]
            accv[phase] = acc[width : width + 8, :]

            @pl.when(phase == phases - 2)
            def _():
                dvec_ref[...] = dvec_in[...]
                for two in range(HEADS // 2):
                    for third in range(3):
                        dvec_ref[4 + third : 5 + third, two * pair : (two + 1) * pair] = accv[
                            two, 0:1, third * pair : (third + 1) * pair
                        ]

    @pl.when(phase == phases - 1)
    def _():
        normed, inverse = stats()
        for image in range(count):
            at = slice(image * pitch, (image + 1) * pitch)
            packed = jnp.concatenate([gp_ref[two, first + image] for two in range(HEADS // 2)], axis=0)
            grad_hidden = dot(wperm[...], packed).T
            grad_x = gr_ref[image] + norm_back(grad_hidden, normed[at], inverse[at], gain)
            gx_ref[image] = grad_x[:length].astype(BF)

        @pl.when(block == blocks_ - 1)
        def _():
            ticks.close(plan.get(-1, []))


SLOTS = {False: (0, 1, 2, 3, 11, 6, 9, 10), True: (0, 1, 0, 2, 17, 9, 0, 16)}


class Reduce:
    def __init__(self, source, bufs, out, sends, recvs, name):
        self.replica, self.group = place()
        self.swapped, self.short = name in SWAPPED, name in SHORT
        self.source, self.out = source, out
        self.r1, self.b1, self.r2, self.b2, self.rx, self.bx, self.rz, self.ez = bufs
        replicas = lax.axis_size("replica")
        self.extra = replicas // 16
        half = out.shape[1] // 2
        self.half, self.quarter, self.piece = half, half // 2, half // 8
        r = self.replica
        self.core = lax.rem(r, 2)
        self.x = lax.rem(r // 2, 2)
        self.z = lax.rem(r // 4, 4)
        self.e = r // 16
        self.m = lax.rem(r // 2, 8)
        self.sends, self.recvs = sends, recvs
        low = self.core * half
        self.at_core = pl.ds(pl.multiple_of(low, half), half)
        self.at_quarter = pl.ds(pl.multiple_of(low + self.x * self.quarter, self.quarter), self.quarter)
        self.at_piece = pl.ds(
            pl.multiple_of(low + self.x * self.quarter + self.z * self.piece, self.piece), self.piece
        )

    def partners(self):
        return [self.to_core(), self.to_group()] + [self.to_m(d) for d in range(1, 8)] + [
            self.to_e(d) for d in range(1, self.extra)
        ]

    def to_core(self):
        return (self.replica + 1 - 2 * self.core, self.group)

    def to_group(self):
        return (self.replica, 1 - self.group)

    def to_x(self):
        return (self.replica + 2 - 4 * self.x, self.group)

    def z_at(self, hop):
        return lax.rem(self.z + hop, 4)

    def to_z(self, hop):
        return (self.replica + 4 * (self.z_at(hop) - self.z), self.group)

    def m_at(self, hop):
        return lax.rem(self.m + hop, 8)

    def to_m(self, hop):
        return (self.replica + 2 * (self.m_at(hop) - self.m), self.group)

    def row_of(self, m):
        start = lax.rem(m, 2) * self.quarter + m // 2 * self.piece
        return pl.ds(pl.multiple_of(start, self.piece), self.piece)

    def to_e(self, hop):
        return (self.replica + 16 * (lax.rem(self.e + hop, self.extra) - self.e), self.group)

    def copy(self, stage, source, target, device, hop=0):
        at = SLOTS[self.short][stage] + hop - (stage in (3, 5)) - (stage == 4)
        return remote(source, target, self.sends.at[at], self.recvs.at[at], device)

    def copies(self, stage):
        if stage == 0:
            other = pl.ds(pl.multiple_of((1 - self.core) * self.half, self.half), self.half)
            return [self.copy(0, self.source.at[:, :, other], self.r1, self.to_core())]
        if stage == 1 and self.swapped:
            other = pl.ds(pl.multiple_of((1 - self.x) * self.quarter, self.quarter), self.quarter)
            return [self.copy(1, self.b1.at[:, :, other], self.r2, self.to_x())]
        if stage == 2 and self.swapped:
            return [self.copy(2, self.b2.at[:, 1 - self.group], self.rx, self.to_group())]
        if stage == 1:
            return [self.copy(1, self.b1.at[:, 1 - self.group], self.r2, self.to_group())]
        if stage == 2:
            other = pl.ds(pl.multiple_of((1 - self.x) * self.quarter, self.quarter), self.quarter)
            return [self.copy(2, self.b2.at[:, other], self.rx, self.to_x())]
        if stage == 3 and self.short:
            return [
                self.copy(3, self.b2.at[:, self.row_of(self.m_at(hop))], self.rz.at[hop - 1], self.to_m(hop), hop)
                for hop in range(1, 8)
            ]
        if stage == 5 and self.short:
            place_ = self.out.at[:, self.at_piece]
            return [self.copy(5, place_, place_, self.to_m(hop), hop) for hop in range(1, 8)]
        if stage == 3:
            out = []
            for hop in (1, 2, 3):
                theirs = pl.ds(pl.multiple_of(self.z_at(hop) * self.piece, self.piece), self.piece)
                out.append(self.copy(3, self.bx.at[:, theirs], self.rz.at[hop - 1], self.to_z(hop), hop))
            return out
        if stage == 4:
            return [
                self.copy(4, self.ez.at[self.e], self.ez.at[self.e], self.to_e(hop), hop) for hop in range(1, self.extra)
            ]
        if stage == 5:
            place_ = self.out.at[:, self.at_piece]
            return [self.copy(5, place_, place_, self.to_z(hop), hop) for hop in (1, 2, 3)]
        if stage == 6:
            place_ = self.out.at[:, self.at_quarter]
            return [self.copy(6, place_, place_, self.to_x())]
        place_ = self.out.at[:, self.at_core]
        return [self.copy(7, place_, place_, self.to_core())]

    def start(self, stage):
        for copy in self.copies(stage):
            copy.start()

    def finish(self, stage):
        for copy in self.copies(stage):
            copy.wait()
        if stage == 0:
            self.b1[...] = self.source[:, :, self.at_core] + self.r1[...]
        elif stage == 1 and self.swapped:
            mine = pl.ds(pl.multiple_of(self.x * self.quarter, self.quarter), self.quarter)
            self.b2[...] = self.b1[:, :, mine] + self.r2[...]
        elif stage == 2 and self.swapped:
            self.bx[...] = self.b2[:, self.group] + self.rx[...]
        elif stage == 1:
            self.b2[...] = self.b1[:, self.group] + self.r2[...]
        elif stage == 2:
            mine = pl.ds(pl.multiple_of(self.x * self.quarter, self.quarter), self.quarter)
            self.bx[...] = self.b2[:, mine] + self.rx[...]
        elif stage == 3:
            mine = pl.ds(pl.multiple_of(self.z * self.piece, self.piece), self.piece)
            own = self.b2.at[:, self.row_of(self.m)] if self.short else self.bx.at[:, mine]
            total = own[...].astype(F32)
            for hop in range(self.rz.shape[0]):
                total = total + self.rz[hop].astype(F32)
            if self.extra > 1:
                self.ez[self.e] = total.astype(BF)
            else:
                self.out[:, self.at_piece] = total.astype(BF)
        elif stage == 4 and self.extra > 1:
            total = self.ez[0].astype(F32)
            for k in range(1, self.extra):
                total = total + self.ez[k].astype(F32)
            self.out[:, self.at_piece] = total.astype(BF)


def reduce_scratch(units, rows, replicas, name):
    half, extra = rows // 2, max(replicas // 16, 1)
    sems = SLOTS[name in SHORT][4] + extra - 1
    second = (units, 2, half // 2, LANES) if name in SWAPPED else (units, half, LANES)
    return [
        pltpu.VMEM((units, 2, half, LANES), BF), pltpu.VMEM((units, 2, half, LANES), BF),
        pltpu.VMEM(second, BF), pltpu.VMEM(second, BF),
        pltpu.VMEM((units, half // 2, LANES), BF), pltpu.VMEM((units, half // 2, LANES), BF),
        pltpu.VMEM((7 if name in SHORT else 3, units, half // 8, LANES), BF), pltpu.VMEM((extra, units, half // 8, LANES), BF),
        pltpu.SemaphoreType.DMA((sems,)), pltpu.SemaphoreType.DMA((sems,)),
    ]


class ReduceVectors:
    def __init__(self, like, v2, v3, slots_z, slots_e, got, sends, recvs, first, out):
        self.like, self.out, self.extra = like, out, like.extra
        self.vals, self.slots_z, self.slots_e, self.got, self.sends, self.recvs = (
            (first, v2, v3), slots_z, slots_e, got, sends, recvs
        )

    def copies(self, stage):
        o = self.like
        if stage < 3:
            device = (o.to_core, o.to_group, o.to_x)[stage]()
            return [remote(self.vals[stage], self.got.at[stage], self.sends.at[stage], self.recvs.at[stage], device)]
        if stage == 3:
            mine = self.slots_z.at[o.z]
            return [
                remote(mine, mine, self.sends.at[2 + hop], self.recvs.at[2 + hop], o.to_z(hop)) for hop in (1, 2, 3)
            ]
        mine = self.slots_e.at[o.e]
        return [
            remote(mine, mine, self.sends.at[5 + hop], self.recvs.at[5 + hop], o.to_e(hop)) for hop in range(1, o.extra)
        ]

    def start(self, stage):
        for copy in self.copies(stage):
            copy.start()

    def finish(self, stage):
        o, out = self.like, self.out
        for copy in self.copies(stage):
            copy.wait()
        if stage < 2:
            self.vals[stage + 1][...] = self.vals[stage][...] + self.got[stage]
        elif stage == 2:
            self.slots_z[o.z] = self.vals[2][...] + self.got[2]
        elif stage == 3:
            total = self.slots_z[0] + self.slots_z[1] + self.slots_z[2] + self.slots_z[3]
            if o.extra > 1:
                self.slots_e[o.e] = total
            else:
                out[...] = total
        elif o.extra > 1:
            total = self.slots_e[0]
            for k in range(1, o.extra):
                total = total + self.slots_e[k]
            out[...] = total


def vector_scratch(shape, replicas):
    extra = max(replicas // 16, 1)
    return [
        pltpu.VMEM(shape, F32), pltpu.VMEM(shape, F32),
        pltpu.VMEM((4,) + shape, F32), pltpu.VMEM((extra,) + shape, F32), pltpu.VMEM((3,) + shape, F32),
        pltpu.SemaphoreType.DMA((5 + extra,)), pltpu.SemaphoreType.DMA((5 + extra,)),
    ]


REDUCE_REFS = 10


def unpack(factor, gx_in, fc_ref, qkv_ref, vec_ref, w_ref, gain_ref, shift_ref, gx_out, g1, s1, wq, bq, bv, wp, bp, g2, s2, w1, b1, w2, b2):
    gx_out[...] = gx_in[...].astype(F32)

    @pl.when(pl.program_id(0) == 0)
    def _():
        share, width = wp.shape
        group = lax.axis_index("group")
        pair = LANES
        column = [
            jnp.broadcast_to(ref[...].reshape(1, share).astype(F32), (8, share)).T[:, 0:1] for ref in (gain_ref, shift_ref)
        ]
        sum_g = jnp.zeros((share, pair), F32)
        sum_s = jnp.zeros((share, pair), F32)
        for two in range(qkv_ref.shape[0]):
            for third in range(3):
                cols = slice(third * width + two * pair, third * width + (two + 1) * pair)
                cross = qkv_ref[two, third * share : (third + 1) * share, :].astype(F32)
                total = vec_ref[4 + third : 5 + third, two * pair : (two + 1) * pair]
                weight = w_ref[:, cols].astype(F32)
                sum_g += weight * cross
                sum_s += weight * total
                wq[:, cols] = (column[0] * cross + column[1] * total) * factor
            wp[:, two * pair : (two + 1) * pair] = qkv_ref[two, 3 * share :, :].astype(F32) * factor
        for ref, total in ((g1, sum_g), (s1, sum_s)):
            ref[...] = (col_sum(total.T) * factor).reshape(share)
        strips = w1.shape[1] // LANES
        for strip in range(strips):
            unit, at = strip // QUAD, strip % QUAD * share
            w1[:, strip * LANES : (strip + 1) * LANES] = fc_ref[unit, at : at + share, :].astype(F32) * factor
        for strip in range(w2.shape[0] // LANES):
            unit, at = strip // 2 + strips // QUAD, strip % 2 * width
            w2[strip * LANES : (strip + 1) * LANES, :] = (fc_ref[unit, at : at + width, :].astype(F32) * factor).T
        rows = vec_ref[...] * factor
        mine = jnp.where(group == 0, rows[:, 0:share], rows[:, share:])
        for k, ref in enumerate((bp, g2, s2, b2, bq, None, bv)):
            if ref is not None:
                ref[...] = mine[k : k + 1, :].reshape(share)
        per = b1.shape[0] // width
        for k in range(per):
            row = jnp.where(group == 0, rows[8 + k : 9 + k, :], rows[8 + per + k : 9 + per + k, :])
            b1[k * width : (k + 1) * width] = row.reshape(width)


def whole(array):
    return pl.BlockSpec(array.shape, lambda *_: (0,) * len(array.shape))


def blocks(count, *rest):
    return pl.BlockSpec((count,) + rest, lambda i: (i,) + (0,) * len(rest))


def fixed(*shape):
    return pl.BlockSpec(shape, lambda *_: (0,) * len(shape))


def params(axes=1, **kw):
    return pltpu.CompilerParams(vmem_limit_bytes=VMEM_LIMIT, dimension_semantics=("arbitrary",) * axes, **kw)


HBM = pl.BlockSpec(memory_space=pl.ANY)
sds = jax.ShapeDtypeStruct


def forward_part(inputs, weights, vectors, pitch, members):
    images, length, width = inputs.shape
    count = 4
    share, wide = vectors[0].shape[0], vectors[-1].shape[0]
    lanes = (share + LANES - 1) // LANES * LANES
    fulls = [(members * w.shape[0], w.shape[1]) for w in weights]
    turned = (images, width, pitch)
    return pl.pallas_call(
        functools.partial(attention_forward, length, pitch, count, 3),
        grid=(images // count,),
        in_specs=[whole(inputs)] + [HBM] * 4 + [whole(v) for v in vectors],
        out_specs=[
            blocks(count, width, pitch), blocks(count, width, pitch), blocks(count, pitch, width),
            blocks(count, HEADS, pitch, pitch), blocks(count, 8, pitch), blocks(count, width, pitch),
            blocks(count, width + 16, pitch), HBM, HBM, HBM, HBM, fixed(8, width), fixed(8, members * wide),
        ],
        out_shape=[
            sds(turned, BF), sds(turned, BF), sds((images, pitch, width), BF),
            sds((images, HEADS, pitch, pitch), BF), sds((images, 8, pitch), F32), sds(turned, BF),
            sds((images, width + 16, pitch), BF),
        ] + [sds(full, BF) for full in fulls] + [sds((8, width), F32), sds((8, members * wide), F32)],
        scratch_shapes=[pltpu.VMEM((images, pitch, width), F32)] + [pltpu.VMEM(full, BF) for full in fulls] + [
            pltpu.VMEM((members, 8, lanes), F32), pltpu.VMEM((members, 8, wide), F32),
            pltpu.VMEM((8, width), F32), pltpu.VMEM((8, members * wide), F32),
            pltpu.VMEM((width, width), BF), pltpu.VMEM((width, pitch), F32), pltpu.VMEM((count, pitch, width), BF),
            pltpu.SemaphoreType.DMA((4,)), pltpu.SemaphoreType.DMA((4,)), pltpu.SemaphoreType.DMA((4,)),
            pltpu.SemaphoreType.DMA((4,)), pltpu.SemaphoreType.DMA((2,)), pltpu.SemaphoreType.DMA((2,)),
            pltpu.SemaphoreType.DMA((4,)), pltpu.SemaphoreType.DMA((4,)),
        ],
        compiler_params=params(collective_id=0, has_side_effects=True),
        name="attention_forward",
    )(inputs, *weights, *vectors)


def middle_part(inputs, cotangent, attended, w_proj, w_fc1, w_fc2, vecs, bias_fc1, pitch):
    images, length, width = inputs.shape
    hidden_units = w_fc1.shape[1]
    count = 5
    rows = count * pitch
    units = 2 * hidden_units // (QUAD * LANES)
    unit_rows = QUAD * width // 2
    unit = (units, 2, unit_rows, LANES)
    strip = (width // LANES, 2, width // 2, LANES)
    return pl.pallas_call(
        functools.partial(mlp_both, length, pitch, count, 256),
        grid=(images // count,),
        in_specs=[blocks(count, length, width), blocks(count, length, width), blocks(count, width, pitch)] + [
            whole(w) for w in (w_proj, w_fc1, w_fc2, vecs, bias_fc1)
        ],
        out_specs=[
            blocks(count, length, width), blocks(count, pitch, width), blocks(count, width, pitch),
            fixed(*unit), fixed(*strip), fixed(16, width),
        ],
        out_shape=[
            sds((images, length, width), BF), sds((images, pitch, width), F32), sds((images, width, pitch), BF),
            sds(unit, BF), sds(strip, BF), sds((16, width), F32),
        ],
        scratch_shapes=[
            pltpu.VMEM((rows, width), BF), pltpu.VMEM((rows, width), BF), pltpu.VMEM((rows, width), BF),
            pltpu.VMEM((rows, hidden_units), BF), pltpu.VMEM((rows, hidden_units), BF),
            pltpu.VMEM((width, hidden_units), BF),
            pltpu.VMEM((width, hidden_units), F32), pltpu.VMEM((width, hidden_units), F32),
            pltpu.VMEM((width, width), F32), pltpu.VMEM((8, width), F32), pltpu.VMEM((8, hidden_units), F32),
        ],
        compiler_params=params(),
        name="mlp_both",
    )(inputs, cotangent, attended, w_proj, w_fc1, w_fc2, vecs, bias_fc1)


def backward_part(inputs, grad_resid, grad_att, qt, kt, values, raised, inverse, turned_x, w_qkv, vecs, strips, dvec, fc_units, pitch, replicas):
    images, length, width = inputs.shape
    count = 5
    rows = count * pitch
    steps = images // count
    pairs = HEADS // 2
    pair = width // pairs
    unit_rows = QUAD * width // 2
    unit = (pairs, 2, unit_rows, LANES)
    fc_sum, qkv_sum = (fc_units.shape[0], unit_rows, LANES), (pairs, unit_rows, LANES)
    scratch = []
    for name in [name for name in CHAINS if name != "v"]:
        units = 1 if name in range(pairs) else fc_units.shape[0] // 3
        scratch += reduce_scratch(units, unit_rows, replicas, name)
    scratch += vector_scratch(dvec.shape, replicas)

    def edge(p, i):
        return jnp.where(p == pairs, i, 0)

    def tail(p, i):
        return jnp.where(p == pairs, i, 0)

    def core(p, i):
        return jnp.where(p == pairs, steps - 1, i), jnp.minimum(p, pairs - 1)

    def turned(p, i):
        at, row = core(p, i)
        return at, row, 0

    def plain(p, i):
        at, col = core(p, i)
        return at, 0, col

    def exp_at(p, i):
        at, col = core(p, i)
        return at, col, 0, 0

    strip = pl.BlockSpec((count, pair, pitch), turned)
    return pl.pallas_call(
        functools.partial(attention_backward, length, pitch, count, steps),
        grid=(pairs + 1, steps),
        in_specs=[
            pl.BlockSpec((count, length, width), lambda p, i: (edge(p, i), 0, 0)),
            pl.BlockSpec((count, pitch, width), lambda p, i: (tail(p, i), 0, 0)),
            strip, strip, strip, pl.BlockSpec((count, pitch, pair), plain),
            pl.BlockSpec((count, 2, pitch, pitch), exp_at),
            pl.BlockSpec((count, 8, pitch), lambda p, i: (core(p, i)[0], 0, 0)),
            pl.BlockSpec((count, width + 16, pitch), lambda p, i: (core(p, i)[0], 0, 0)),
            whole(w_qkv), whole(vecs), whole(strips), whole(dvec), whole(fc_units),
        ],
        out_specs=[pl.BlockSpec((count, length, width), lambda p, i: (tail(p, i), 0, 0)), HBM, HBM, HBM],
        out_shape=[sds((images, length, width), BF), sds(fc_sum, BF), sds(qkv_sum, BF), sds(dvec.shape, F32)],
        scratch_shapes=[
            pltpu.VMEM((rows, width), BF),
            pltpu.VMEM((pairs, images, 3 * pair, pitch), BF), pltpu.VMEM((width, 3 * width), BF),
            pltpu.VMEM((width + 16, 3 * pair), F32), pltpu.VMEM((pairs, 8, 3 * pair), F32), pltpu.VMEM(unit, BF), pltpu.VMEM(dvec.shape, F32),
            pltpu.VMEM(fc_sum, BF), pltpu.VMEM(qkv_sum, BF), pltpu.VMEM(dvec.shape, F32),
            pltpu.SemaphoreType.DMA((len(CHAINS) + 1,)),
        ] + scratch,
        compiler_params=params(2, collective_id=1, has_side_effects=True),
        name="attention_backward",
    )(inputs, grad_resid, grad_att, qt, kt, values, raised, inverse, turned_x, w_qkv, vecs, strips, dvec, fc_units)


def local(
    inputs, cotangent, gain_one, shift_one, w_qkv, b_query, b_value, w_proj, b_proj,
    gain_two, shift_two, w_fc1, b_fc1, w_fc2, b_fc2,
):
    images, length, width = inputs.shape
    members = lax.axis_size("group")
    replicas = lax.axis_size("replica")
    pitch = (length + 7) // 8 * 8
    qt, kt, values, raised, inverse, attended, turned_x, wq, wp, w1, w2, vecs, bias_fc1 = forward_part(
        inputs, (w_qkv, w_proj, w_fc1, w_fc2),
        (gain_one, shift_one, b_query, b_value, b_proj, gain_two, shift_two, b_fc2, b_fc1), pitch, members,
    )
    outputs, grad_resid, grad_att, fc_units, strips, dvec = middle_part(
        inputs, cotangent, attended, wp, w1, w2, vecs, bias_fc1, pitch
    )
    grad_inputs, fc_sum, qkv_sum, vec_sum = backward_part(
        inputs, grad_resid, grad_att, qt, kt, values, raised, inverse, turned_x, wq, vecs, strips, dvec, fc_units,
        pitch, replicas
    )
    factor = float(images * length * replicas * members) ** (-0.5)
    weights = (gain_one, shift_one, w_qkv, b_query, b_value, w_proj, b_proj, gain_two, shift_two, w_fc1, b_fc1, w_fc2, b_fc2)
    grad_inputs, *grads = pl.pallas_call(
        functools.partial(unpack, factor),
        grid=(1,),
        in_specs=[blocks(images, length, width), whole(fc_sum), whole(qkv_sum), whole(vec_sum)] + [
            whole(w) for w in (w_qkv, gain_one, shift_one)
        ],
        out_specs=[blocks(images, length, width)] + [whole(w) for w in weights],
        out_shape=[sds(inputs.shape, F32)] + [sds(w.shape, F32) for w in weights],
        compiler_params=params(),
        name="unpack",
    )(grad_inputs, fc_sum, qkv_sum, vec_sum, w_qkv, gain_one, shift_one)
    return (outputs, grad_inputs) + tuple(grads)


def solution(mesh):
    images = P(("replica", "group"), None, None)
    line, table = P("group"), P("group", None)
    specs = (line, line, table, line, line, table, line, line, line, table, line, table, line)
    return jax.shard_map(
        local, mesh=mesh, in_specs=(images, images) + specs, out_specs=(images, images) + specs, check_vma=False
    )
```

```python
import functools

import jax
import jax.numpy as jnp
from jax import lax
from jax.experimental import pallas as pl
from jax.experimental.pallas import tpu as pltpu
from jax.sharding import PartitionSpec as P

HEADS = 6
EPS = 1e-06
BF = jnp.bfloat16
F32 = jnp.float32
LOG2E = 1.4426950408889634
VMEM_LIMIT = 60 * 1024 * 1024
MESH = pl.DeviceIdType.MESH
LANES = 128
QUAD = 4


def dot(left, right):
    return jnp.dot(left, right, preferred_element_type=F32)


def dot_lt(left, right):
    return lax.dot_general(left, right, (((0,), (0,)), ((), ())), preferred_element_type=F32)


def dot_rt(left, right):
    return lax.dot_general(left, right, (((1,), (1,)), ((), ())), preferred_element_type=F32)


def row_stats(rows):
    centre = jnp.mean(rows, axis=-1, keepdims=True)
    centered = rows - centre
    inverse = lax.rsqrt(jnp.mean(centered * centered, axis=-1, keepdims=True) + EPS)
    return centered * inverse, inverse


def norm_back(grad_hidden, normed, inverse, gain):
    grad_normed = grad_hidden * gain
    one = jnp.mean(grad_normed, axis=-1, keepdims=True)
    two = jnp.mean(grad_normed * normed, axis=-1, keepdims=True)
    return inverse * (grad_normed - one - normed * two)


def col_sum(rows):
    return jnp.sum(rows, axis=0, keepdims=True)


def place():
    return lax.axis_index("replica"), lax.axis_index("group")


def greet(partners):
    barrier = pltpu.get_barrier_semaphore()
    for partner in partners:
        pl.semaphore_signal(barrier, inc=1, device_id=partner, device_id_type=MESH)
    pl.semaphore_wait(barrier, len(partners))


def remote(source, target, send, recv, device):
    return pltpu.make_async_remote_copy(
        src_ref=source, dst_ref=target, send_sem=send, recv_sem=recv, device_id=device, device_id_type=MESH
    )


class Gather:
    def __init__(self, shards, wholes, sends, recvs, passes, arrivals):
        self.replica, self.group = place()
        core = lax.rem(self.replica, 2)
        self.across = (self.replica, 1 - self.group)
        self.beside = (self.replica + 1 - 2 * core, self.group)
        self.first, self.second = [], []
        for k, (shard, whole_ref) in enumerate(zip(shards, wholes)):
            rows = shard.shape[0]
            half = rows // 2
            mine = pl.ds(pl.multiple_of(core * half, half), half)
            there = pl.ds(pl.multiple_of(self.group * rows + core * half, half), half)
            here = pl.ds(pl.multiple_of((1 - self.group) * rows + core * half, half), half)
            self.first.append(remote(shard.at[mine], whole_ref.at[there], sends.at[k], recvs.at[k], self.across))
            self.second.append(
                remote(whole_ref.at[here], whole_ref.at[here], passes.at[k], arrivals.at[k], self.beside)
            )


def pipeline(items, *stages):
    for tick in range(len(items) + len(stages) - 1):
        for late, stage in enumerate(stages):
            if 0 <= tick - late < len(items):
                stage(items[tick - late])


def attention_forward(
    length, pitch, count, late,
    x_ref, wq_hbm, wp_hbm, w1_hbm, w2_hbm, g1, s1, bq, bv, bp, g2, s2, b2, b1,
    qt_ref, kt_ref, v_ref, exp_ref, inv_ref, att_ref, nt_ref, wq_out, wp_out, w1_out, w2_out, vec_out, b1_out,
    normed_ref, wq, wp, w1, w2, small, wide, vec, b1_full, wqt, bias_q, k_ref,
    sends, recvs, passes, arrivals, vec_send, vec_recv, own_sem, out_sem,
):
    step = pl.program_id(0)
    width = x_ref.shape[2]
    head_dim = width // HEADS
    factor = head_dim ** (-0.5) * LOG2E
    shards = (wq_hbm, wp_hbm, w1_hbm, w2_hbm)
    wholes = (wq, wp, w1, w2)
    outs = (wq_out, wp_out, w1_out, w2_out)
    move = Gather(shards, wholes, sends, recvs, passes, arrivals)
    group = move.group
    small_copy = remote(small.at[group], small.at[group], vec_send.at[0], vec_recv.at[0], move.across)
    wide_copy = remote(wide.at[group], wide.at[group], vec_send.at[1], vec_recv.at[1], move.across)
    owns = [
        pltpu.make_async_copy(
            shard, full.at[pl.ds(pl.multiple_of(group * shard.shape[0], shard.shape[0]), shard.shape[0])], own_sem.at[k]
        )
        for k, (shard, full) in enumerate(zip(shards, wholes))
    ]
    flush = [pltpu.make_async_copy(full, out, out_sem.at[k]) for k, (full, out) in enumerate(zip(wholes, outs))]
    last = pl.num_programs(0) - 1

    @pl.when(step == 0)
    def _():
        share = g1.shape[0]
        for k, ref in enumerate((g1, s1, bq, bv, bp, g2, s2, b2)):
            small[group, k : k + 1, 0:share] = ref[...].reshape(1, share).astype(F32)
        wide[group, 0:1, :] = b1[...].reshape(1, b1.shape[0]).astype(F32)
        greet((move.across, move.beside))
        small_copy.start()
        for copy in move.first:
            copy.start()
        wide_copy.start()
        for copy in owns:
            copy.start()
        tail_ = length // 8 * 8

        @pl.loop(0, x_ref.shape[0])
        def _(image):
            normed_ref[image, tail_:, :] = jnp.zeros((pitch - tail_, width), F32)
            normed_ref[image, 0:length, :] = row_stats(x_ref[image].astype(F32))[0]

        small_copy.wait()
        for side in range(2):
            vec[:, side * share : (side + 1) * share] = small[side, :, 0:share]
        vec_out[...] = vec[...]
        bias_q[...] = jnp.broadcast_to(vec[...].T[:, 2:3], bias_q.shape)
        move.first[0].wait()
        move.second[0].start()
        owns[0].wait()
        move.second[0].wait()
        wqt[...] = wq[:, 0:width].T

    @pl.when(step == late)
    def _():
        for k in range(1, 4):
            move.first[k].wait()
            move.second[k].start()
        wide_copy.wait()
        for side in range(2):
            b1_full[0:1, side * b1.shape[0] : (side + 1) * b1.shape[0]] = wide[side, 0:1, :]
        b1_out[...] = b1_full[...]
        for k in range(1, 4):
            owns[k].wait()

    @pl.when(step == late + 1)
    def _():
        for k in range(1, 4):
            move.second[k].wait()
        for copy in flush:
            copy.start()

    gain = vec[0:1, :]
    shift = vec[1:2, :]
    normed = normed_ref[pl.ds(step * count, count)].reshape(count * pitch, width)
    hidden = (normed * gain + shift).astype(BF)
    keys_all = dot(hidden, wq[:, width : 2 * width]).astype(BF)
    values_all = (dot(hidden, wq[:, 2 * width :]) + vec[3:4, :]).astype(BF)
    for image in range(count):
        rows = slice(image * pitch, (image + 1) * pitch)
        nt_ref[image, 0:width, :] = normed[rows].astype(BF).T
        nt_ref[image, width:, :] = jnp.ones((16, pitch), BF)
        k_ref[image] = keys_all[rows]
        v_ref[image] = values_all[rows]
        qt_ref[image] = ((dot_rt(wqt[...], hidden[rows]) + bias_q[...]) * factor).astype(BF)
    tail = length // 8 * 8
    row = lax.broadcasted_iota(jnp.int32, (pitch - tail, pitch), 0) + tail
    zero = jnp.zeros((head_dim, pitch), BF)
    ones = jnp.ones((16, pitch), BF)
    kept = {}

    def score(item):
        image, two, side = item
        cols = slice(two * LANES, (two + 1) * LANES)
        if side == 0:
            kt_ref[image, cols, :] = k_ref[image, :, cols].T
            kept["vt", image, two] = v_ref[image, :, cols].T
        at = two * LANES + side * head_dim
        own = qt_ref[image, at : at + head_dim, :]
        full = jnp.concatenate([own, zero] if side == 0 else [zero, own], axis=0)
        kept[item] = dot(k_ref[image, :, cols], full)

    def soften(item):
        image, two, side = item
        scores = kept.pop(item)
        low = jnp.where(row < length, scores[tail:], -1e30)
        scores = jnp.concatenate([scores[:tail], low], axis=0)
        top = jnp.max(scores, axis=0, keepdims=True)
        raised = jnp.exp2(scores - top).astype(BF)
        exp_ref[image, 2 * two + side] = raised
        kept[item] = raised

    def mix(item):
        image, two, side = item
        own = kept["vt", image, two][side * head_dim : (side + 1) * head_dim]
        mixed = dot(jnp.concatenate([own, ones], axis=0), kept.pop(item))
        inverse = 1.0 / mixed[head_dim : head_dim + 1]
        at = two * LANES + side * head_dim
        inv_ref[image, 2 * two + side : 2 * two + side + 1, :] = inverse
        att_ref[image, at : at + head_dim, :] = (mixed[:head_dim] * inverse).astype(BF)

    items = [(image, two, side) for image in range(count) for two in range(HEADS // 2) for side in range(2)]
    pipeline(items, score, soften, mix)

    @pl.when(step == last)
    def _():
        for copy in flush:
            copy.wait()


def gelu_parts(values):
    half = 0.5 * (1.0 + lax.erf(values * 0.7071067811865476))
    slope = half + values * jnp.exp(-0.5 * values * values) * 0.3989422804014327
    return half, slope


def mlp_both(
    length, pitch, count, chunk,
    x_ref, ct_ref, att_ref, wp_ref, w1_ref, w2_ref, vec_ref, b1_ref,
    y_ref, gr_ref, ga_ref, unit_ref, strip_ref, dvec_ref,
    xpad, ctpad, att_s, act_ref, gp_ref, w2t, acc1, acc2, accp, accv, accb,
):
    step = pl.program_id(0)
    width = x_ref.shape[2]
    hidden_units = w1_ref.shape[1]

    @pl.when(step == 0)
    def _():
        for ref in (xpad, ctpad, acc1, acc2, accp, accv, accb):
            ref[...] = jnp.zeros_like(ref)
        w2t[...] = w2_ref[...].T

    for image in range(count):
        att_s[image * pitch : (image + 1) * pitch, :] = att_ref[image].T
        xpad[image * pitch : image * pitch + length, :] = x_ref[image]
        ctpad[image * pitch : image * pitch + length, :] = ct_ref[image]
    bias_p = vec_ref[4:5, :]
    gain = vec_ref[5:6, :]
    shift = vec_ref[6:7, :]
    bias_2 = vec_ref[7:8, :]
    ct = ctpad[...]
    att = att_s[...]
    resid = xpad[...].astype(F32) + dot(att, wp_ref[...]) + bias_p
    normed, inverse = row_stats(resid)
    hidden = (normed * gain + shift).astype(BF)
    for start in range(0, hidden_units, chunk):
        cols = slice(start, start + chunk)
        pre = dot(hidden, w1_ref[:, cols]) + b1_ref[0:1, cols]
        half, slope = gelu_parts(pre)
        act_ref[:, cols] = (pre * half).astype(BF)
        grad_pre = dot_rt(ct, w2_ref[cols, :]) * slope
        accb[0:1, cols] += col_sum(grad_pre)
        gp_ref[:, cols] = grad_pre.astype(BF)
    out = resid + dot_rt(w2t[...], act_ref[...]).T + bias_2
    for image in range(count):
        y_ref[image] = out[image * pitch : image * pitch + length].astype(BF)
    grad_hidden = dot_rt(w1_ref[...], gp_ref[...]).T
    top = ct.astype(F32)
    grad_resid = top + norm_back(grad_hidden, normed, inverse, gain)
    accv[0:1, :] += col_sum(grad_resid)
    accv[1:2, :] += col_sum(grad_hidden * normed)
    accv[2:3, :] += col_sum(grad_hidden)
    accv[3:4, :] += col_sum(top)
    grad_resid_b = grad_resid.astype(BF)
    for image in range(count):
        rows = slice(image * pitch, (image + 1) * pitch)
        gr_ref[image] = grad_resid[rows]
        ga_ref[image] = dot_rt(wp_ref[...], grad_resid_b[rows]).astype(BF)
    acc1[...] += dot_lt(hidden, gp_ref[...])
    acc2[...] += dot_lt(ct, act_ref[...])
    accp[...] += dot_lt(att, grad_resid_b)

    @pl.when(step == pl.num_programs(0) - 1)
    def _():
        share = width // 2
        wide = hidden_units // 2
        for side in range(2):
            rows = slice(side * share, (side + 1) * share)
            for strip in range(hidden_units // LANES):
                unit, at = strip // QUAD, strip % QUAD * share
                unit_ref[unit, side, at : at + share, :] = acc1[rows, strip * LANES : (strip + 1) * LANES].astype(BF)
            for strip in range(wide // LANES):
                unit, at = strip // 2 + hidden_units // (QUAD * LANES), strip % 2 * width
                start = side * wide + strip * LANES
                unit_ref[unit, side, at : at + width, :] = acc2[:, start : start + LANES].astype(BF)
            for strip in range(width // LANES):
                strip_ref[strip, side] = accp[rows, strip * LANES : (strip + 1) * LANES].astype(BF)
        dvec_ref[...] = jnp.zeros_like(dvec_ref)
        dvec_ref[0:4, :] = accv[0:4, :]
        for k in range(hidden_units // width):
            dvec_ref[8 + k : 9 + k, :] = accb[0:1, k * width : (k + 1) * width]


CHAINS = {
    "a": (0, 1, 4, 6, 8, 11, 13, 14),
    "b": (0, 1, 4, 6, 8, 11, 13, 14),
    "c": (0, 4, 7, 9, 11, 13, 15, 16),
    0: (4, 5, 8, 10, 12, 13, 14, 15),
    1: (8, 9, 12, 14, 16, 16),
    2: (12, 13, 14, 16, 16, 16),
    "v": (12, 13, 14, 15, 16),
}
SWAPPED = ("b", 0)
SHORT = (1, 2)


def schedule(total):
    plan = {0: [("greet", None, None)]}
    for name, starts in CHAINS.items():
        order = order_of(name)
        for k, at in enumerate(starts):
            work = (name, order[k - 1] if k else None, order[k] if k < len(order) else None)
            plan.setdefault(at if at < total else -1, []).append(work)
    return plan


def order_of(name):
    if name == "v":
        return (0, 1, 2, 3)
    return (0, 1, 3, 5, 7) if name in SHORT else (0, 1, 2, 3, 5, 6, 7)


class Ticks:
    def __init__(self, parts, flushes):
        self.parts, self.flushes = parts, flushes

    def run(self, work):
        for name, done, start in work:
            if name == "greet":
                greet(self.parts["a"].partners())
                continue
            part = self.parts[name]
            if done is not None:
                part.finish(done)
                if done == 3 and part.extra > 1:
                    part.start(4)
                    part.finish(4)
                if done == order_of(name)[-1]:
                    self.flushes[name].start()
            if start is not None:
                part.start(start)

    def close(self, work):
        pending = list(work)
        while pending:
            names, later = set(), []
            for item in pending:
                if item[0] in names:
                    later.append(item)
                else:
                    names.add(item[0])
                    self.run([item])
            pending = later
        for copy in self.flushes.values():
            copy.wait()


def make_ticks(fc_ref, unit_ref, dvec_ref, fc_out, qkv_out, vec_out, fc_hbm, qkv_hbm, vec_hbm, flush_sem, scratch):
    third = fc_ref.shape[0] // 3
    pairs = unit_ref.shape[0]
    sources = {name: (fc_ref, fc_out, fc_hbm, k * third, third) for k, name in enumerate("abc")}
    for k in range(pairs):
        sources[k] = (unit_ref, qkv_out, qkv_hbm, k, 1)
    parts, flushes = {}, {}
    for k, (name, (source, out, hbm, at, size)) in enumerate(sources.items()):
        refs = scratch[k * REDUCE_REFS : (k + 1) * REDUCE_REFS]
        mine = pl.ds(at, size)
        parts[name] = Reduce(source.at[mine], refs[:8], out.at[mine], refs[8], refs[9], name)
        flushes[name] = pltpu.make_async_copy(out.at[mine], hbm.at[mine], flush_sem.at[k])
    parts["v"] = ReduceVectors(parts["a"], *scratch[len(sources) * REDUCE_REFS :], first=dvec_ref, out=vec_out)
    flushes["v"] = pltpu.make_async_copy(vec_out, vec_hbm, flush_sem.at[len(sources)])
    return Ticks(parts, flushes)


def attention_backward(
    length, pitch, count, steps,
    x_ref, gr_ref, ga_ref, qt_ref, kt_ref, v_ref, exp_ref, inv_ref, nt_ref, wq_ref, vec_ref, strip_ref, dvec_in, fc_ref,
    gx_ref, fc_hbm, qkv_hbm, vec_hbm,
    pad_ref, gp_ref, wperm, acc, accv, unit_ref, dvec_ref, fc_out, qkv_out, vec_out, flush_sem, *scratch,
):
    phase, block = pl.program_id(0), pl.program_id(1)
    phases, blocks_ = pl.num_programs(0), pl.num_programs(1)
    step = phase * blocks_ + block
    ticks = make_ticks(
        fc_ref, unit_ref, dvec_ref, fc_out, qkv_out, vec_out, fc_hbm, qkv_hbm, vec_hbm, flush_sem, scratch
    )
    plan = schedule((HEADS // 2 + 1) * steps)
    for at, work in plan.items():
        if at >= 0:
            @pl.when(step == at)
            def _(work=work):
                ticks.run(work)
    width = x_ref.shape[2]
    head_dim = width // HEADS
    pair = 2 * head_dim
    factor = head_dim ** (-0.5)
    rows = count * pitch
    first = block * count
    gain = vec_ref[0:1, :]

    @pl.when(jnp.logical_and(phase == 0, block == 0))
    def _():
        pad_ref[...] = jnp.zeros_like(pad_ref)
        for two in range(HEADS // 2):
            for third in range(3):
                to, at = (3 * two + third) * pair, third * width + two * pair
                wperm[:, to : to + pair] = wq_ref[:, at : at + pair]

    def stats():
        for image in range(count):
            pad_ref[image * pitch : image * pitch + length, :] = x_ref[image]
        return row_stats(pad_ref[...].astype(F32))

    @pl.when(phase < phases - 1)
    def _():
        @pl.when(block == 0)
        def _():
            acc[...] = jnp.zeros_like(acc)

        zero = jnp.zeros((head_dim, pitch), BF)
        kept = {}

        def probe(item):
            image, side = item
            own = slice(side * head_dim, (side + 1) * head_dim)
            inverse = inv_ref[image, pl.ds(2 * phase + side, 1), :]
            grad_out = (ga_ref[image, own, :].astype(F32) * inverse).astype(BF)
            full = jnp.concatenate([grad_out, zero] if side == 0 else [zero, grad_out], axis=0)
            kept[item] = (dot(v_ref[image], full), grad_out, inverse)

        def soften(item):
            image, side = item
            grad_probs, grad_out, inverse = kept[item]
            raised = exp_ref[image, side].astype(F32)
            delta = jnp.sum(raised * grad_probs, axis=0, keepdims=True) * inverse
            kept[item] = ((raised * (grad_probs - delta)).astype(BF), grad_out)

        def spread(item):
            image, side = item
            scores, grad_out = kept.pop(item)
            own = slice(side * head_dim, (side + 1) * head_dim)
            grad_q = dot(kt_ref[image, own, :], scores) * factor
            grad_k = dot_rt(qt_ref[image, own, :], scores) * (1.0 / LOG2E)
            grad_v = dot_rt(grad_out, exp_ref[image, side])
            for third, part in enumerate((grad_q, grad_k, grad_v)):
                at = third * pair + side * head_dim
                gp_ref[phase, first + image, at : at + head_dim, :] = part.astype(BF)

        def gather(item):
            image, side = item
            if side == 1:
                acc[...] += dot_rt(nt_ref[image], gp_ref[phase, first + image])

        items = [(image, side) for image in range(count) for side in range(2)]
        pipeline(items, probe, soften, spread, gather)

        @pl.when(block == blocks_ - 1)
        def _():
            share = width // 2
            for side in range(2):
                for strip in range(3):
                    unit_ref[phase, side, strip * share : (strip + 1) * share, :] = acc[
                        side * share : (side + 1) * share, strip * pair : (strip + 1) * pair
                    ].astype(BF)
                unit_ref[phase, side, 3 * share :, :] = strip_ref[phase, side]
            accv[phase] = acc[width : width + 8, :]

            @pl.when(phase == phases - 2)
            def _():
                dvec_ref[...] = dvec_in[...]
                for two in range(HEADS // 2):
                    for third in range(3):
                        dvec_ref[4 + third : 5 + third, two * pair : (two + 1) * pair] = accv[
                            two, 0:1, third * pair : (third + 1) * pair
                        ]

    @pl.when(phase == phases - 1)
    def _():
        normed, inverse = stats()
        for image in range(count):
            at = slice(image * pitch, (image + 1) * pitch)
            packed = jnp.concatenate([gp_ref[two, first + image] for two in range(HEADS // 2)], axis=0)
            grad_hidden = dot(wperm[...], packed).T
            grad_x = gr_ref[image] + norm_back(grad_hidden, normed[at], inverse[at], gain)
            gx_ref[image] = grad_x[:length].astype(BF)

        @pl.when(block == blocks_ - 1)
        def _():
            ticks.close(plan.get(-1, []))


SLOTS = {False: (0, 1, 2, 3, 11, 6, 9, 10), True: (0, 1, 0, 2, 17, 9, 0, 16)}


class Reduce:
    def __init__(self, source, bufs, out, sends, recvs, name):
        self.replica, self.group = place()
        self.swapped, self.short = name in SWAPPED, name in SHORT
        self.source, self.out = source, out
        self.r1, self.b1, self.r2, self.b2, self.rx, self.bx, self.rz, self.ez = bufs
        replicas = lax.axis_size("replica")
        self.extra = replicas // 16
        half = out.shape[1] // 2
        self.half, self.quarter, self.piece = half, half // 2, half // 8
        r = self.replica
        self.core = lax.rem(r, 2)
        self.x = lax.rem(r // 2, 2)
        self.z = lax.rem(r // 4, 4)
        self.e = r // 16
        self.m = lax.rem(r // 2, 8)
        self.sends, self.recvs = sends, recvs
        low = self.core * half
        self.at_core = pl.ds(pl.multiple_of(low, half), half)
        self.at_quarter = pl.ds(pl.multiple_of(low + self.x * self.quarter, self.quarter), self.quarter)
        self.at_piece = pl.ds(
            pl.multiple_of(low + self.x * self.quarter + self.z * self.piece, self.piece), self.piece
        )

    def partners(self):
        return [self.to_core(), self.to_group()] + [self.to_m(d) for d in range(1, 8)] + [
            self.to_e(d) for d in range(1, self.extra)
        ]

    def to_core(self):
        return (self.replica + 1 - 2 * self.core, self.group)

    def to_group(self):
        return (self.replica, 1 - self.group)

    def to_x(self):
        return (self.replica + 2 - 4 * self.x, self.group)

    def z_at(self, hop):
        return lax.rem(self.z + hop, 4)

    def to_z(self, hop):
        return (self.replica + 4 * (self.z_at(hop) - self.z), self.group)

    def m_at(self, hop):
        return lax.rem(self.m + hop, 8)

    def to_m(self, hop):
        return (self.replica + 2 * (self.m_at(hop) - self.m), self.group)

    def row_of(self, m):
        start = lax.rem(m, 2) * self.quarter + m // 2 * self.piece
        return pl.ds(pl.multiple_of(start, self.piece), self.piece)

    def to_e(self, hop):
        return (self.replica + 16 * (lax.rem(self.e + hop, self.extra) - self.e), self.group)

    def copy(self, stage, source, target, device, hop=0):
        at = SLOTS[self.short][stage] + hop - (stage in (3, 5)) - (stage == 4)
        return remote(source, target, self.sends.at[at], self.recvs.at[at], device)

    def copies(self, stage):
        if stage == 0:
            other = pl.ds(pl.multiple_of((1 - self.core) * self.half, self.half), self.half)
            return [self.copy(0, self.source.at[:, :, other], self.r1, self.to_core())]
        if stage == 1 and self.swapped:
            other = pl.ds(pl.multiple_of((1 - self.x) * self.quarter, self.quarter), self.quarter)
            return [self.copy(1, self.b1.at[:, :, other], self.r2, self.to_x())]
        if stage == 2 and self.swapped:
            return [self.copy(2, self.b2.at[:, 1 - self.group], self.rx, self.to_group())]
        if stage == 1:
            return [self.copy(1, self.b1.at[:, 1 - self.group], self.r2, self.to_group())]
        if stage == 2:
            other = pl.ds(pl.multiple_of((1 - self.x) * self.quarter, self.quarter), self.quarter)
            return [self.copy(2, self.b2.at[:, other], self.rx, self.to_x())]
        if stage == 3 and self.short:
            return [
                self.copy(3, self.b2.at[:, self.row_of(self.m_at(hop))], self.rz.at[hop - 1], self.to_m(hop), hop)
                for hop in range(1, 8)
            ]
        if stage == 5 and self.short:
            place_ = self.out.at[:, self.at_piece]
            return [self.copy(5, place_, place_, self.to_m(hop), hop) for hop in range(1, 8)]
        if stage == 3:
            out = []
            for hop in (1, 2, 3):
                theirs = pl.ds(pl.multiple_of(self.z_at(hop) * self.piece, self.piece), self.piece)
                out.append(self.copy(3, self.bx.at[:, theirs], self.rz.at[hop - 1], self.to_z(hop), hop))
            return out
        if stage == 4:
            return [
                self.copy(4, self.ez.at[self.e], self.ez.at[self.e], self.to_e(hop), hop) for hop in range(1, self.extra)
            ]
        if stage == 5:
            place_ = self.out.at[:, self.at_piece]
            return [self.copy(5, place_, place_, self.to_z(hop), hop) for hop in (1, 2, 3)]
        if stage == 6:
            place_ = self.out.at[:, self.at_quarter]
            return [self.copy(6, place_, place_, self.to_x())]
        place_ = self.out.at[:, self.at_core]
        return [self.copy(7, place_, place_, self.to_core())]

    def start(self, stage):
        for copy in self.copies(stage):
            copy.start()

    def finish(self, stage):
        for copy in self.copies(stage):
            copy.wait()
        if stage == 0:
            self.b1[...] = self.source[:, :, self.at_core] + self.r1[...]
        elif stage == 1 and self.swapped:
            mine = pl.ds(pl.multiple_of(self.x * self.quarter, self.quarter), self.quarter)
            self.b2[...] = self.b1[:, :, mine] + self.r2[...]
        elif stage == 2 and self.swapped:
            self.bx[...] = self.b2[:, self.group] + self.rx[...]
        elif stage == 1:
            self.b2[...] = self.b1[:, self.group] + self.r2[...]
        elif stage == 2:
            mine = pl.ds(pl.multiple_of(self.x * self.quarter, self.quarter), self.quarter)
            self.bx[...] = self.b2[:, mine] + self.rx[...]
        elif stage == 3:
            mine = pl.ds(pl.multiple_of(self.z * self.piece, self.piece), self.piece)
            own = self.b2.at[:, self.row_of(self.m)] if self.short else self.bx.at[:, mine]
            total = own[...].astype(F32)
            for hop in range(self.rz.shape[0]):
                total = total + self.rz[hop].astype(F32)
            if self.extra > 1:
                self.ez[self.e] = total.astype(BF)
            else:
                self.out[:, self.at_piece] = total.astype(BF)
        elif stage == 4 and self.extra > 1:
            total = self.ez[0].astype(F32)
            for k in range(1, self.extra):
                total = total + self.ez[k].astype(F32)
            self.out[:, self.at_piece] = total.astype(BF)


def reduce_scratch(units, rows, replicas, name):
    half, extra = rows // 2, max(replicas // 16, 1)
    sems = SLOTS[name in SHORT][4] + extra - 1
    second = (units, 2, half // 2, LANES) if name in SWAPPED else (units, half, LANES)
    return [
        pltpu.VMEM((units, 2, half, LANES), BF), pltpu.VMEM((units, 2, half, LANES), BF),
        pltpu.VMEM(second, BF), pltpu.VMEM(second, BF),
        pltpu.VMEM((units, half // 2, LANES), BF), pltpu.VMEM((units, half // 2, LANES), BF),
        pltpu.VMEM((7 if name in SHORT else 3, units, half // 8, LANES), BF), pltpu.VMEM((extra, units, half // 8, LANES), BF),
        pltpu.SemaphoreType.DMA((sems,)), pltpu.SemaphoreType.DMA((sems,)),
    ]


class ReduceVectors:
    def __init__(self, like, v2, v3, slots_z, slots_e, got, sends, recvs, first, out):
        self.like, self.out, self.extra = like, out, like.extra
        self.vals, self.slots_z, self.slots_e, self.got, self.sends, self.recvs = (
            (first, v2, v3), slots_z, slots_e, got, sends, recvs
        )

    def copies(self, stage):
        o = self.like
        if stage < 3:
            device = (o.to_core, o.to_group, o.to_x)[stage]()
            return [remote(self.vals[stage], self.got.at[stage], self.sends.at[stage], self.recvs.at[stage], device)]
        if stage == 3:
            mine = self.slots_z.at[o.z]
            return [
                remote(mine, mine, self.sends.at[2 + hop], self.recvs.at[2 + hop], o.to_z(hop)) for hop in (1, 2, 3)
            ]
        mine = self.slots_e.at[o.e]
        return [
            remote(mine, mine, self.sends.at[5 + hop], self.recvs.at[5 + hop], o.to_e(hop)) for hop in range(1, o.extra)
        ]

    def start(self, stage):
        for copy in self.copies(stage):
            copy.start()

    def finish(self, stage):
        o, out = self.like, self.out
        for copy in self.copies(stage):
            copy.wait()
        if stage < 2:
            self.vals[stage + 1][...] = self.vals[stage][...] + self.got[stage]
        elif stage == 2:
            self.slots_z[o.z] = self.vals[2][...] + self.got[2]
        elif stage == 3:
            total = self.slots_z[0] + self.slots_z[1] + self.slots_z[2] + self.slots_z[3]
            if o.extra > 1:
                self.slots_e[o.e] = total
            else:
                out[...] = total
        elif o.extra > 1:
            total = self.slots_e[0]
            for k in range(1, o.extra):
                total = total + self.slots_e[k]
            out[...] = total


def vector_scratch(shape, replicas):
    extra = max(replicas // 16, 1)
    return [
        pltpu.VMEM(shape, F32), pltpu.VMEM(shape, F32),
        pltpu.VMEM((4,) + shape, F32), pltpu.VMEM((extra,) + shape, F32), pltpu.VMEM((3,) + shape, F32),
        pltpu.SemaphoreType.DMA((5 + extra,)), pltpu.SemaphoreType.DMA((5 + extra,)),
    ]


REDUCE_REFS = 10


def unpack(factor, gx_in, fc_ref, qkv_ref, vec_ref, w_ref, gain_ref, shift_ref, gx_out, g1, s1, wq, bq, bv, wp, bp, g2, s2, w1, b1, w2, b2):
    gx_out[...] = gx_in[...].astype(F32)

    @pl.when(pl.program_id(0) == 0)
    def _():
        share, width = wp.shape
        group = lax.axis_index("group")
        pair = LANES
        column = [
            jnp.broadcast_to(ref[...].reshape(1, share).astype(F32), (8, share)).T[:, 0:1] for ref in (gain_ref, shift_ref)
        ]
        sum_g = jnp.zeros((share, pair), F32)
        sum_s = jnp.zeros((share, pair), F32)
        for two in range(qkv_ref.shape[0]):
            for third in range(3):
                cols = slice(third * width + two * pair, third * width + (two + 1) * pair)
                cross = qkv_ref[two, third * share : (third + 1) * share, :].astype(F32)
                total = vec_ref[4 + third : 5 + third, two * pair : (two + 1) * pair]
                weight = w_ref[:, cols].astype(F32)
                sum_g += weight * cross
                sum_s += weight * total
                wq[:, cols] = (column[0] * cross + column[1] * total) * factor
            wp[:, two * pair : (two + 1) * pair] = qkv_ref[two, 3 * share :, :].astype(F32) * factor
        for ref, total in ((g1, sum_g), (s1, sum_s)):
            ref[...] = (col_sum(total.T) * factor).reshape(share)
        strips = w1.shape[1] // LANES
        for strip in range(strips):
            unit, at = strip // QUAD, strip % QUAD * share
            w1[:, strip * LANES : (strip + 1) * LANES] = fc_ref[unit, at : at + share, :].astype(F32) * factor
        for strip in range(w2.shape[0] // LANES):
            unit, at = strip // 2 + strips // QUAD, strip % 2 * width
            w2[strip * LANES : (strip + 1) * LANES, :] = (fc_ref[unit, at : at + width, :].astype(F32) * factor).T
        rows = vec_ref[...] * factor
        mine = jnp.where(group == 0, rows[:, 0:share], rows[:, share:])
        for k, ref in enumerate((bp, g2, s2, b2, bq, None, bv)):
            if ref is not None:
                ref[...] = mine[k : k + 1, :].reshape(share)
        per = b1.shape[0] // width
        for k in range(per):
            row = jnp.where(group == 0, rows[8 + k : 9 + k, :], rows[8 + per + k : 9 + per + k, :])
            b1[k * width : (k + 1) * width] = row.reshape(width)


def whole(array):
    return pl.BlockSpec(array.shape, lambda *_: (0,) * len(array.shape))


def blocks(count, *rest):
    return pl.BlockSpec((count,) + rest, lambda i: (i,) + (0,) * len(rest))


def fixed(*shape):
    return pl.BlockSpec(shape, lambda *_: (0,) * len(shape))


def params(axes=1, **kw):
    return pltpu.CompilerParams(vmem_limit_bytes=VMEM_LIMIT, dimension_semantics=("arbitrary",) * axes, **kw)


HBM = pl.BlockSpec(memory_space=pl.ANY)
sds = jax.ShapeDtypeStruct


def forward_part(inputs, weights, vectors, pitch, members):
    images, length, width = inputs.shape
    count = 4
    share, wide = vectors[0].shape[0], vectors[-1].shape[0]
    lanes = (share + LANES - 1) // LANES * LANES
    fulls = [(members * w.shape[0], w.shape[1]) for w in weights]
    turned = (images, width, pitch)
    return pl.pallas_call(
        functools.partial(attention_forward, length, pitch, count, 3),
        grid=(images // count,),
        in_specs=[whole(inputs)] + [HBM] * 4 + [whole(v) for v in vectors],
        out_specs=[
            blocks(count, width, pitch), blocks(count, width, pitch), blocks(count, pitch, width),
            blocks(count, HEADS, pitch, pitch), blocks(count, 8, pitch), blocks(count, width, pitch),
            blocks(count, width + 16, pitch), HBM, HBM, HBM, HBM, fixed(8, width), fixed(8, members * wide),
        ],
        out_shape=[
            sds(turned, BF), sds(turned, BF), sds((images, pitch, width), BF),
            sds((images, HEADS, pitch, pitch), BF), sds((images, 8, pitch), F32), sds(turned, BF),
            sds((images, width + 16, pitch), BF),
        ] + [sds(full, BF) for full in fulls] + [sds((8, width), F32), sds((8, members * wide), F32)],
        scratch_shapes=[pltpu.VMEM((images, pitch, width), F32)] + [pltpu.VMEM(full, BF) for full in fulls] + [
            pltpu.VMEM((members, 8, lanes), F32), pltpu.VMEM((members, 8, wide), F32),
            pltpu.VMEM((8, width), F32), pltpu.VMEM((8, members * wide), F32),
            pltpu.VMEM((width, width), BF), pltpu.VMEM((width, pitch), F32), pltpu.VMEM((count, pitch, width), BF),
            pltpu.SemaphoreType.DMA((4,)), pltpu.SemaphoreType.DMA((4,)), pltpu.SemaphoreType.DMA((4,)),
            pltpu.SemaphoreType.DMA((4,)), pltpu.SemaphoreType.DMA((2,)), pltpu.SemaphoreType.DMA((2,)),
            pltpu.SemaphoreType.DMA((4,)), pltpu.SemaphoreType.DMA((4,)),
        ],
        compiler_params=params(collective_id=0, has_side_effects=True),
        name="attention_forward",
    )(inputs, *weights, *vectors)


def middle_part(inputs, cotangent, attended, w_proj, w_fc1, w_fc2, vecs, bias_fc1, pitch):
    images, length, width = inputs.shape
    hidden_units = w_fc1.shape[1]
    count = 5
    rows = count * pitch
    units = 2 * hidden_units // (QUAD * LANES)
    unit_rows = QUAD * width // 2
    unit = (units, 2, unit_rows, LANES)
    strip = (width // LANES, 2, width // 2, LANES)
    return pl.pallas_call(
        functools.partial(mlp_both, length, pitch, count, 256),
        grid=(images // count,),
        in_specs=[blocks(count, length, width), blocks(count, length, width), blocks(count, width, pitch)] + [
            whole(w) for w in (w_proj, w_fc1, w_fc2, vecs, bias_fc1)
        ],
        out_specs=[
            blocks(count, length, width), blocks(count, pitch, width), blocks(count, width, pitch),
            fixed(*unit), fixed(*strip), fixed(16, width),
        ],
        out_shape=[
            sds((images, length, width), BF), sds((images, pitch, width), F32), sds((images, width, pitch), BF),
            sds(unit, BF), sds(strip, BF), sds((16, width), F32),
        ],
        scratch_shapes=[
            pltpu.VMEM((rows, width), BF), pltpu.VMEM((rows, width), BF), pltpu.VMEM((rows, width), BF),
            pltpu.VMEM((rows, hidden_units), BF), pltpu.VMEM((rows, hidden_units), BF),
            pltpu.VMEM((width, hidden_units), BF),
            pltpu.VMEM((width, hidden_units), F32), pltpu.VMEM((width, hidden_units), F32),
            pltpu.VMEM((width, width), F32), pltpu.VMEM((8, width), F32), pltpu.VMEM((8, hidden_units), F32),
        ],
        compiler_params=params(),
        name="mlp_both",
    )(inputs, cotangent, attended, w_proj, w_fc1, w_fc2, vecs, bias_fc1)


def backward_part(inputs, grad_resid, grad_att, qt, kt, values, raised, inverse, turned_x, w_qkv, vecs, strips, dvec, fc_units, pitch, replicas):
    images, length, width = inputs.shape
    count = 5
    rows = count * pitch
    steps = images // count
    pairs = HEADS // 2
    pair = width // pairs
    unit_rows = QUAD * width // 2
    unit = (pairs, 2, unit_rows, LANES)
    fc_sum, qkv_sum = (fc_units.shape[0], unit_rows, LANES), (pairs, unit_rows, LANES)
    scratch = []
    for name in [name for name in CHAINS if name != "v"]:
        units = 1 if name in range(pairs) else fc_units.shape[0] // 3
        scratch += reduce_scratch(units, unit_rows, replicas, name)
    scratch += vector_scratch(dvec.shape, replicas)

    def edge(p, i):
        return jnp.where(p == pairs, i, 0)

    def tail(p, i):
        return jnp.where(p == pairs, i, 0)

    def core(p, i):
        return jnp.where(p == pairs, steps - 1, i), jnp.minimum(p, pairs - 1)

    def turned(p, i):
        at, row = core(p, i)
        return at, row, 0

    def plain(p, i):
        at, col = core(p, i)
        return at, 0, col

    def exp_at(p, i):
        at, col = core(p, i)
        return at, col, 0, 0

    strip = pl.BlockSpec((count, pair, pitch), turned)
    return pl.pallas_call(
        functools.partial(attention_backward, length, pitch, count, steps),
        grid=(pairs + 1, steps),
        in_specs=[
            pl.BlockSpec((count, length, width), lambda p, i: (edge(p, i), 0, 0)),
            pl.BlockSpec((count, pitch, width), lambda p, i: (tail(p, i), 0, 0)),
            strip, strip, strip, pl.BlockSpec((count, pitch, pair), plain),
            pl.BlockSpec((count, 2, pitch, pitch), exp_at),
            pl.BlockSpec((count, 8, pitch), lambda p, i: (core(p, i)[0], 0, 0)),
            pl.BlockSpec((count, width + 16, pitch), lambda p, i: (core(p, i)[0], 0, 0)),
            whole(w_qkv), whole(vecs), whole(strips), whole(dvec), whole(fc_units),
        ],
        out_specs=[pl.BlockSpec((count, length, width), lambda p, i: (tail(p, i), 0, 0)), HBM, HBM, HBM],
        out_shape=[sds((images, length, width), BF), sds(fc_sum, BF), sds(qkv_sum, BF), sds(dvec.shape, F32)],
        scratch_shapes=[
            pltpu.VMEM((rows, width), BF),
            pltpu.VMEM((pairs, images, 3 * pair, pitch), BF), pltpu.VMEM((width, 3 * width), BF),
            pltpu.VMEM((width + 16, 3 * pair), F32), pltpu.VMEM((pairs, 8, 3 * pair), F32), pltpu.VMEM(unit, BF), pltpu.VMEM(dvec.shape, F32),
            pltpu.VMEM(fc_sum, BF), pltpu.VMEM(qkv_sum, BF), pltpu.VMEM(dvec.shape, F32),
            pltpu.SemaphoreType.DMA((len(CHAINS) + 1,)),
        ] + scratch,
        compiler_params=params(2, collective_id=1, has_side_effects=True),
        name="attention_backward",
    )(inputs, grad_resid, grad_att, qt, kt, values, raised, inverse, turned_x, w_qkv, vecs, strips, dvec, fc_units)


def local(
    inputs, cotangent, gain_one, shift_one, w_qkv, b_query, b_value, w_proj, b_proj,
    gain_two, shift_two, w_fc1, b_fc1, w_fc2, b_fc2,
):
    images, length, width = inputs.shape
    members = lax.axis_size("group")
    replicas = lax.axis_size("replica")
    pitch = (length + 7) // 8 * 8
    qt, kt, values, raised, inverse, attended, turned_x, wq, wp, w1, w2, vecs, bias_fc1 = forward_part(
        inputs, (w_qkv, w_proj, w_fc1, w_fc2),
        (gain_one, shift_one, b_query, b_value, b_proj, gain_two, shift_two, b_fc2, b_fc1), pitch, members,
    )
    outputs, grad_resid, grad_att, fc_units, strips, dvec = middle_part(
        inputs, cotangent, attended, wp, w1, w2, vecs, bias_fc1, pitch
    )
    grad_inputs, fc_sum, qkv_sum, vec_sum = backward_part(
        inputs, grad_resid, grad_att, qt, kt, values, raised, inverse, turned_x, wq, vecs, strips, dvec, fc_units,
        pitch, replicas
    )
    factor = float(images * length * replicas * members) ** (-0.5)
    weights = (gain_one, shift_one, w_qkv, b_query, b_value, w_proj, b_proj, gain_two, shift_two, w_fc1, b_fc1, w_fc2, b_fc2)
    grad_inputs, *grads = pl.pallas_call(
        functools.partial(unpack, factor),
        grid=(1,),
        in_specs=[blocks(images, length, width), whole(fc_sum), whole(qkv_sum), whole(vec_sum)] + [
            whole(w) for w in (w_qkv, gain_one, shift_one)
        ],
        out_specs=[blocks(images, length, width)] + [whole(w) for w in weights],
        out_shape=[sds(inputs.shape, F32)] + [sds(w.shape, F32) for w in weights],
        compiler_params=params(),
        name="unpack",
    )(grad_inputs, fc_sum, qkv_sum, vec_sum, w_qkv, gain_one, shift_one)
    return (outputs, grad_inputs) + tuple(grads)


def solution(mesh):
    images = P(("replica", "group"), None, None)
    line, table = P("group"), P("group", None)
    specs = (line, line, table, line, line, table, line, line, line, table, line, table, line)
    return jax.shard_map(
        local, mesh=mesh, in_specs=(images, images) + specs, out_specs=(images, images) + specs, check_vma=False
    )
```
